32 devices in a mesh: dp: 2 (over x), tp: 16 (over z, y, core).
Axes of the slice: x: 2, y: 2, z: 4, core: 2. Of those that a mesh axis runs over, the one named last changes fastest.
Arguments:
- token_ids: int32 [2, 2048], P('dp'), parts along dimension 0
- route_idx: int32 [2, 2048, 8], P('dp'), parts along dimension 0
- embed_table: bfloat16 [50304, 2048], P('tp')
- attn_norm: bfloat16 [2048], replicated
- w_query: bfloat16 [2048, 2048], P(None, 'tp')
- w_key: bfloat16 [2048, 2048], P(None, 'tp')
- w_value: bfloat16 [2048, 2048], P(None, 'tp')
- w_out: bfloat16 [2048, 2048], P('tp')
- q_gain: bfloat16 [2048], P('tp')
- k_gain: bfloat16 [2048], P('tp')
- mlp_norm: bfloat16 [2048], replicated
- w_router: bfloat16 [2048, 64], replicated
- w_gate: bfloat16 [64, 2048, 1024], P(None, None, 'tp')
- w_up: bfloat16 [64, 2048, 1024], P(None, None, 'tp')
- w_down: bfloat16 [64, 1024, 2048], P(None, 'tp')
Outputs:
- output: bfloat16 [2, 2048, 2048], P('dp', 'tp'), parts along dimension 0
There are 2 independent parts. The reference program is written for one: setup_inputs(seed, part) draws one part's arguments, and reference() takes and returns one part's arrays. A program takes and returns all parts, laid end to end along the dimension named above; an argument that names none is the same for every part.
All inputs are finite; a program needn't handle non-finite values.
Results may differ from the reference program's by a relative error of at most 0.010359.
Values are sent between devices in bfloat16 or wider.
A program may use at most 1 GiB of HBM per device.

```python
import jax
import jax.numpy as jnp
from jax import lax

VOCAB_SIZE = 50304
MODEL_DIM = 2048
NUM_HEADS = 16
HEAD_DIM = 128
NUM_EXPERTS = 64
TOP_K = 8
EXPERT_FF = 1024
BATCH_SIZE = 1
SEQ_LEN = 2048


def rms_norm(act_in, norm_gain):
    act_f32 = act_in.astype(jnp.float32)
    mean_sq = jnp.mean(act_f32 * act_f32, axis=-1, keepdims=True)
    return act_f32 * lax.rsqrt(mean_sq + 1e-5) * norm_gain.astype(jnp.float32)


def rope_tables(seq_len):
    half_dim = HEAD_DIM // 2
    inv_freq = 1.0 / (10000.0 ** (jnp.arange(half_dim, dtype=jnp.float32) * (2.0 / HEAD_DIM)))
    angles = jnp.arange(seq_len, dtype=jnp.float32)[:, None] * inv_freq[None, :]
    return jnp.cos(angles), jnp.sin(angles)


def apply_rope(heads_f32, cos_tab, sin_tab):
    half_dim = HEAD_DIM // 2
    first_half = heads_f32[..., :half_dim]
    second_half = heads_f32[..., half_dim:]
    cos_b = cos_tab[:, None, :]
    sin_b = sin_tab[:, None, :]
    rotated = jnp.concatenate([first_half * cos_b - second_half * sin_b, second_half * cos_b + first_half * sin_b], axis=-1)
    return rotated.astype(jnp.bfloat16)


def attend_head(operands):
    query_h, key_h, value_h = operands
    seq_len = query_h.shape[0]
    scores = jnp.dot(query_h, key_h.T, preferred_element_type=jnp.float32) * (HEAD_DIM ** -0.5)
    positions = jnp.arange(seq_len)
    scores = jnp.where(positions[:, None] >= positions[None, :], scores, -1e30)
    attn_prob = jax.nn.softmax(scores, axis=-1)
    return jnp.dot(attn_prob.astype(jnp.bfloat16), value_h, preferred_element_type=jnp.float32).astype(jnp.bfloat16)


def setup_inputs(seed: int = 0, part: int = 0) -> dict:
    base_key = jax.random.key(seed)
    part_key = jax.random.fold_in(base_key, part)
    shared = jax.random.split(base_key, 16)
    own_keys = jax.random.split(part_key, 5)
    q_width = NUM_HEADS * HEAD_DIM
    tok_shape = (BATCH_SIZE, SEQ_LEN)

    def normal_draw(key_in, shape_in, scale_in):
        return (jax.random.normal(key_in, shape_in, jnp.float32) * scale_in).astype(jnp.bfloat16)

    def gain_draw(key_in, gain_width, low_val, high_val):
        return jax.random.uniform(key_in, (gain_width,), jnp.float32, low_val, high_val).astype(jnp.bfloat16)

    uniform_ids = jax.random.randint(own_keys[0], tok_shape, 0, VOCAB_SIZE)
    hot_ids = jax.random.randint(own_keys[1], tok_shape, 0, VOCAB_SIZE // 8)
    pick_hot = jax.random.randint(own_keys[2], tok_shape, 0, 2)
    token_ids = jnp.where(pick_hot == 1, hot_ids, uniform_ids)
    token_ids = token_ids.at[0, 0].set(VOCAB_SIZE - 1).at[0, 1].set(0).astype(jnp.int32)

    expert_iota = jnp.arange(NUM_EXPERTS, dtype=jnp.int32)
    expert_bias = jax.random.randint(own_keys[3], (NUM_EXPERTS,), 0, 2 * NUM_EXPERTS)
    route_noise = jax.random.randint(own_keys[4], (BATCH_SIZE, SEQ_LEN, NUM_EXPERTS), 0, 4 * NUM_EXPERTS)
    route_score = (expert_bias[None, None, :] + route_noise) * NUM_EXPERTS + expert_iota[None, None, :]
    edge_bonus = jnp.where((expert_iota == 0) | (expert_iota == NUM_EXPERTS - 1), 16 * NUM_EXPERTS * NUM_EXPERTS, 0)
    route_score = route_score.at[0, 0].add(edge_bonus)
    route_idx = lax.top_k(route_score, TOP_K)[1].astype(jnp.int32)

    head_q = jnp.repeat(jnp.exp(jax.random.uniform(shared[0], (NUM_HEADS,), jnp.float32, -0.5, 0.5)), HEAD_DIM)
    head_k = jnp.repeat(jnp.exp(jax.random.uniform(shared[1], (NUM_HEADS,), jnp.float32, -0.5, 0.5)), HEAD_DIM)
    down_scale = EXPERT_FF ** -0.5 * NUM_EXPERTS / (2.0 * TOP_K ** 0.5)
    return {
        "token_ids": token_ids,
        "route_idx": route_idx,
        "embed_table": normal_draw(shared[2], (VOCAB_SIZE, MODEL_DIM), 1.0),
        "attn_norm": gain_draw(shared[3], MODEL_DIM, 0.5, 1.5),
        "w_query": normal_draw(shared[4], (MODEL_DIM, q_width), MODEL_DIM ** -0.5 * head_q[None, :]),
        "w_key": normal_draw(shared[5], (MODEL_DIM, q_width), MODEL_DIM ** -0.5 * head_k[None, :]),
        "w_value": normal_draw(shared[6], (MODEL_DIM, q_width), MODEL_DIM ** -0.5),
        "w_out": normal_draw(shared[7], (q_width, MODEL_DIM), q_width ** -0.5),
        "q_gain": gain_draw(shared[8], q_width, 0.8, 1.6),
        "k_gain": gain_draw(shared[9], q_width, 0.8, 1.6),
        "mlp_norm": gain_draw(shared[10], MODEL_DIM, 0.5, 1.5),
        "w_router": normal_draw(shared[11], (MODEL_DIM, NUM_EXPERTS), MODEL_DIM ** -0.5),
        "w_gate": normal_draw(shared[12], (NUM_EXPERTS, MODEL_DIM, EXPERT_FF), MODEL_DIM ** -0.5),
        "w_up": normal_draw(shared[13], (NUM_EXPERTS, MODEL_DIM, EXPERT_FF), MODEL_DIM ** -0.5),
        "w_down": normal_draw(shared[14], (NUM_EXPERTS, EXPERT_FF, MODEL_DIM), down_scale),
    }


def reference(token_ids, route_idx, embed_table, attn_norm, w_query, w_key, w_value, w_out, q_gain, k_gain, mlp_norm, w_router, w_gate, w_up, w_down):
    tok_count = BATCH_SIZE * SEQ_LEN
    q_width = NUM_HEADS * HEAD_DIM
    x_embed = jnp.take(embed_table, token_ids.reshape(tok_count), axis=0)
    normed = rms_norm(x_embed, attn_norm).astype(jnp.bfloat16)
    q_raw = jnp.dot(normed, w_query, preferred_element_type=jnp.float32)
    k_raw = jnp.dot(normed, w_key, preferred_element_type=jnp.float32)
    v_proj = jnp.dot(normed, w_value, preferred_element_type=jnp.float32).astype(jnp.bfloat16)
    cos_tab, sin_tab = rope_tables(SEQ_LEN)
    head_shape = (BATCH_SIZE, SEQ_LEN, NUM_HEADS, HEAD_DIM)
    q_heads = apply_rope(rms_norm(q_raw, q_gain).reshape(head_shape), cos_tab, sin_tab)
    k_heads = apply_rope(rms_norm(k_raw, k_gain).reshape(head_shape), cos_tab, sin_tab)
    v_heads = v_proj.reshape(head_shape)

    def to_rows(heads_in):
        return jnp.transpose(heads_in, (0, 2, 1, 3)).reshape(BATCH_SIZE * NUM_HEADS, SEQ_LEN, HEAD_DIM)

    context = lax.map(attend_head, (to_rows(q_heads), to_rows(k_heads), to_rows(v_heads)))
    context = jnp.transpose(context.reshape(BATCH_SIZE, NUM_HEADS, SEQ_LEN, HEAD_DIM), (0, 2, 1, 3)).reshape(tok_count, q_width)
    attn_out = jnp.dot(context, w_out, preferred_element_type=jnp.float32).astype(jnp.bfloat16)
    hidden = (x_embed.astype(jnp.float32) + attn_out.astype(jnp.float32)).astype(jnp.bfloat16)

    moe_in = rms_norm(hidden, mlp_norm).astype(jnp.bfloat16)
    router_prob = jax.nn.softmax(jnp.dot(moe_in, w_router, preferred_element_type=jnp.float32), axis=-1)
    flat_choice = route_idx.reshape(tok_count, TOP_K)
    expert_iota = jnp.arange(NUM_EXPERTS, dtype=jnp.int32)
    gate_dense = jnp.sum(jnp.where(flat_choice[:, :, None] == expert_iota[None, None, :], router_prob[:, None, :], 0.0), axis=1)

    def expert_step(acc_sum, operands):
        gate_w, up_w, down_w, gate_col = operands
        gate_proj = jnp.dot(moe_in, gate_w, preferred_element_type=jnp.float32)
        up_proj = jnp.dot(moe_in, up_w, preferred_element_type=jnp.float32)
        hidden_act = (jax.nn.silu(gate_proj) * up_proj).astype(jnp.bfloat16)
        return acc_sum + gate_col[:, None] * jnp.dot(hidden_act, down_w, preferred_element_type=jnp.float32), None

    expert_sum = lax.scan(expert_step, jnp.zeros((tok_count, MODEL_DIM), jnp.float32), (w_gate, w_up, w_down, gate_dense.T))[0]
    moe_out = expert_sum.astype(jnp.bfloat16)
    layer_out = (hidden.astype(jnp.float32) + moe_out.astype(jnp.float32)).astype(jnp.bfloat16)
    return layer_out.reshape(BATCH_SIZE, SEQ_LEN, MODEL_DIM)
```

```python
import jax
import jax.numpy as jnp
from jax import lax
from jax.experimental import pallas as pl
from jax.experimental.pallas import tpu as pltpu
from jax.sharding import PartitionSpec as P

HEAD_DIM = 128
NORM_EPS = 1e-5
N_CHUNKS = 4


def rms_scale(act_in, norm_gain):
    act_f32 = act_in.astype(jnp.float32)
    mean_sq = jnp.mean(act_f32 * act_f32, axis=-1, keepdims=True)
    return act_f32 * lax.rsqrt(mean_sq + NORM_EPS) * norm_gain.astype(jnp.float32)


def rope_tables(seq_len):
    half_dim = HEAD_DIM // 2
    inv_freq = 1.0 / (10000.0 ** (jnp.arange(half_dim, dtype=jnp.float32) * (2.0 / HEAD_DIM)))
    angles = jnp.arange(seq_len, dtype=jnp.float32)[:, None] * inv_freq[None, :]
    return jnp.cos(angles), jnp.sin(angles)


def apply_rope(heads_f32, cos_tab, sin_tab):
    half_dim = HEAD_DIM // 2
    first_half = heads_f32[..., :half_dim]
    second_half = heads_f32[..., half_dim:]
    cos_b = cos_tab[:, None, :]
    sin_b = sin_tab[:, None, :]
    rotated = jnp.concatenate([first_half * cos_b - second_half * sin_b, second_half * cos_b + first_half * sin_b], axis=-1)
    return rotated.astype(jnp.bfloat16)


EXP_PER_STEP = 8
ROW_TILE = 256


def moe_kernel(m_ref, mask_ref, wr_ref, wg_ref, wu_ref, wd_ref, out_ref, acc_ref, gate_ref):
    step = pl.program_id(0)
    n_tok = m_ref.shape[0]
    ff_cols = wg_ref.shape[0]
    n_exp = wr_ref.shape[0]
    exp_ff = ff_cols // EXP_PER_STEP
    nt_dims = (((1,), (1,)), ((), ()))

    @pl.when(step == 0)
    def _():
        logits = lax.dot_general(m_ref[...], wr_ref[...], nt_dims, preferred_element_type=jnp.float32)
        logits = logits - jnp.max(logits, axis=-1, keepdims=True)
        expd = jnp.exp(logits)
        gates = expd / jnp.sum(expd, axis=-1, keepdims=True) * mask_ref[...]
        for grp in range(n_exp // EXP_PER_STEP):
            gate_ref[grp] = gates[:, grp * EXP_PER_STEP:(grp + 1) * EXP_PER_STEP]
        acc_ref[...] = jnp.zeros_like(acc_ref)

    def row_body(i, carry):
        rows = pl.ds(pl.multiple_of(i * ROW_TILE, ROW_TILE), ROW_TILE)
        m_tile = m_ref[rows, :]
        gate_proj = lax.dot_general(m_tile, wg_ref[...], nt_dims, preferred_element_type=jnp.float32)
        up_proj = lax.dot_general(m_tile, wu_ref[...], nt_dims, preferred_element_type=jnp.float32)
        act = (gate_proj / (1.0 + jnp.exp(-gate_proj)) * up_proj).astype(jnp.bfloat16).astype(jnp.float32)
        gates = gate_ref[step, rows, :]
        lane = lax.broadcasted_iota(jnp.int32, (ROW_TILE, 2 * exp_ff), 1)
        pieces = []
        for pair in range(EXP_PER_STEP // 2):
            pieces.append(jnp.where(lane < exp_ff, gates[:, 2 * pair:2 * pair + 1], gates[:, 2 * pair + 1:2 * pair + 2]))
        scaled = act * jnp.concatenate(pieces, axis=1)
        high = scaled.astype(jnp.bfloat16)
        low = (scaled - high.astype(jnp.float32)).astype(jnp.bfloat16)
        down = jnp.dot(high, wd_ref[...], preferred_element_type=jnp.float32) + jnp.dot(low, wd_ref[...], preferred_element_type=jnp.float32)
        acc_ref[rows, :] += down
        return carry

    lax.fori_loop(0, n_tok // ROW_TILE, row_body, 0)

    @pl.when(step == pl.num_programs(0) - 1)
    def _():
        out_ref[...] = acc_ref[...].astype(out_ref.dtype)


def dense_moe(m_rows, mask, wr_t, wg_t, wu_t, w_dn):
    n_tok, model_dim = m_rows.shape
    n_exp = wr_t.shape[0]
    n_ff = wg_t.shape[0]
    step_cols = n_ff // n_exp * EXP_PER_STEP
    flops = 2 * n_tok * model_dim * n_ff * 4
    return pl.pallas_call(
        moe_kernel,
        grid=(n_ff // step_cols,),
        in_specs=[
            pl.BlockSpec((n_tok, model_dim), lambda s: (0, 0)),
            pl.BlockSpec((n_tok, n_exp), lambda s: (0, 0)),
            pl.BlockSpec((n_exp, model_dim), lambda s: (0, 0)),
            pl.BlockSpec((step_cols, model_dim), lambda s: (s, 0)),
            pl.BlockSpec((step_cols, model_dim), lambda s: (s, 0)),
            pl.BlockSpec((step_cols, model_dim), lambda s: (s, 0)),
        ],
        out_specs=pl.BlockSpec((n_tok, model_dim), lambda s: (0, 0)),
        out_shape=jax.ShapeDtypeStruct((n_tok, model_dim), jnp.bfloat16),
        scratch_shapes=[pltpu.VMEM((n_tok, model_dim), jnp.float32), pltpu.VMEM((n_exp // EXP_PER_STEP, n_tok, EXP_PER_STEP), jnp.float32)],
        compiler_params=pltpu.CompilerParams(dimension_semantics=("arbitrary",), vmem_limit_bytes=56 * 1024 * 1024),
        cost_estimate=pl.CostEstimate(flops=flops, bytes_accessed=3 * n_ff * model_dim * 2, transcendentals=n_tok * n_ff),
        name="dense_moe",
    )(m_rows, mask, wr_t, wg_t, wu_t, w_dn)


def solution(mesh):
    tp_size = mesh.shape["tp"]
    in_specs = (P("dp", None), P("dp", None, None), P("tp", None), P(None), P(None, "tp"), P(None, "tp"), P(None, "tp"), P("tp", None), P("tp"), P("tp"), P(None), P(None, None), P(None, None, "tp"), P(None, None, "tp"), P(None, "tp", None))

    def device_fn(token_ids, route_idx, embed_table, attn_norm, w_query, w_key, w_value, w_out, q_gain, k_gain, mlp_norm, w_router, w_gate, w_up, w_down):
        batch_loc, seq_len = token_ids.shape
        vocab_loc, model_dim = embed_table.shape
        tp_rank = lax.axis_index("tp")
        local_ids = token_ids - tp_rank * vocab_loc
        in_range = (local_ids >= 0) & (local_ids < vocab_loc)
        looked_up = jnp.take(embed_table, jnp.clip(local_ids, 0, vocab_loc - 1), axis=0)
        embed_part = jnp.where(in_range[..., None], looked_up, jnp.zeros((), jnp.bfloat16))
        x_embed = lax.psum_scatter(embed_part, "tp", scatter_dimension=1, tiled=True)

        a_loc = rms_scale(x_embed, attn_norm).astype(jnp.bfloat16)
        normed = lax.all_gather(a_loc, "tp", axis=1, tiled=True)
        q_raw = jnp.einsum("bsd,dq->bsq", normed, w_query, preferred_element_type=jnp.float32)
        k_raw = jnp.einsum("bsd,dq->bsq", normed, w_key, preferred_element_type=jnp.float32)
        heads_loc = w_query.shape[1] // HEAD_DIM
        head_shape = (batch_loc, seq_len, heads_loc, HEAD_DIM)
        v_heads = jnp.einsum("bsd,dq->bsq", normed, w_value, preferred_element_type=jnp.float32).astype(jnp.bfloat16).reshape(head_shape)
        sq_sums = jnp.stack([jnp.sum(q_raw * q_raw, axis=-1), jnp.sum(k_raw * k_raw, axis=-1)])
        sq_total = lax.psum(sq_sums, "tp")
        inv_rms = lax.rsqrt(sq_total / (w_query.shape[1] * tp_size) + NORM_EPS)
        cos_tab, sin_tab = rope_tables(seq_len)
        q_heads = apply_rope((q_raw * inv_rms[0][..., None] * q_gain.astype(jnp.float32)).reshape(head_shape), cos_tab, sin_tab)
        k_heads = apply_rope((k_raw * inv_rms[1][..., None] * k_gain.astype(jnp.float32)).reshape(head_shape), cos_tab, sin_tab)
        scores = jnp.einsum("bqhd,bkhd->bhqk", q_heads, k_heads, preferred_element_type=jnp.float32) * (HEAD_DIM ** -0.5)
        positions = jnp.arange(seq_len)
        scores = jnp.where(positions[:, None] >= positions[None, :], scores, -1e30)
        attn_prob = jax.nn.softmax(scores, axis=-1).astype(jnp.bfloat16)
        context = jnp.einsum("bhqk,bkhd->bqhd", attn_prob, v_heads, preferred_element_type=jnp.float32).astype(jnp.bfloat16)
        attn_part = jnp.einsum("bqhd,hde->bqe", context, w_out.reshape(heads_loc, HEAD_DIM, model_dim), preferred_element_type=jnp.float32).astype(jnp.bfloat16)
        attn_out = lax.psum_scatter(attn_part, "tp", scatter_dimension=1, tiled=True)
        hidden = (x_embed.astype(jnp.float32) + attn_out.astype(jnp.float32)).astype(jnp.bfloat16)

        m_loc = rms_scale(hidden, mlp_norm).astype(jnp.bfloat16).reshape(batch_loc * seq_len // tp_size, model_dim)
        n_exp = w_gate.shape[0]
        wg_t = jnp.swapaxes(w_gate, 1, 2).reshape(-1, model_dim)
        wu_t = jnp.swapaxes(w_up, 1, 2).reshape(-1, model_dim)
        w_dn = w_down.reshape(-1, model_dim)
        wr_t = w_router.T
        expert_iota = jnp.arange(n_exp, dtype=jnp.int32)
        chosen = route_idx.reshape(batch_loc * seq_len, -1)
        mask = jnp.any(chosen[:, :, None] == expert_iota[None, None, :], axis=1).astype(jnp.float32)
        rows_loc = m_loc.shape[0]
        rows_chunk = rows_loc // N_CHUNKS
        mask = mask.reshape(tp_size, N_CHUNKS, rows_chunk, n_exp)
        moe_parts = []
        for chunk in range(N_CHUNKS):
            m_chunk = lax.all_gather(m_loc[chunk * rows_chunk:(chunk + 1) * rows_chunk], "tp", axis=0, tiled=True)
            mask_chunk = mask[:, chunk].reshape(tp_size * rows_chunk, n_exp)
            part = dense_moe(m_chunk, mask_chunk, wr_t, wg_t, wu_t, w_dn)
            moe_parts.append(lax.psum_scatter(part, "tp", scatter_dimension=0, tiled=True))
        moe_out = jnp.concatenate(moe_parts, axis=0).reshape(hidden.shape)
        return (hidden.astype(jnp.float32) + moe_out.astype(jnp.float32)).astype(jnp.bfloat16)

    return jax.shard_map(device_fn, mesh=mesh, in_specs=in_specs, out_specs=P("dp", "tp", None), check_vma=False)
```

```python
import functools

import jax
import jax.numpy as jnp
from jax import lax
from jax.experimental import pallas as pl
from jax.experimental.pallas import tpu as pltpu
from jax.sharding import PartitionSpec as P

HEAD_DIM = 128
NORM_EPS = 1e-5
N_CHUNKS = 4
EXP_PER_STEP = 8
VMEM_LIMIT = 63 * 1024 * 1024


def rms_scale(act_in, norm_gain):
    act_f32 = act_in.astype(jnp.float32)
    mean_sq = jnp.mean(act_f32 * act_f32, axis=-1, keepdims=True)
    return act_f32 * lax.rsqrt(mean_sq + NORM_EPS) * norm_gain.astype(jnp.float32)


def rope_tables(seq_len):
    half_dim = HEAD_DIM // 2
    inv_freq = 1.0 / (10000.0 ** (jnp.arange(half_dim, dtype=jnp.float32) * (2.0 / HEAD_DIM)))
    angles = jnp.arange(seq_len, dtype=jnp.float32)[:, None] * inv_freq[None, :]
    return jnp.cos(angles), jnp.sin(angles)


def apply_rope(heads_f32, cos_tab, sin_tab):
    half_dim = HEAD_DIM // 2
    first_half = heads_f32[..., :half_dim]
    second_half = heads_f32[..., half_dim:]
    cos_b = cos_tab[:, None, :]
    sin_b = sin_tab[:, None, :]
    rotated = jnp.concatenate([first_half * cos_b - second_half * sin_b, second_half * cos_b + first_half * sin_b], axis=-1)
    return rotated.astype(jnp.bfloat16)


ROW_TILE = 256
N_STAGES = 6
N_Z, N_Y = 4, 2
MESH = pl.DeviceIdType.MESH


class Place:
    def __init__(self):
        self.me = lax.axis_index("tp")
        self.z = self.me // 4
        self.y = self.me % 4 // 2
        self.c = self.me % 2
        self.core_peer = self.me + 1 - 2 * self.c
        self.y_peer = self.me + 2 - 4 * self.y
        self.up = self.me + 4
        self.down = self.me - 4

    def index(self, zz, yy, cc):
        return zz * 4 + yy * 2 + cc


def remote(src, dst, send_sem, recv_sem, device):
    return pltpu.make_async_remote_copy(src_ref=src, dst_ref=dst, send_sem=send_sem, recv_sem=recv_sem, device_id={"tp": device}, device_id_type=MESH)


def entry_barrier(place):
    barrier = pltpu.get_barrier_semaphore()
    for peer in (place.core_peer, place.y_peer):
        pl.semaphore_signal(barrier, inc=1, device_id={"tp": peer}, device_id_type=MESH)

    @pl.when(place.z > 0)
    def _():
        pl.semaphore_signal(barrier, inc=1, device_id={"tp": place.down}, device_id_type=MESH)

    @pl.when(place.z < N_Z - 1)
    def _():
        pl.semaphore_signal(barrier, inc=1, device_id={"tp": place.up}, device_id_type=MESH)

    pl.semaphore_wait(barrier, 2 + (place.z + 3) // 4 + (6 - place.z) // 4)


def by_distance(place, dist, act):
    if dist == 0:
        act(place.z)
        return

    @pl.when(place.z + dist < N_Z)
    def _():
        act(place.z + dist)

    @pl.when(place.z >= dist)
    def _():
        act(place.z - dist)


class Gather:
    SEMS = [(4,), (4,), (4,), (4,), (4,), (8,), (8,)]

    def __init__(self, place, own, shard, sems):
        self.place, self.own, self.shard = place, own, shard
        self.up_send, self.down_send, self.z_recv, self.y_send, self.y_recv, self.c_send, self.c_recv = sems

    def src(self, d, k, mine):
        return self.own(k) if mine else self.shard(d, k)

    def to_up(self, zz, k, mine=False):
        d = self.place.index(zz, self.place.y, self.place.c)
        return remote(self.src(d, k, mine), self.shard(d, k), self.up_send.at[k, zz], self.z_recv.at[k, zz], self.place.up)

    def to_down(self, zz, k, mine=False):
        d = self.place.index(zz, self.place.y, self.place.c)
        return remote(self.src(d, k, mine), self.shard(d, k), self.down_send.at[k, zz], self.z_recv.at[k, zz], self.place.down)

    def to_y(self, zz, k, mine=False, flip=False):
        d = self.place.index(zz, 1 - self.place.y if flip else self.place.y, self.place.c)
        return remote(self.src(d, k, mine), self.shard(d, k), self.y_send.at[k, zz], self.y_recv.at[k, zz], self.place.y_peer)

    def to_core(self, zz, yy, k, mine=False, flip=False):
        d = self.place.index(zz, yy, 1 - self.place.c if flip else self.place.c)
        slot = zz * 2 + yy
        return remote(self.src(d, k, mine), self.shard(d, k), self.c_send.at[k, slot], self.c_recv.at[k, slot], self.place.core_peer)

    def stage(self, number, k):
        place = self.place
        z, y = place.z, place.y
        if number == 0:
            @pl.when(z < N_Z - 1)
            def _():
                self.to_up(z, k, True).start()

            @pl.when(z > 0)
            def _():
                self.to_down(z, k, True).start()

            self.to_y(z, k, True).start()
            self.to_core(z, y, k, True).start()
        elif number < N_Z:
            @pl.when(z >= number)
            def _():
                zz = z - number
                self.to_up(zz, k).wait_recv()

                @pl.when(z < N_Z - 1)
                def _():
                    self.to_up(zz, k).start()

                self.to_y(zz, k).start()
                self.to_core(zz, y, k).start()

            @pl.when(z + number < N_Z)
            def _():
                zz = z + number
                self.to_down(zz, k).wait_recv()

                @pl.when(z > 0)
                def _():
                    self.to_down(zz, k).start()

                self.to_y(zz, k).start()
                self.to_core(zz, y, k).start()
        if 1 <= number <= N_Z:
            def pass_on(zz):
                self.to_y(zz, k, flip=True).wait_recv()
                self.to_core(zz, 1 - y, k).start()

            by_distance(place, number - 1, pass_on)
        if number == N_STAGES - 1:
            for zz in range(N_Z):
                for yy in range(N_Y):
                    self.to_core(zz, yy, k, flip=True).wait_recv()

    def drain(self, k):
        z = self.place.z
        for zz in range(N_Z):
            @pl.when((z >= zz) & (z < N_Z - 1))
            def _():
                self.to_up(zz, k).wait_send()

            @pl.when((z <= zz) & (z > 0))
            def _():
                self.to_down(zz, k).wait_send()

            self.to_y(zz, k).wait_send()
            for yy in range(N_Y):
                self.to_core(zz, yy, k).wait_send()


class Scatter:
    SEMS = [(8,), (8,), (4,), (4,), (4,), (4,), (4,), (4,)]
    BUFS = (8, 4, 4, 4, 4, 4)

    def __init__(self, place, shard, bufs, total, sems):
        self.place, self.shard, self.total = place, shard, total
        self.c_buf, self.y_out, self.y_in, self.z_out, self.from_down, self.from_up = bufs
        self.c_send, self.c_recv, self.y_send, self.y_recv, self.up_send, self.up_recv, self.down_send, self.down_recv = sems

    def to_core(self, zz, yy, k):
        slot = zz * 2 + yy
        d = self.place.index(zz, yy, 1 - self.place.c)
        return remote(self.shard(d, k), self.c_buf.at[k, slot], self.c_send.at[k, slot], self.c_recv.at[k, slot], self.place.core_peer)

    def to_y(self, zz, k):
        return remote(self.y_out.at[k, zz], self.y_in.at[k, zz], self.y_send.at[k, zz], self.y_recv.at[k, zz], self.place.y_peer)

    def to_up(self, zz, k):
        return remote(self.z_out.at[k, zz], self.from_down.at[k, zz], self.up_send.at[k, zz], self.up_recv.at[k, zz], self.place.up)

    def to_down(self, zz, k):
        return remote(self.z_out.at[k, zz], self.from_up.at[k, zz], self.down_send.at[k, zz], self.down_recv.at[k, zz], self.place.down)

    def pair_sum(self, zz, yy, k):
        self.to_core(zz, yy, k).wait_recv()
        mine = self.shard(self.place.index(zz, yy, self.place.c), k)[...].astype(jnp.float32)
        return mine + self.c_buf[k, zz * 2 + yy].astype(jnp.float32)

    def chip_pair_sum(self, zz, k):
        both = self.pair_sum(zz, self.place.y, k)
        self.to_y(zz, k).wait_recv()
        return both + self.y_in[k, zz].astype(jnp.float32)

    def stage(self, number, k):
        place = self.place
        z, y = place.z, place.y
        if number == 0:
            for yy in (1 - y, y):
                for zz in range(N_Z):
                    self.to_core(zz, yy, k).start()
        elif number == 1:
            def send_y(zz):
                self.y_out[k, zz] = self.pair_sum(zz, 1 - y, k).astype(jnp.bfloat16)
                self.to_y(zz, k).start()

            for dist in (3, 2, 1, 0):
                by_distance(place, dist, send_y)
        elif number < N_STAGES - 1:
            dist = N_STAGES - 1 - number

            @pl.when(z + dist < N_Z)
            def _():
                zz = z + dist
                self.total[...] = self.chip_pair_sum(zz, k)

                @pl.when(z > 0)
                def _():
                    self.to_up(zz, k).wait_recv()
                    self.total[...] += self.from_down[k, zz].astype(jnp.float32)

                self.z_out[k, zz] = self.total[...].astype(jnp.bfloat16)
                self.to_up(zz, k).start()

            @pl.when(z >= dist)
            def _():
                zz = z - dist
                self.total[...] = self.chip_pair_sum(zz, k)

                @pl.when(z < N_Z - 1)
                def _():
                    self.to_down(zz, k).wait_recv()
                    self.total[...] += self.from_up[k, zz].astype(jnp.float32)

                self.z_out[k, zz] = self.total[...].astype(jnp.bfloat16)
                self.to_down(zz, k).start()
        else:
            self.total[...] = self.chip_pair_sum(z, k)

            @pl.when(z > 0)
            def _():
                self.to_up(z, k).wait_recv()
                self.total[...] += self.from_down[k, z].astype(jnp.float32)

            @pl.when(z < N_Z - 1)
            def _():
                self.to_down(z, k).wait_recv()
                self.total[...] += self.from_up[k, z].astype(jnp.float32)

    def drain(self, k):
        z = self.place.z
        for zz in range(N_Z):
            for yy in range(N_Y):
                self.to_core(zz, yy, k).wait_send()
            self.to_y(zz, k).wait_send()

            @pl.when(z < zz)
            def _():
                self.to_up(zz, k).wait_send()

            @pl.when(z > zz)
            def _():
                self.to_down(zz, k).wait_send()


def chunk_sems(kind, n_chunks):
    return [pltpu.SemaphoreType.DMA((n_chunks,) + shape) for shape in kind.SEMS]


def chunk_bufs(n_chunks, rows, width):
    return [pltpu.VMEM((n_chunks, slots, rows, width), jnp.bfloat16) for slots in Scatter.BUFS]


def norm_rows(rows_f32, gain_f32):
    mean_sq = jnp.mean(rows_f32 * rows_f32, axis=-1, keepdims=True)
    return (rows_f32 * lax.rsqrt(mean_sq + NORM_EPS) * gain_f32).astype(jnp.bfloat16)


def scatter_kernel(n_chunks, with_residual, *refs):
    n_in = 3 if with_residual else 2
    part, gain = refs[0], refs[1]
    residual = refs[2] if with_residual else None
    sum_ref, norm_ref = refs[n_in:n_in + 2]
    scratch = refs[n_in + 2:]
    total = scratch[0]
    bufs, sems = scratch[1:7], scratch[7:]
    rows = total.shape[0]
    place = Place()
    scat = Scatter(place, lambda d, k: part.at[d, pl.ds(pl.multiple_of(k * rows, rows), rows), :], bufs, total, sems)
    entry_barrier(place)

    def first(k, carry):
        scat.stage(0, k)
        return carry

    def second(k, carry):
        scat.stage(1, k)
        return carry

    def finish(k):
        out_rows = pl.ds(pl.multiple_of(k * rows, rows), rows)
        value = total[...].astype(jnp.bfloat16)
        if residual is not None:
            value = (residual[out_rows, :].astype(jnp.float32) + value.astype(jnp.float32)).astype(jnp.bfloat16)
        sum_ref[out_rows, :] = value
        norm_ref[out_rows, :] = norm_rows(value.astype(jnp.float32), gain[...].astype(jnp.float32))

    def wave(t, carry):
        for number in range(N_STAGES - 1, 1, -1):
            k = t - (number - 2)

            @pl.when((k >= 0) & (k < n_chunks))
            def _():
                scat.stage(number, k)
                if number == N_STAGES - 1:
                    finish(k)
        return carry

    def drain(k, carry):
        scat.drain(k)
        return carry

    lax.fori_loop(0, n_chunks, first, 0)
    lax.fori_loop(0, n_chunks, second, 0)
    lax.fori_loop(0, n_chunks + N_STAGES - 3, wave, 0)
    lax.fori_loop(0, n_chunks, drain, 0)


def scatter_rows(part, gain, residual, collective_id):
    n_dev = N_Z * N_Y * 2
    width = part.shape[-1]
    rows_loc = part.shape[0] // n_dev
    rows = rows_loc // N_CHUNKS
    operands = [part.reshape(n_dev, rows_loc, width), gain.reshape(1, width)]
    if residual is not None:
        operands.append(residual)
    out = jax.ShapeDtypeStruct((rows_loc, width), jnp.bfloat16)
    return pl.pallas_call(
        functools.partial(scatter_kernel, N_CHUNKS, residual is not None),
        in_specs=[pl.BlockSpec(memory_space=pltpu.VMEM)] * len(operands),
        out_specs=[pl.BlockSpec(memory_space=pltpu.VMEM)] * 2,
        out_shape=[out, out],
        scratch_shapes=[pltpu.VMEM((rows, width), jnp.float32)] + chunk_bufs(N_CHUNKS, rows, width) + chunk_sems(Scatter, N_CHUNKS),
        compiler_params=pltpu.CompilerParams(collective_id=collective_id, has_side_effects=True, vmem_limit_bytes=VMEM_LIMIT),
        name="scatter_rows",
    )(*operands)


def gather_kernel(n_chunks, own_ref, out_ref, full, copy_sem, *sems):
    rows = own_ref.shape[0] // n_chunks
    place = Place()
    chunk_rows = lambda k: pl.ds(pl.multiple_of(k * rows, rows), rows)
    gath = Gather(place, lambda k: own_ref.at[chunk_rows(k), :], lambda d, k: full.at[d, chunk_rows(k), :], sems)
    entry_barrier(place)

    def put(k):
        return pltpu.make_async_copy(full.at[:, chunk_rows(k), :], out_ref.at[:, chunk_rows(k), :], copy_sem.at[k])

    def first(k, carry):
        gath.stage(0, k)
        full[place.me, chunk_rows(k), :] = own_ref[chunk_rows(k), :]
        return carry

    def wave(t, carry):
        for number in range(N_STAGES - 1, 0, -1):
            k = t - (number - 1)

            @pl.when((k >= 0) & (k < n_chunks))
            def _():
                gath.stage(number, k)
                if number == N_STAGES - 1:
                    put(k).start()
        return carry

    def drain(k, carry):
        gath.drain(k)
        put(k).wait()
        return carry

    lax.fori_loop(0, n_chunks, first, 0)
    lax.fori_loop(0, n_chunks + N_STAGES - 2, wave, 0)
    lax.fori_loop(0, n_chunks, drain, 0)


def gather_rows(own, collective_id):
    n_dev = N_Z * N_Y * 2
    rows_loc, width = own.shape
    full = pl.pallas_call(
        functools.partial(gather_kernel, N_CHUNKS),
        in_specs=[pl.BlockSpec(memory_space=pltpu.VMEM)],
        out_specs=pl.BlockSpec(memory_space=pl.ANY),
        out_shape=jax.ShapeDtypeStruct((n_dev, rows_loc, width), jnp.bfloat16),
        scratch_shapes=[pltpu.VMEM((n_dev, rows_loc, width), jnp.bfloat16), pltpu.SemaphoreType.DMA((N_CHUNKS,))] + chunk_sems(Gather, N_CHUNKS),
        compiler_params=pltpu.CompilerParams(collective_id=collective_id, has_side_effects=True, vmem_limit_bytes=VMEM_LIMIT),
        name="gather_rows",
    )(own)
    return full.reshape(n_dev * rows_loc, width)


def group_sum_kernel(x_ref, out_ref, slots, send_sem, recv_sem):
    n_dev = slots.shape[0]
    me = lax.axis_index("tp")
    barrier = pltpu.get_barrier_semaphore()
    for off in range(1, n_dev):
        pl.semaphore_signal(barrier, inc=1, device_id={"tp": (me + off) % n_dev}, device_id_type=MESH)
    pl.semaphore_wait(barrier, n_dev - 1)
    for off in range(1, n_dev):
        remote(x_ref, slots.at[me], send_sem.at[off], recv_sem.at[me], (me + off) % n_dev).start()
    slots[me] = x_ref[...]
    for off in range(1, n_dev):
        other = (me + off) % n_dev
        remote(x_ref, slots.at[other], send_sem.at[off], recv_sem.at[other], other).wait_recv()
    out_ref[...] = jnp.sum(slots[...], axis=0)
    for off in range(1, n_dev):
        remote(x_ref, slots.at[me], send_sem.at[off], recv_sem.at[me], (me + off) % n_dev).wait_send()


def group_sum(x, n_dev, collective_id):
    return pl.pallas_call(
        group_sum_kernel,
        in_specs=[pl.BlockSpec(memory_space=pltpu.VMEM)],
        out_specs=pl.BlockSpec(memory_space=pltpu.VMEM),
        out_shape=jax.ShapeDtypeStruct(x.shape, x.dtype),
        scratch_shapes=[pltpu.VMEM((n_dev,) + x.shape, x.dtype), pltpu.SemaphoreType.DMA((n_dev,)), pltpu.SemaphoreType.DMA((n_dev,))],
        compiler_params=pltpu.CompilerParams(collective_id=collective_id, has_side_effects=True),
        name="group_sum",
    )(x)


def moe_kernel(n_chunks, exp_step, own_ref, hid_ref, mask_ref, wr_ref, wg_ref, wu_ref, wd_ref, out_ref, acc_ref, gate_ref, full, part, total, *rest):
    bufs, rest = rest[:6], rest[6:]
    gather_sems, scatter_sems = rest[:len(Gather.SEMS)], rest[len(Gather.SEMS):]
    chunk, step = pl.program_id(0), pl.program_id(1)
    n_steps = pl.num_programs(1)
    rows = own_ref.shape[0] // n_chunks
    n_tok = full.shape[1]
    n_exp = wr_ref.shape[0]
    exp_ff = wg_ref.shape[0] // exp_step
    nt_dims = (((1,), (1,)), ((), ()))
    place = Place()
    loc_rows = lambda k: pl.ds(pl.multiple_of(k * rows, rows), rows)
    block = lambda ref: (lambda d, k: ref.at[k, pl.ds(pl.multiple_of(d * rows, rows), rows), :])
    gath = Gather(place, lambda k: own_ref.at[loc_rows(k), :], block(full), gather_sems)
    scat = Scatter(place, block(part), bufs, total, scatter_sems)

    def finish(k):
        moe_out = total[...].astype(jnp.bfloat16).astype(jnp.float32)
        out_ref[loc_rows(k), :] = (hid_ref[loc_rows(k), :].astype(jnp.float32) + moe_out).astype(jnp.bfloat16)

    @pl.when((chunk == 0) & (step == 0))
    def _():
        entry_barrier(place)
        for k in range(n_chunks):
            full[k, pl.ds(pl.multiple_of(place.me * rows, rows), rows), :] = own_ref[k * rows:(k + 1) * rows, :]
        for number in range(N_STAGES):
            gath.stage(number, 0)

    for number in range(N_STAGES):
        @pl.when((step == number) & (chunk + 1 < n_chunks))
        def _():
            gath.stage(number, chunk + 1)

        @pl.when((step == number) & (chunk > 0))
        def _():
            scat.stage(number, chunk - 1)
            if number == N_STAGES - 1:
                finish(chunk - 1)

    @pl.when(step == 0)
    def _():
        logits = lax.dot_general(full[chunk], wr_ref[...], nt_dims, preferred_element_type=jnp.float32)
        logits = logits - jnp.max(logits, axis=-1, keepdims=True)
        expd = jnp.exp(logits)
        gates = expd / jnp.sum(expd, axis=-1, keepdims=True) * mask_ref[0]
        for grp in range(n_exp // exp_step):
            gate_ref[grp] = gates[:, grp * exp_step:(grp + 1) * exp_step]
        acc_ref[...] = jnp.zeros_like(acc_ref)

    def row_body(i, carry):
        tile = pl.ds(pl.multiple_of(i * ROW_TILE, ROW_TILE), ROW_TILE)
        m_tile = full[chunk, tile, :]
        gate_proj = lax.dot_general(m_tile, wg_ref[...], nt_dims, preferred_element_type=jnp.float32)
        up_proj = lax.dot_general(m_tile, wu_ref[...], nt_dims, preferred_element_type=jnp.float32)
        act = (gate_proj / (1.0 + jnp.exp(-gate_proj)) * up_proj).astype(jnp.bfloat16).astype(jnp.float32)
        gates = gate_ref[step, tile, :]
        lane = lax.broadcasted_iota(jnp.int32, (ROW_TILE, 2 * exp_ff), 1)
        pieces = []
        for pair in range(exp_step // 2):
            pieces.append(jnp.where(lane < exp_ff, gates[:, 2 * pair:2 * pair + 1], gates[:, 2 * pair + 1:2 * pair + 2]))
        scaled = act * jnp.concatenate(pieces, axis=1)
        high = scaled.astype(jnp.bfloat16)
        low = (scaled - high.astype(jnp.float32)).astype(jnp.bfloat16)
        down = jnp.dot(high, wd_ref[...], preferred_element_type=jnp.float32) + jnp.dot(low, wd_ref[...], preferred_element_type=jnp.float32)
        acc_ref[tile, :] += down
        return carry

    lax.fori_loop(0, n_tok // ROW_TILE, row_body, 0)

    @pl.when(step == n_steps - 1)
    def _():
        part[chunk] = acc_ref[...].astype(jnp.bfloat16)

    @pl.when((step == n_steps - 1) & (chunk == n_chunks - 1))
    def _():
        for number in range(N_STAGES):
            scat.stage(number, n_chunks - 1)
        finish(n_chunks - 1)

        def drain(k, carry):
            gath.drain(k)
            scat.drain(k)
            return carry

        lax.fori_loop(0, n_chunks, drain, 0)


def moe_layer(own, hidden, mask, wr_t, wg_t, wu_t, w_dn, collective_id):
    rows_loc, width = own.shape
    n_chunks, n_tok, n_exp = mask.shape
    n_ff = wg_t.shape[0]
    step_cols = n_ff // n_exp * EXP_PER_STEP
    rows = rows_loc // n_chunks
    const = lambda k, s: (0, 0)
    return pl.pallas_call(
        functools.partial(moe_kernel, n_chunks, EXP_PER_STEP),
        grid=(n_chunks, n_ff // step_cols),
        in_specs=[
            pl.BlockSpec((rows_loc, width), const),
            pl.BlockSpec((rows_loc, width), const),
            pl.BlockSpec((1, n_tok, n_exp), lambda k, s: (k, 0, 0)),
            pl.BlockSpec((n_exp, width), const),
            pl.BlockSpec((step_cols, width), lambda k, s: (s, 0)),
            pl.BlockSpec((step_cols, width), lambda k, s: (s, 0)),
            pl.BlockSpec((step_cols, width), lambda k, s: (s, 0)),
        ],
        out_specs=pl.BlockSpec((rows_loc, width), const),
        out_shape=jax.ShapeDtypeStruct((rows_loc, width), jnp.bfloat16),
        scratch_shapes=[
            pltpu.VMEM((n_tok, width), jnp.float32),
            pltpu.VMEM((n_exp // EXP_PER_STEP, n_tok, EXP_PER_STEP), jnp.float32),
            pltpu.VMEM((n_chunks, n_tok, width), jnp.bfloat16),
            pltpu.VMEM((n_chunks, n_tok, width), jnp.bfloat16),
            pltpu.VMEM((rows, width), jnp.float32),
        ] + chunk_bufs(n_chunks, rows, width) + chunk_sems(Gather, n_chunks) + chunk_sems(Scatter, n_chunks),
        compiler_params=pltpu.CompilerParams(dimension_semantics=("arbitrary", "arbitrary"), collective_id=collective_id, has_side_effects=True, vmem_limit_bytes=VMEM_LIMIT),
        name="moe_layer",
    )(own, hidden, mask, wr_t, wg_t, wu_t, w_dn)


def solution(mesh):
    tp_size = mesh.shape["tp"]
    in_specs = (P("dp", None), P("dp", None, None), P("tp", None), P(None), P(None, "tp"), P(None, "tp"), P(None, "tp"), P("tp", None), P("tp"), P("tp"), P(None), P(None, None), P(None, None, "tp"), P(None, None, "tp"), P(None, "tp", None))

    def device_fn(token_ids, route_idx, embed_table, attn_norm, w_query, w_key, w_value, w_out, q_gain, k_gain, mlp_norm, w_router, w_gate, w_up, w_down):
        batch_loc, seq_len = token_ids.shape
        vocab_loc, model_dim = embed_table.shape
        tp_rank = lax.axis_index("tp")
        local_ids = token_ids - tp_rank * vocab_loc
        in_range = (local_ids >= 0) & (local_ids < vocab_loc)
        looked_up = jnp.take(embed_table, jnp.clip(local_ids, 0, vocab_loc - 1), axis=0)
        embed_part = jnp.where(in_range[..., None], looked_up, jnp.zeros((), jnp.bfloat16))
        x_loc, a_loc = scatter_rows(embed_part.reshape(-1, model_dim), attn_norm, None, 0)
        normed = gather_rows(a_loc, 1).reshape(batch_loc, seq_len, model_dim)
        q_raw = jnp.einsum("bsd,dq->bsq", normed, w_query, preferred_element_type=jnp.float32)
        k_raw = jnp.einsum("bsd,dq->bsq", normed, w_key, preferred_element_type=jnp.float32)
        heads_loc = w_query.shape[1] // HEAD_DIM
        head_shape = (batch_loc, seq_len, heads_loc, HEAD_DIM)
        v_heads = jnp.einsum("bsd,dq->bsq", normed, w_value, preferred_element_type=jnp.float32).astype(jnp.bfloat16).reshape(head_shape)
        sq_sums = jnp.stack([jnp.sum(q_raw * q_raw, axis=-1), jnp.sum(k_raw * k_raw, axis=-1)])
        sq_total = group_sum(sq_sums.reshape(2, -1), tp_size, 2).reshape(sq_sums.shape)
        inv_rms = lax.rsqrt(sq_total / (w_query.shape[1] * tp_size) + NORM_EPS)
        cos_tab, sin_tab = rope_tables(seq_len)
        q_heads = apply_rope((q_raw * inv_rms[0][..., None] * q_gain.astype(jnp.float32)).reshape(head_shape), cos_tab, sin_tab)
        k_heads = apply_rope((k_raw * inv_rms[1][..., None] * k_gain.astype(jnp.float32)).reshape(head_shape), cos_tab, sin_tab)
        scores = jnp.einsum("bqhd,bkhd->bhqk", q_heads, k_heads, preferred_element_type=jnp.float32) * (HEAD_DIM ** -0.5)
        positions = jnp.arange(seq_len)
        scores = jnp.where(positions[:, None] >= positions[None, :], scores, -1e30)
        attn_prob = jax.nn.softmax(scores, axis=-1).astype(jnp.bfloat16)
        context = jnp.einsum("bhqk,bkhd->bqhd", attn_prob, v_heads, preferred_element_type=jnp.float32).astype(jnp.bfloat16)
        attn_part = jnp.einsum("bqhd,hde->bqe", context, w_out.reshape(heads_loc, HEAD_DIM, model_dim), preferred_element_type=jnp.float32).astype(jnp.bfloat16)
        h_loc, m_loc = scatter_rows(attn_part.reshape(-1, model_dim), mlp_norm, x_loc, 3)
        n_exp = w_gate.shape[0]
        wg_t = jnp.swapaxes(w_gate, 1, 2).reshape(-1, model_dim)
        wu_t = jnp.swapaxes(w_up, 1, 2).reshape(-1, model_dim)
        w_dn = w_down.reshape(-1, model_dim)
        wr_t = w_router.T
        expert_iota = jnp.arange(n_exp, dtype=jnp.int32)
        chosen = route_idx.reshape(batch_loc * seq_len, -1)
        mask = jnp.any(chosen[:, :, None] == expert_iota[None, None, :], axis=1).astype(jnp.float32)
        rows_chunk = m_loc.shape[0] // N_CHUNKS
        mask = mask.reshape(tp_size, N_CHUNKS, rows_chunk, n_exp).swapaxes(0, 1).reshape(N_CHUNKS, tp_size * rows_chunk, n_exp)
        out_loc = moe_layer(m_loc, h_loc, mask, wr_t, wg_t, wu_t, w_dn, 4)
        return out_loc.reshape(batch_loc, -1, model_dim)

    return jax.shard_map(device_fn, mesh=mesh, in_specs=in_specs, out_specs=P("dp", "tp", None), check_vma=False)
```

```python
import functools

import jax
import jax.numpy as jnp
from jax import lax
from jax.experimental import pallas as pl
from jax.experimental.pallas import tpu as pltpu
from jax.sharding import PartitionSpec as P

HEAD_DIM = 128
NORM_EPS = 1e-5
N_CHUNKS = 4
EXP_PER_STEP = 8
VMEM_LIMIT = 63 * 1024 * 1024


def rms_scale(act_in, norm_gain):
    act_f32 = act_in.astype(jnp.float32)
    mean_sq = jnp.mean(act_f32 * act_f32, axis=-1, keepdims=True)
    return act_f32 * lax.rsqrt(mean_sq + NORM_EPS) * norm_gain.astype(jnp.float32)


def rope_tables(seq_len):
    half_dim = HEAD_DIM // 2
    inv_freq = 1.0 / (10000.0 ** (jnp.arange(half_dim, dtype=jnp.float32) * (2.0 / HEAD_DIM)))
    angles = jnp.arange(seq_len, dtype=jnp.float32)[:, None] * inv_freq[None, :]
    return jnp.cos(angles), jnp.sin(angles)


def apply_rope(heads_f32, cos_tab, sin_tab):
    half_dim = HEAD_DIM // 2
    first_half = heads_f32[..., :half_dim]
    second_half = heads_f32[..., half_dim:]
    cos_b = cos_tab[:, None, :]
    sin_b = sin_tab[:, None, :]
    rotated = jnp.concatenate([first_half * cos_b - second_half * sin_b, second_half * cos_b + first_half * sin_b], axis=-1)
    return rotated.astype(jnp.bfloat16)


N_STAGES = 6
N_Z, N_Y = 4, 2
GATHER_LAST = 8
GATHER_WAVE = ((1, 4), (2, 5), (3, 6), (7,), (8,))
MESH = pl.DeviceIdType.MESH


class Place:
    def __init__(self):
        self.me = lax.axis_index("tp")
        self.z = self.me // 4
        self.y = self.me % 4 // 2
        self.c = self.me % 2
        self.core_peer = self.me + 1 - 2 * self.c
        self.y_peer = self.me + 2 - 4 * self.y
        self.up = self.me + 4
        self.down = self.me - 4

    def index(self, zz, yy, cc):
        return zz * 4 + yy * 2 + cc


def remote(src, dst, send_sem, recv_sem, device):
    return pltpu.make_async_remote_copy(src_ref=src, dst_ref=dst, send_sem=send_sem, recv_sem=recv_sem, device_id={"tp": device}, device_id_type=MESH)


def entry_barrier(place):
    barrier = pltpu.get_barrier_semaphore()
    for peer in (place.core_peer, place.y_peer):
        pl.semaphore_signal(barrier, inc=1, device_id={"tp": peer}, device_id_type=MESH)

    @pl.when(place.z > 0)
    def _():
        pl.semaphore_signal(barrier, inc=1, device_id={"tp": place.down}, device_id_type=MESH)

    @pl.when(place.z < N_Z - 1)
    def _():
        pl.semaphore_signal(barrier, inc=1, device_id={"tp": place.up}, device_id_type=MESH)

    pl.semaphore_wait(barrier, 2 + (place.z + 3) // 4 + (6 - place.z) // 4)


def by_distance(place, dist, act):
    if dist == 0:
        act(place.z)
        return

    @pl.when(place.z + dist < N_Z)
    def _():
        act(place.z + dist)

    @pl.when(place.z >= dist)
    def _():
        act(place.z - dist)


class Gather:
    SEMS = [(4,), (4,), (4,), (4,), (4,), (8,), (8,)]

    def __init__(self, place, own, shard, sems):
        self.place, self.own, self.shard = place, own, shard
        self.up_send, self.down_send, self.z_recv, self.y_send, self.y_recv, self.c_send, self.c_recv = sems

    def src(self, d, k, mine):
        return self.own(k) if mine else self.shard(d, k)

    def to_up(self, zz, k, mine=False):
        d = self.place.index(zz, self.place.y, self.place.c)
        return remote(self.src(d, k, mine), self.shard(d, k), self.up_send.at[k, zz], self.z_recv.at[k, zz], self.place.up)

    def to_down(self, zz, k, mine=False):
        d = self.place.index(zz, self.place.y, self.place.c)
        return remote(self.src(d, k, mine), self.shard(d, k), self.down_send.at[k, zz], self.z_recv.at[k, zz], self.place.down)

    def to_y(self, zz, k, mine=False, flip=False):
        d = self.place.index(zz, 1 - self.place.y if flip else self.place.y, self.place.c)
        return remote(self.src(d, k, mine), self.shard(d, k), self.y_send.at[k, zz], self.y_recv.at[k, zz], self.place.y_peer)

    def to_core(self, zz, yy, k, mine=False, flip=False):
        d = self.place.index(zz, yy, 1 - self.place.c if flip else self.place.c)
        slot = zz * 2 + yy
        return remote(self.src(d, k, mine), self.shard(d, k), self.c_send.at[k, slot], self.c_recv.at[k, slot], self.place.core_peer)

    def stage(self, number, k):
        place = self.place
        z, y = place.z, place.y
        if number == 0:
            @pl.when(z < N_Z - 1)
            def _():
                self.to_up(z, k, True).start()

            @pl.when(z > 0)
            def _():
                self.to_down(z, k, True).start()

            self.to_y(z, k, True).start()
            self.to_core(z, y, k, True).start()
        elif number < N_Z:
            @pl.when(z >= number)
            def _():
                zz = z - number
                self.to_up(zz, k).wait_recv()

                @pl.when(z < N_Z - 1)
                def _():
                    self.to_up(zz, k).start()

                self.to_y(zz, k).start()
                self.to_core(zz, y, k).start()

            @pl.when(z + number < N_Z)
            def _():
                zz = z + number
                self.to_down(zz, k).wait_recv()

                @pl.when(z > 0)
                def _():
                    self.to_down(zz, k).start()

                self.to_y(zz, k).start()
                self.to_core(zz, y, k).start()
        elif number < 2 * N_Z:
            def pass_on(zz):
                self.to_y(zz, k, flip=True).wait_recv()
                self.to_core(zz, 1 - y, k).start()

            by_distance(place, number - N_Z, pass_on)
        else:
            for zz in range(N_Z):
                for yy in range(N_Y):
                    self.to_core(zz, yy, k, flip=True).wait_recv()

    def drain(self, k):
        z = self.place.z
        for zz in range(N_Z):
            @pl.when((z >= zz) & (z < N_Z - 1))
            def _():
                self.to_up(zz, k).wait_send()

            @pl.when((z <= zz) & (z > 0))
            def _():
                self.to_down(zz, k).wait_send()

            self.to_y(zz, k).wait_send()
            for yy in range(N_Y):
                self.to_core(zz, yy, k).wait_send()


class Scatter:
    SEMS = [(8,), (8,), (4,), (4,), (4,), (4,), (4,), (4,)]
    BUFS = (8, 4, 4, 4, 4, 4)

    def __init__(self, place, shard, bufs, total, sems):
        self.place, self.shard, self.total = place, shard, total
        self.c_buf, self.y_out, self.y_in, self.z_out, self.from_down, self.from_up = bufs
        self.c_send, self.c_recv, self.y_send, self.y_recv, self.up_send, self.up_recv, self.down_send, self.down_recv = sems

    def to_core(self, zz, yy, k):
        slot = zz * 2 + yy
        d = self.place.index(zz, yy, 1 - self.place.c)
        return remote(self.shard(d, k), self.c_buf.at[k, slot], self.c_send.at[k, slot], self.c_recv.at[k, slot], self.place.core_peer)

    def to_y(self, zz, k):
        return remote(self.y_out.at[k, zz], self.y_in.at[k, zz], self.y_send.at[k, zz], self.y_recv.at[k, zz], self.place.y_peer)

    def to_up(self, zz, k):
        return remote(self.z_out.at[k, zz], self.from_down.at[k, zz], self.up_send.at[k, zz], self.up_recv.at[k, zz], self.place.up)

    def to_down(self, zz, k):
        return remote(self.z_out.at[k, zz], self.from_up.at[k, zz], self.down_send.at[k, zz], self.down_recv.at[k, zz], self.place.down)

    def pair_sum(self, zz, yy, k):
        self.to_core(zz, yy, k).wait_recv()
        mine = self.shard(self.place.index(zz, yy, self.place.c), k)[...].astype(jnp.float32)
        return mine + self.c_buf[k, zz * 2 + yy].astype(jnp.float32)

    def chip_pair_sum(self, zz, k):
        both = self.pair_sum(zz, self.place.y, k)
        self.to_y(zz, k).wait_recv()
        return both + self.y_in[k, zz].astype(jnp.float32)

    def stage(self, number, k):
        place = self.place
        z, y = place.z, place.y
        if number == 0:
            for yy in (1 - y, y):
                for zz in range(N_Z):
                    self.to_core(zz, yy, k).start()
        elif number == 1:
            def send_y(zz):
                self.y_out[k, zz] = self.pair_sum(zz, 1 - y, k).astype(jnp.bfloat16)
                self.to_y(zz, k).start()

            for dist in (3, 2, 1, 0):
                by_distance(place, dist, send_y)
        elif number < N_STAGES - 1:
            dist = N_STAGES - 1 - number

            @pl.when(z + dist < N_Z)
            def _():
                zz = z + dist
                self.total[...] = self.chip_pair_sum(zz, k)

                @pl.when(z > 0)
                def _():
                    self.to_up(zz, k).wait_recv()
                    self.total[...] += self.from_down[k, zz].astype(jnp.float32)

                self.z_out[k, zz] = self.total[...].astype(jnp.bfloat16)
                self.to_up(zz, k).start()

            @pl.when(z >= dist)
            def _():
                zz = z - dist
                self.total[...] = self.chip_pair_sum(zz, k)

                @pl.when(z < N_Z - 1)
                def _():
                    self.to_down(zz, k).wait_recv()
                    self.total[...] += self.from_up[k, zz].astype(jnp.float32)

                self.z_out[k, zz] = self.total[...].astype(jnp.bfloat16)
                self.to_down(zz, k).start()
        else:
            self.total[...] = self.chip_pair_sum(z, k)

            @pl.when(z > 0)
            def _():
                self.to_up(z, k).wait_recv()
                self.total[...] += self.from_down[k, z].astype(jnp.float32)

            @pl.when(z < N_Z - 1)
            def _():
                self.to_down(z, k).wait_recv()
                self.total[...] += self.from_up[k, z].astype(jnp.float32)

    def drain(self, k):
        z = self.place.z
        for zz in range(N_Z):
            for yy in range(N_Y):
                self.to_core(zz, yy, k).wait_send()
            self.to_y(zz, k).wait_send()

            @pl.when(z < zz)
            def _():
                self.to_up(zz, k).wait_send()

            @pl.when(z > zz)
            def _():
                self.to_down(zz, k).wait_send()


def chunk_sems(kind, n_chunks):
    return [pltpu.SemaphoreType.DMA((n_chunks,) + shape) for shape in kind.SEMS]


def chunk_bufs(n_chunks, rows, width):
    return [pltpu.VMEM((n_chunks, slots, rows, width), jnp.bfloat16) for slots in Scatter.BUFS]


def norm_rows(rows_f32, gain_f32):
    mean_sq = jnp.mean(rows_f32 * rows_f32, axis=-1, keepdims=True)
    return (rows_f32 * lax.rsqrt(mean_sq + NORM_EPS) * gain_f32).astype(jnp.bfloat16)


def scatter_kernel(n_chunks, with_residual, *refs):
    n_in = 3 if with_residual else 2
    part, gain = refs[0], refs[1]
    residual = refs[2] if with_residual else None
    sum_ref, norm_ref = refs[n_in:n_in + 2]
    scratch = refs[n_in + 2:]
    total = scratch[0]
    bufs, sems = scratch[1:7], scratch[7:]
    rows = total.shape[0]
    place = Place()
    scat = Scatter(place, lambda d, k: part.at[d, pl.ds(pl.multiple_of(k * rows, rows), rows), :], bufs, total, sems)
    entry_barrier(place)

    def first(k, carry):
        scat.stage(0, k)
        return carry

    def second(k, carry):
        scat.stage(1, k)
        return carry

    def finish(k):
        out_rows = pl.ds(pl.multiple_of(k * rows, rows), rows)
        value = total[...].astype(jnp.bfloat16)
        if residual is not None:
            value = (residual[out_rows, :].astype(jnp.float32) + value.astype(jnp.float32)).astype(jnp.bfloat16)
        sum_ref[out_rows, :] = value
        norm_ref[out_rows, :] = norm_rows(value.astype(jnp.float32), gain[...].astype(jnp.float32))

    def wave(t, carry):
        for number in range(N_STAGES - 1, 1, -1):
            k = t - (number - 2)

            @pl.when((k >= 0) & (k < n_chunks))
            def _():
                scat.stage(number, k)
                if number == N_STAGES - 1:
                    finish(k)
        return carry

    def drain(k, carry):
        scat.drain(k)
        return carry

    lax.fori_loop(0, n_chunks, first, 0)
    lax.fori_loop(0, n_chunks, second, 0)
    lax.fori_loop(0, n_chunks + N_STAGES - 3, wave, 0)
    lax.fori_loop(0, n_chunks, drain, 0)


def scatter_rows(part, gain, residual, collective_id):
    n_dev = N_Z * N_Y * 2
    width = part.shape[-1]
    rows_loc = part.shape[0] // n_dev
    rows = rows_loc // N_CHUNKS
    operands = [part.reshape(n_dev, rows_loc, width), gain.reshape(1, width)]
    if residual is not None:
        operands.append(residual)
    out = jax.ShapeDtypeStruct((rows_loc, width), jnp.bfloat16)
    return pl.pallas_call(
        functools.partial(scatter_kernel, N_CHUNKS, residual is not None),
        in_specs=[pl.BlockSpec(memory_space=pltpu.VMEM)] * len(operands),
        out_specs=[pl.BlockSpec(memory_space=pltpu.VMEM)] * 2,
        out_shape=[out, out],
        scratch_shapes=[pltpu.VMEM((rows, width), jnp.float32)] + chunk_bufs(N_CHUNKS, rows, width) + chunk_sems(Scatter, N_CHUNKS),
        compiler_params=pltpu.CompilerParams(collective_id=collective_id, has_side_effects=True, vmem_limit_bytes=VMEM_LIMIT),
        name="scatter_rows",
    )(*operands)


def gather_kernel(n_chunks, own_ref, out_ref, full, copy_sem, *sems):
    rows = own_ref.shape[0] // n_chunks
    place = Place()
    chunk_rows = lambda k: pl.ds(pl.multiple_of(k * rows, rows), rows)
    gath = Gather(place, lambda k: own_ref.at[chunk_rows(k), :], lambda d, k: full.at[d, chunk_rows(k), :], sems)
    entry_barrier(place)

    def put(k):
        return pltpu.make_async_copy(full.at[:, chunk_rows(k), :], out_ref.at[:, chunk_rows(k), :], copy_sem.at[k])

    def first(k, carry):
        gath.stage(0, k)
        full[place.me, chunk_rows(k), :] = own_ref[chunk_rows(k), :]
        return carry

    def wave(t, carry):
        for back in range(len(GATHER_WAVE) - 1, -1, -1):
            k = t - back

            @pl.when((k >= 0) & (k < n_chunks))
            def _():
                for number in GATHER_WAVE[back]:
                    gath.stage(number, k)
                if back == len(GATHER_WAVE) - 1:
                    put(k).start()
        return carry

    def drain(k, carry):
        gath.drain(k)
        put(k).wait()
        return carry

    lax.fori_loop(0, n_chunks, first, 0)
    lax.fori_loop(0, n_chunks + len(GATHER_WAVE) - 1, wave, 0)
    lax.fori_loop(0, n_chunks, drain, 0)


def gather_rows(own, collective_id):
    n_dev = N_Z * N_Y * 2
    rows_loc, width = own.shape
    full = pl.pallas_call(
        functools.partial(gather_kernel, N_CHUNKS),
        in_specs=[pl.BlockSpec(memory_space=pltpu.VMEM)],
        out_specs=pl.BlockSpec(memory_space=pl.ANY),
        out_shape=jax.ShapeDtypeStruct((n_dev, rows_loc, width), jnp.bfloat16),
        scratch_shapes=[pltpu.VMEM((n_dev, rows_loc, width), jnp.bfloat16), pltpu.SemaphoreType.DMA((N_CHUNKS,))] + chunk_sems(Gather, N_CHUNKS),
        compiler_params=pltpu.CompilerParams(collective_id=collective_id, has_side_effects=True, vmem_limit_bytes=VMEM_LIMIT),
        name="gather_rows",
    )(own)
    return full.reshape(n_dev * rows_loc, width)


def group_sum_kernel(x_ref, out_ref, slots, send_sem, recv_sem):
    n_dev = slots.shape[0]
    me = lax.axis_index("tp")
    barrier = pltpu.get_barrier_semaphore()
    for off in range(1, n_dev):
        pl.semaphore_signal(barrier, inc=1, device_id={"tp": (me + off) % n_dev}, device_id_type=MESH)
    pl.semaphore_wait(barrier, n_dev - 1)
    for off in range(1, n_dev):
        remote(x_ref, slots.at[me], send_sem.at[off], recv_sem.at[me], (me + off) % n_dev).start()
    slots[me] = x_ref[...]
    for off in range(1, n_dev):
        other = (me + off) % n_dev
        remote(x_ref, slots.at[other], send_sem.at[off], recv_sem.at[other], other).wait_recv()
    out_ref[...] = jnp.sum(slots[...], axis=0)
    for off in range(1, n_dev):
        remote(x_ref, slots.at[me], send_sem.at[off], recv_sem.at[me], (me + off) % n_dev).wait_send()


def group_sum(x, n_dev, collective_id):
    return pl.pallas_call(
        group_sum_kernel,
        in_specs=[pl.BlockSpec(memory_space=pltpu.VMEM)],
        out_specs=pl.BlockSpec(memory_space=pltpu.VMEM),
        out_shape=jax.ShapeDtypeStruct(x.shape, x.dtype),
        scratch_shapes=[pltpu.VMEM((n_dev,) + x.shape, x.dtype), pltpu.SemaphoreType.DMA((n_dev,)), pltpu.SemaphoreType.DMA((n_dev,))],
        compiler_params=pltpu.CompilerParams(collective_id=collective_id, has_side_effects=True),
        name="group_sum",
    )(x)


SUM_STEPS = {0: 0, 1: 1, 3: 2, 4: 3, 5: 4, 6: 5}


def moe_kernel(n_chunks, exp_step, ctx_ref, wo_ref, x_ref, gain_ref, mask_ref, wr_ref, wg_ref, wu_ref, wd_ref, out_ref, acc_ref, gate_ref, full, part, total, m_own, h_own, *rest):
    bufs, rest = rest[:6], rest[6:]
    n_sc = len(Scatter.SEMS)
    attn_sems, moe_sems, gather_sems = rest[:n_sc], rest[n_sc:2 * n_sc], rest[2 * n_sc:]
    chunk, step = pl.program_id(0), pl.program_id(1)
    n_steps = pl.num_programs(1)
    rows = m_own.shape[0] // n_chunks
    n_exp = wr_ref.shape[0]
    exp_ff = wg_ref.shape[0] // exp_step
    n_tok = full.shape[1]
    nt_dims = (((1,), (1,)), ((), ()))
    place = Place()
    loc_rows = lambda k: pl.ds(pl.multiple_of(k * rows, rows), rows)
    block = lambda ref: (lambda d, k: ref.at[k, pl.ds(pl.multiple_of(d * rows, rows), rows), :])
    gath = Gather(place, lambda k: m_own.at[loc_rows(k), :], block(full), gather_sems)
    attn = Scatter(place, block(part), bufs, total, attn_sems)
    scat = Scatter(place, block(part), bufs, total, moe_sems)

    def project(k):
        part[k] = jnp.dot(ctx_ref[k], wo_ref[...], preferred_element_type=jnp.float32).astype(jnp.bfloat16)

    def attn_stage(number, k):
        attn.stage(number, k)
        if number == N_STAGES - 1:
            attn_out = total[...].astype(jnp.bfloat16).astype(jnp.float32)
            hidden = (x_ref[loc_rows(k), :].astype(jnp.float32) + attn_out).astype(jnp.bfloat16)
            h_own[loc_rows(k), :] = hidden
            normed = norm_rows(hidden.astype(jnp.float32), gain_ref[...].astype(jnp.float32))
            m_own[loc_rows(k), :] = normed
            full[k, pl.ds(pl.multiple_of(place.me * rows, rows), rows), :] = normed

    def moe_stage(number, k):
        scat.stage(number, k)
        if number == N_STAGES - 1:
            moe_out = total[...].astype(jnp.bfloat16).astype(jnp.float32)
            out_ref[loc_rows(k), :] = (h_own[loc_rows(k), :].astype(jnp.float32) + moe_out).astype(jnp.bfloat16)

    @pl.when((chunk == 0) & (step == 0))
    def _():
        entry_barrier(place)
        for k in (0, 1):
            project(k)
            attn_stage(0, k)
        attn_stage(1, 0)
        for k in range(2, n_chunks):
            project(k)
            attn_stage(0, k)
        attn_stage(1, 1)
        for number in range(2, N_STAGES):
            attn_stage(number, 0)
        attn_stage(2, 1)
        gath.stage(0, 0)
        attn_stage(3, 1)
        for number in (1, 4):
            gath.stage(number, 0)
        attn_stage(4, 1)
        for number in (2, 5):
            gath.stage(number, 0)
        attn_stage(5, 1)
        for number in (3, 6, 7, 8):
            gath.stage(number, 0)

    for at in range(2 * N_Z):
        @pl.when((step == at) & (chunk + 1 < n_chunks))
        def _():
            gath.stage(at, chunk + 1)

        if at in SUM_STEPS:
            @pl.when((step == at) & (chunk > 0))
            def _():
                moe_stage(SUM_STEPS[at], chunk - 1)

            if at > 0:
                @pl.when((step == at) & (chunk == 0))
                def _():
                    attn_stage(SUM_STEPS[at], 2)

    for at_chunk, at, number in ((0, 5, 1), (0, 7, 2), (1, 0, 3), (1, 1, 4), (1, 2, 5)):
        @pl.when((step == at) & (chunk == at_chunk))
        def _():
            attn_stage(number, 3)

    @pl.when((step == 0) & (chunk > 0))
    def _():
        gath.stage(GATHER_LAST, chunk)

    @pl.when(step == 0)
    def _():
        logits = lax.dot_general(full[chunk], wr_ref[...], nt_dims, preferred_element_type=jnp.float32)
        logits = logits - jnp.max(logits, axis=-1, keepdims=True)
        expd = jnp.exp(logits)
        gates = expd / jnp.sum(expd, axis=-1, keepdims=True) * mask_ref[0]
        for grp in range(n_exp // exp_step):
            gate_ref[grp] = gates[:, grp * exp_step:(grp + 1) * exp_step]
        acc_ref[...] = jnp.zeros_like(acc_ref)

    m_rows = full[chunk]
    gate_proj = lax.dot_general(m_rows, wg_ref[...], nt_dims, preferred_element_type=jnp.float32)
    up_proj = lax.dot_general(m_rows, wu_ref[...], nt_dims, preferred_element_type=jnp.float32)
    act = (gate_proj / (1.0 + jnp.exp(-gate_proj)) * up_proj).astype(jnp.bfloat16).astype(jnp.float32)
    gates = gate_ref[step]
    lane = lax.broadcasted_iota(jnp.int32, (n_tok, 2 * exp_ff), 1)
    pieces = []
    for pair in range(exp_step // 2):
        pieces.append(jnp.where(lane < exp_ff, gates[:, 2 * pair:2 * pair + 1], gates[:, 2 * pair + 1:2 * pair + 2]))
    scaled = act * jnp.concatenate(pieces, axis=1)
    high = scaled.astype(jnp.bfloat16)
    low = (scaled - high.astype(jnp.float32)).astype(jnp.bfloat16)
    acc_ref[...] += jnp.dot(high, wd_ref[...], preferred_element_type=jnp.float32) + jnp.dot(low, wd_ref[...], preferred_element_type=jnp.float32)

    @pl.when(step == n_steps - 1)
    def _():
        attn.drain(chunk)
        part[chunk] = acc_ref[...].astype(jnp.bfloat16)

    @pl.when((step == n_steps - 1) & (chunk == n_chunks - 1))
    def _():
        for number in range(N_STAGES):
            moe_stage(number, n_chunks - 1)

        def drain(k, carry):
            gath.drain(k)
            scat.drain(k)
            return carry

        lax.fori_loop(0, n_chunks, drain, 0)


def moe_layer(ctx, w_out, x_loc, gain, mask, wr_t, wg_t, wu_t, w_dn, collective_id):
    rows_loc, width = x_loc.shape
    n_chunks, n_tok, n_exp = mask.shape
    n_ff = wg_t.shape[0]
    step_cols = n_ff // n_exp * EXP_PER_STEP
    rows = rows_loc // n_chunks
    const = lambda k, s: (0, 0)
    return pl.pallas_call(
        functools.partial(moe_kernel, n_chunks, EXP_PER_STEP),
        grid=(n_chunks, n_ff // step_cols),
        in_specs=[
            pl.BlockSpec(ctx.shape, lambda k, s: (0, 0, 0)),
            pl.BlockSpec(w_out.shape, const),
            pl.BlockSpec((rows_loc, width), const),
            pl.BlockSpec((1, width), const),
            pl.BlockSpec((1, n_tok, n_exp), lambda k, s: (k, 0, 0)),
            pl.BlockSpec((n_exp, width), const),
            pl.BlockSpec((step_cols, width), lambda k, s: (s, 0)),
            pl.BlockSpec((step_cols, width), lambda k, s: (s, 0)),
            pl.BlockSpec((step_cols, width), lambda k, s: (s, 0)),
        ],
        out_specs=pl.BlockSpec((rows_loc, width), const),
        out_shape=jax.ShapeDtypeStruct((rows_loc, width), jnp.bfloat16),
        scratch_shapes=[
            pltpu.VMEM((n_tok, width), jnp.float32),
            pltpu.VMEM((n_exp // EXP_PER_STEP, n_tok, EXP_PER_STEP), jnp.float32),
            pltpu.VMEM((n_chunks, n_tok, width), jnp.bfloat16),
            pltpu.VMEM((n_chunks, n_tok, width), jnp.bfloat16),
            pltpu.VMEM((rows, width), jnp.float32),
            pltpu.VMEM((rows_loc, width), jnp.bfloat16),
            pltpu.VMEM((rows_loc, width), jnp.bfloat16),
        ] + chunk_bufs(n_chunks, rows, width) + chunk_sems(Scatter, n_chunks) + chunk_sems(Scatter, n_chunks) + chunk_sems(Gather, n_chunks),
        compiler_params=pltpu.CompilerParams(dimension_semantics=("arbitrary", "arbitrary"), collective_id=collective_id, has_side_effects=True, vmem_limit_bytes=VMEM_LIMIT),
        name="moe_layer",
    )(ctx, w_out, x_loc, gain.reshape(1, width), mask, wr_t, wg_t, wu_t, w_dn)


def solution(mesh):
    tp_size = mesh.shape["tp"]
    in_specs = (P("dp", None), P("dp", None, None), P("tp", None), P(None), P(None, "tp"), P(None, "tp"), P(None, "tp"), P("tp", None), P("tp"), P("tp"), P(None), P(None, None), P(None, None, "tp"), P(None, None, "tp"), P(None, "tp", None))

    def device_fn(token_ids, route_idx, embed_table, attn_norm, w_query, w_key, w_value, w_out, q_gain, k_gain, mlp_norm, w_router, w_gate, w_up, w_down):
        batch_loc, seq_len = token_ids.shape
        vocab_loc, model_dim = embed_table.shape
        tp_rank = lax.axis_index("tp")
        local_ids = token_ids - tp_rank * vocab_loc
        in_range = (local_ids >= 0) & (local_ids < vocab_loc)
        looked_up = jnp.take(embed_table, jnp.clip(local_ids, 0, vocab_loc - 1), axis=0)
        embed_part = jnp.where(in_range[..., None], looked_up, jnp.zeros((), jnp.bfloat16))
        x_loc, a_loc = scatter_rows(embed_part.reshape(-1, model_dim), attn_norm, None, 0)
        normed = gather_rows(a_loc, 1).reshape(batch_loc, seq_len, model_dim)
        q_raw = jnp.einsum("bsd,dq->bsq", normed, w_query, preferred_element_type=jnp.float32)
        k_raw = jnp.einsum("bsd,dq->bsq", normed, w_key, preferred_element_type=jnp.float32)
        heads_loc = w_query.shape[1] // HEAD_DIM
        head_shape = (batch_loc, seq_len, heads_loc, HEAD_DIM)
        v_heads = jnp.einsum("bsd,dq->bsq", normed, w_value, preferred_element_type=jnp.float32).astype(jnp.bfloat16).reshape(head_shape)
        sq_sums = jnp.stack([jnp.sum(q_raw * q_raw, axis=-1), jnp.sum(k_raw * k_raw, axis=-1)])
        sq_total = group_sum(sq_sums.reshape(2, -1), tp_size, 2).reshape(sq_sums.shape)
        inv_rms = lax.rsqrt(sq_total / (w_query.shape[1] * tp_size) + NORM_EPS)
        cos_tab, sin_tab = rope_tables(seq_len)
        q_heads = apply_rope((q_raw * inv_rms[0][..., None] * q_gain.astype(jnp.float32)).reshape(head_shape), cos_tab, sin_tab)
        k_heads = apply_rope((k_raw * inv_rms[1][..., None] * k_gain.astype(jnp.float32)).reshape(head_shape), cos_tab, sin_tab)
        scores = jnp.einsum("bqhd,bkhd->bhqk", q_heads, k_heads, preferred_element_type=jnp.float32) * (HEAD_DIM ** -0.5)
        positions = jnp.arange(seq_len)
        scores = jnp.where(positions[:, None] >= positions[None, :], scores, -1e30)
        attn_prob = jax.nn.softmax(scores, axis=-1).astype(jnp.bfloat16)
        context = jnp.einsum("bhqk,bkhd->bqhd", attn_prob, v_heads, preferred_element_type=jnp.float32).astype(jnp.bfloat16)
        n_exp = w_gate.shape[0]
        wg_t = jnp.swapaxes(w_gate, 1, 2).reshape(-1, model_dim)
        wu_t = jnp.swapaxes(w_up, 1, 2).reshape(-1, model_dim)
        w_dn = w_down.reshape(-1, model_dim)
        wr_t = w_router.T
        expert_iota = jnp.arange(n_exp, dtype=jnp.int32)
        chosen = route_idx.reshape(batch_loc * seq_len, -1)
        mask = jnp.any(chosen[:, :, None] == expert_iota[None, None, :], axis=1).astype(jnp.float32)
        rows_chunk = x_loc.shape[0] // N_CHUNKS
        to_chunks = lambda arr: arr.reshape(tp_size, N_CHUNKS, rows_chunk, -1).swapaxes(0, 1).reshape(N_CHUNKS, tp_size * rows_chunk, -1)
        out_loc = moe_layer(to_chunks(context), w_out, x_loc, mlp_norm, to_chunks(mask), wr_t, wg_t, wu_t, w_dn, 4)
        return out_loc.reshape(batch_loc, -1, model_dim)

    return jax.shard_map(device_fn, mesh=mesh, in_specs=in_specs, out_specs=P("dp", "tp", None), check_vma=False)
```

```python
import functools

import jax
import jax.numpy as jnp
from jax import lax
from jax.experimental import pallas as pl
from jax.experimental.pallas import tpu as pltpu
from jax.sharding import PartitionSpec as P

HEAD_DIM = 128
NORM_EPS = 1e-5
N_CHUNKS = 4
EXP_PER_STEP = 8
VMEM_LIMIT = 63 * 1024 * 1024


def rope_tables(seq_len):
    half_dim = HEAD_DIM // 2
    inv_freq = 1.0 / (10000.0 ** (jnp.arange(half_dim, dtype=jnp.float32) * (2.0 / HEAD_DIM)))
    angles = jnp.arange(seq_len, dtype=jnp.float32)[:, None] * inv_freq[None, :]
    return jnp.cos(angles), jnp.sin(angles)


N_STAGES = 6
N_Z, N_Y = 4, 2
GATHER_LAST = 8
MESH = pl.DeviceIdType.MESH


class Place:
    def __init__(self):
        self.me = lax.axis_index("tp")
        self.z = self.me // 4
        self.y = self.me % 4 // 2
        self.c = self.me % 2
        self.core_peer = self.me + 1 - 2 * self.c
        self.y_peer = self.me + 2 - 4 * self.y
        self.up = self.me + 4
        self.down = self.me - 4

    def index(self, zz, yy, cc):
        return zz * 4 + yy * 2 + cc


def remote(src, dst, send_sem, recv_sem, device):
    return pltpu.make_async_remote_copy(src_ref=src, dst_ref=dst, send_sem=send_sem, recv_sem=recv_sem, device_id={"tp": device}, device_id_type=MESH)


def entry_barrier(place):
    barrier = pltpu.get_barrier_semaphore()
    for peer in (place.core_peer, place.y_peer):
        pl.semaphore_signal(barrier, inc=1, device_id={"tp": peer}, device_id_type=MESH)

    @pl.when(place.z > 0)
    def _():
        pl.semaphore_signal(barrier, inc=1, device_id={"tp": place.down}, device_id_type=MESH)

    @pl.when(place.z < N_Z - 1)
    def _():
        pl.semaphore_signal(barrier, inc=1, device_id={"tp": place.up}, device_id_type=MESH)

    pl.semaphore_wait(barrier, 2 + (place.z + 3) // 4 + (6 - place.z) // 4)


def by_distance(place, dist, act):
    if dist == 0:
        act(place.z)
        return

    @pl.when(place.z + dist < N_Z)
    def _():
        act(place.z + dist)

    @pl.when(place.z >= dist)
    def _():
        act(place.z - dist)


class Gather:
    SEMS = [(4,), (4,), (4,), (4,), (4,), (8,), (8,)]

    def __init__(self, place, own, shard, sems):
        self.place, self.own, self.shard = place, own, shard
        self.up_send, self.down_send, self.z_recv, self.y_send, self.y_recv, self.c_send, self.c_recv = sems

    def src(self, d, k, mine):
        return self.own(k) if mine else self.shard(d, k)

    def to_up(self, zz, k, mine=False):
        d = self.place.index(zz, self.place.y, self.place.c)
        return remote(self.src(d, k, mine), self.shard(d, k), self.up_send.at[k, zz], self.z_recv.at[k, zz], self.place.up)

    def to_down(self, zz, k, mine=False):
        d = self.place.index(zz, self.place.y, self.place.c)
        return remote(self.src(d, k, mine), self.shard(d, k), self.down_send.at[k, zz], self.z_recv.at[k, zz], self.place.down)

    def to_y(self, zz, k, mine=False, flip=False):
        d = self.place.index(zz, 1 - self.place.y if flip else self.place.y, self.place.c)
        return remote(self.src(d, k, mine), self.shard(d, k), self.y_send.at[k, zz], self.y_recv.at[k, zz], self.place.y_peer)

    def to_core(self, zz, yy, k, mine=False, flip=False):
        d = self.place.index(zz, yy, 1 - self.place.c if flip else self.place.c)
        slot = zz * 2 + yy
        return remote(self.src(d, k, mine), self.shard(d, k), self.c_send.at[k, slot], self.c_recv.at[k, slot], self.place.core_peer)

    def stage(self, number, k):
        place = self.place
        z, y = place.z, place.y
        if number == 0:
            @pl.when(z < N_Z - 1)
            def _():
                self.to_up(z, k, True).start()

            @pl.when(z > 0)
            def _():
                self.to_down(z, k, True).start()

            self.to_y(z, k, True).start()
            self.to_core(z, y, k, True).start()
        elif number < N_Z:
            @pl.when(z >= number)
            def _():
                zz = z - number
                self.to_up(zz, k).wait_recv()

                @pl.when(z < N_Z - 1)
                def _():
                    self.to_up(zz, k).start()

                self.to_y(zz, k).start()
                self.to_core(zz, y, k).start()

            @pl.when(z + number < N_Z)
            def _():
                zz = z + number
                self.to_down(zz, k).wait_recv()

                @pl.when(z > 0)
                def _():
                    self.to_down(zz, k).start()

                self.to_y(zz, k).start()
                self.to_core(zz, y, k).start()
        elif number < 2 * N_Z:
            def pass_on(zz):
                self.to_y(zz, k, flip=True).wait_recv()
                self.to_core(zz, 1 - y, k).start()

            by_distance(place, number - N_Z, pass_on)
        else:
            for zz in range(N_Z):
                for yy in range(N_Y):
                    self.to_core(zz, yy, k, flip=True).wait_recv()

    def drain(self, k):
        z = self.place.z
        for zz in range(N_Z):
            @pl.when((z >= zz) & (z < N_Z - 1))
            def _():
                self.to_up(zz, k).wait_send()

            @pl.when((z <= zz) & (z > 0))
            def _():
                self.to_down(zz, k).wait_send()

            self.to_y(zz, k).wait_send()
            for yy in range(N_Y):
                self.to_core(zz, yy, k).wait_send()


class Scatter:
    SEMS = [(8,), (8,), (4,), (4,), (4,), (4,), (4,), (4,)]
    BUFS = (8, 4, 4, 4, 4, 4)

    def __init__(self, place, shard, bufs, total, sems):
        self.place, self.shard, self.total = place, shard, total
        self.c_buf, self.y_out, self.y_in, self.z_out, self.from_down, self.from_up = bufs
        self.c_send, self.c_recv, self.y_send, self.y_recv, self.up_send, self.up_recv, self.down_send, self.down_recv = sems

    def to_core(self, zz, yy, k):
        slot = zz * 2 + yy
        d = self.place.index(zz, yy, 1 - self.place.c)
        return remote(self.shard(d, k), self.c_buf.at[k, slot], self.c_send.at[k, slot], self.c_recv.at[k, slot], self.place.core_peer)

    def to_y(self, zz, k):
        return remote(self.y_out.at[k, zz], self.y_in.at[k, zz], self.y_send.at[k, zz], self.y_recv.at[k, zz], self.place.y_peer)

    def to_up(self, zz, k):
        return remote(self.z_out.at[k, zz], self.from_down.at[k, zz], self.up_send.at[k, zz], self.up_recv.at[k, zz], self.place.up)

    def to_down(self, zz, k):
        return remote(self.z_out.at[k, zz], self.from_up.at[k, zz], self.down_send.at[k, zz], self.down_recv.at[k, zz], self.place.down)

    def pair_sum(self, zz, yy, k):
        self.to_core(zz, yy, k).wait_recv()
        mine = self.shard(self.place.index(zz, yy, self.place.c), k)[...].astype(jnp.float32)
        return mine + self.c_buf[k, zz * 2 + yy].astype(jnp.float32)

    def chip_pair_sum(self, zz, k):
        both = self.pair_sum(zz, self.place.y, k)
        self.to_y(zz, k).wait_recv()
        return both + self.y_in[k, zz].astype(jnp.float32)

    def stage(self, number, k):
        place = self.place
        z, y = place.z, place.y
        if number == 0:
            for yy in (1 - y, y):
                for zz in range(N_Z):
                    self.to_core(zz, yy, k).start()
        elif number == 1:
            def send_y(zz):
                self.y_out[k, zz] = self.pair_sum(zz, 1 - y, k).astype(jnp.bfloat16)
                self.to_y(zz, k).start()

            for dist in (3, 2, 1, 0):
                by_distance(place, dist, send_y)
        elif number < N_STAGES - 1:
            dist = N_STAGES - 1 - number

            @pl.when(z + dist < N_Z)
            def _():
                zz = z + dist
                self.total[...] = self.chip_pair_sum(zz, k)

                @pl.when(z > 0)
                def _():
                    self.to_up(zz, k).wait_recv()
                    self.total[...] += self.from_down[k, zz].astype(jnp.float32)

                self.z_out[k, zz] = self.total[...].astype(jnp.bfloat16)
                self.to_up(zz, k).start()

            @pl.when(z >= dist)
            def _():
                zz = z - dist
                self.total[...] = self.chip_pair_sum(zz, k)

                @pl.when(z < N_Z - 1)
                def _():
                    self.to_down(zz, k).wait_recv()
                    self.total[...] += self.from_up[k, zz].astype(jnp.float32)

                self.z_out[k, zz] = self.total[...].astype(jnp.bfloat16)
                self.to_down(zz, k).start()
        else:
            self.total[...] = self.chip_pair_sum(z, k)

            @pl.when(z > 0)
            def _():
                self.to_up(z, k).wait_recv()
                self.total[...] += self.from_down[k, z].astype(jnp.float32)

            @pl.when(z < N_Z - 1)
            def _():
                self.to_down(z, k).wait_recv()
                self.total[...] += self.from_up[k, z].astype(jnp.float32)

    def drain(self, k):
        z = self.place.z
        for zz in range(N_Z):
            for yy in range(N_Y):
                self.to_core(zz, yy, k).wait_send()
            self.to_y(zz, k).wait_send()

            @pl.when(z < zz)
            def _():
                self.to_up(zz, k).wait_send()

            @pl.when(z > zz)
            def _():
                self.to_down(zz, k).wait_send()


def chunk_sems(kind, n_chunks):
    return [pltpu.SemaphoreType.DMA((n_chunks,) + shape) for shape in kind.SEMS]


def chunk_bufs(n_chunks, rows, width):
    return [pltpu.VMEM((n_chunks, slots, rows, width), jnp.bfloat16) for slots in Scatter.BUFS]


def norm_rows(rows_f32, gain_f32):
    mean_sq = jnp.mean(rows_f32 * rows_f32, axis=-1, keepdims=True)
    return (rows_f32 * lax.rsqrt(mean_sq + NORM_EPS) * gain_f32).astype(jnp.bfloat16)


def scatter_kernel(n_chunks, looked, keep, gain, sum_ref, norm_ref, part, total, *scratch):
    bufs, sems = scratch[:6], scratch[6:]
    rows = total.shape[0]
    place = Place()
    chunk_rows = lambda k: pl.ds(pl.multiple_of(k * rows, rows), rows)
    scat = Scatter(place, lambda d, k: part.at[d, chunk_rows(k), :], bufs, total, sems)
    entry_barrier(place)

    def first(k, carry):
        def mask_rows(d, inner):
            part[d, chunk_rows(k), :] = (looked[d, chunk_rows(k), :].astype(jnp.float32) * keep[d, chunk_rows(k), :]).astype(jnp.bfloat16)
            return inner

        lax.fori_loop(0, part.shape[0], mask_rows, 0)
        scat.stage(0, k)
        return carry

    def second(k, carry):
        scat.stage(1, k)
        return carry

    def finish(k):
        value = total[...].astype(jnp.bfloat16)
        sum_ref[chunk_rows(k), :] = value
        norm_ref[chunk_rows(k), :] = norm_rows(value.astype(jnp.float32), gain[...].astype(jnp.float32))

    def wave(t, carry):
        for number in range(N_STAGES - 1, 1, -1):
            k = t - (number - 2)

            @pl.when((k >= 0) & (k < n_chunks))
            def _():
                scat.stage(number, k)
                if number == N_STAGES - 1:
                    finish(k)
        return carry

    def drain(k, carry):
        scat.drain(k)
        return carry

    lax.fori_loop(0, n_chunks, first, 0)
    lax.fori_loop(0, n_chunks, second, 0)
    lax.fori_loop(0, n_chunks + N_STAGES - 3, wave, 0)
    lax.fori_loop(0, n_chunks, drain, 0)


def scatter_rows(looked, keep, gain, collective_id):
    n_dev = N_Z * N_Y * 2
    width = looked.shape[-1]
    rows_loc = looked.shape[0] // n_dev
    rows = rows_loc // N_CHUNKS
    out = jax.ShapeDtypeStruct((rows_loc, width), jnp.bfloat16)
    return pl.pallas_call(
        functools.partial(scatter_kernel, N_CHUNKS),
        in_specs=[pl.BlockSpec(memory_space=pltpu.VMEM)] * 3,
        out_specs=[pl.BlockSpec(memory_space=pltpu.VMEM)] * 2,
        out_shape=[out, out],
        scratch_shapes=[pltpu.VMEM((n_dev, rows_loc, width), jnp.bfloat16), pltpu.VMEM((rows, width), jnp.float32)] + chunk_bufs(N_CHUNKS, rows, width) + chunk_sems(Scatter, N_CHUNKS),
        compiler_params=pltpu.CompilerParams(collective_id=collective_id, has_side_effects=True, vmem_limit_bytes=VMEM_LIMIT),
        name="scatter_rows",
    )(looked.reshape(n_dev, rows_loc, width), keep.reshape(n_dev, rows_loc, 1), gain.reshape(1, width))


KEY_BLOCK = 512


def attend_kernel(own_ref, wq_ref, wk_ref, wv_ref, qg_ref, kg_ref, cos_ref, sin_ref, out_ref, full, w_all, q_t, k_t, v_t, q_b, k_rows, stat, slots, scores, stat_send, stat_recv, *sems):
    n_dev, rows, width = full.shape
    n_tok = n_dev * rows
    dim = HEAD_DIM
    half = dim // 2
    place = Place()
    me, z, y, c = place.me, place.z, place.y, place.c
    gath = Gather(place, lambda k: own_ref, lambda d, k: full.at[d], sems)
    barrier = pltpu.get_barrier_semaphore()
    for off in range(1, n_dev):
        pl.semaphore_signal(barrier, inc=1, device_id={"tp": (me + off) % n_dev}, device_id_type=MESH)
    pl.semaphore_wait(barrier, n_dev - 1)
    gath.stage(0, 0)
    full[me] = own_ref[...]
    for pos, w_ref in enumerate((wq_ref, wk_ref, wv_ref)):
        w_all[:, pos * dim:(pos + 1) * dim] = w_ref[...]
    packed = jnp.where(z == 0, 228, jnp.where(z == 1, 225, jnp.where(z == 2, 30, 27)))

    def event(e, carry):
        turn, kind = e // 4, e % 4
        rank = turn - (kind + 1) // 2
        valid = (rank >= 0) & (rank < N_Z)
        zz = (packed >> (2 * jnp.clip(rank, 0, N_Z - 1))) & 3

        @pl.when(valid & (kind == 0) & (zz < z))
        def _():
            gath.to_up(zz, 0).wait_recv()

            @pl.when(z < N_Z - 1)
            def _():
                gath.to_up(zz, 0).start()

        @pl.when(valid & (kind == 0) & (zz > z))
        def _():
            gath.to_down(zz, 0).wait_recv()

            @pl.when(z > 0)
            def _():
                gath.to_down(zz, 0).start()

        @pl.when(valid & (kind == 0) & (rank > 0))
        def _():
            gath.to_y(zz, 0).start()
            gath.to_core(zz, y, 0).start()

        @pl.when(valid & (kind == 1))
        def _():
            gath.to_core(zz, y, 0, flip=True).wait_recv()

        @pl.when(valid & (kind == 2))
        def _():
            gath.to_y(zz, 0, flip=True).wait_recv()
            gath.to_core(zz, 1 - y, 0).start()

        @pl.when(valid & (kind == 3))
        def _():
            gath.to_core(zz, 1 - y, 0, flip=True).wait_recv()

        @pl.when(valid)
        def _():
            d = zz * 4 + (y + kind // 2) % 2 * 2 + (c + kind) % 2
            lanes = pl.ds(pl.multiple_of(d * rows, rows), rows)
            qkv = jnp.dot(full[d], w_all[...], preferred_element_type=jnp.float32)
            q_blk, k_blk, v_blk = (qkv[:, i * dim:(i + 1) * dim].T for i in range(3))
            q_t[:, lanes] = q_blk
            k_t[:, lanes] = k_blk
            v_t[:, lanes] = v_blk.astype(jnp.bfloat16)
            stat[0:1, lanes] = jnp.sum(q_blk * q_blk, axis=0, keepdims=True)
            stat[1:2, lanes] = jnp.sum(k_blk * k_blk, axis=0, keepdims=True)
        return carry

    lax.fori_loop(0, 24, event, 0)
    gath.drain(0)

    def to_peer(off):
        return remote(stat, slots.at[me], stat_send.at[off], stat_recv.at[me], (me + off) % n_dev)

    for off in range(1, n_dev):
        to_peer(off).start()
    slots[me] = stat[...]
    for off in range(1, n_dev):
        other = (me + off) % n_dev
        remote(stat, slots.at[other], stat_send.at[off], stat_recv.at[other], other).wait_recv()
    stat_total = jnp.sum(slots[...], axis=0)
    inv_rms = lax.rsqrt(stat_total / (n_dev * dim) + NORM_EPS)
    for off in range(1, n_dev):
        to_peer(off).wait_send()
    slots[0] = inv_rms

    def rotate(blk, carry):
        lanes = pl.ds(pl.multiple_of(blk * KEY_BLOCK, KEY_BLOCK), KEY_BLOCK)
        cos_b, sin_b = cos_ref[:, lanes], sin_ref[:, lanes]
        heads = []
        for row, raw, gain in ((0, q_t, qg_ref), (1, k_t, kg_ref)):
            normed = raw[:, lanes] * slots[0, row:row + 1, lanes] * gain[...]
            first, second = normed[:half], normed[half:]
            heads.append(jnp.concatenate([first * cos_b - second * sin_b, second * cos_b + first * sin_b], axis=0))
        q_b[:, lanes] = heads[0].astype(jnp.bfloat16)
        k_rows[lanes, :] = heads[1].T.astype(jnp.bfloat16)
        return carry

    lax.fori_loop(0, n_tok // KEY_BLOCK, rotate, 0)

    def attend(blk, carry):
        queries = pl.ds(pl.multiple_of(blk * KEY_BLOCK, KEY_BLOCK), KEY_BLOCK)
        q_blk = q_b[:, queries]
        key_rows = lambda j: pl.ds(pl.multiple_of(j * KEY_BLOCK, KEY_BLOCK), KEY_BLOCK)

        def score(j, top):
            raw = jnp.dot(k_rows[key_rows(j), :], q_blk, preferred_element_type=jnp.float32) * (dim ** -0.5)
            key_pos = lax.broadcasted_iota(jnp.int32, raw.shape, 0) + (j - blk) * KEY_BLOCK
            raw = jnp.where(key_pos <= lax.broadcasted_iota(jnp.int32, raw.shape, 1), raw, -1e30)
            scores[key_rows(j), :] = raw
            return jnp.maximum(top, jnp.max(raw, axis=0, keepdims=True))

        top = lax.fori_loop(0, blk + 1, score, jnp.full((1, KEY_BLOCK), -1e30, jnp.float32))

        def expo(j, norm):
            raised = jnp.exp(scores[key_rows(j), :] - top)
            scores[key_rows(j), :] = raised
            return norm + jnp.sum(raised, axis=0, keepdims=True)

        norm = lax.fori_loop(0, blk + 1, expo, jnp.zeros((1, KEY_BLOCK), jnp.float32))
        inv_norm = 1.0 / norm

        def weigh(j, acc):
            prob = (scores[key_rows(j), :] * inv_norm).astype(jnp.bfloat16)
            return acc + jnp.dot(v_t[:, key_rows(j)], prob, preferred_element_type=jnp.float32)

        ctx = lax.fori_loop(0, blk + 1, weigh, jnp.zeros((dim, KEY_BLOCK), jnp.float32)).T.astype(jnp.bfloat16)
        n_chunks = out_ref.shape[0]
        piece = rows // n_chunks
        for dev in range(KEY_BLOCK // rows):
            at = pl.ds(pl.multiple_of((blk * (KEY_BLOCK // rows) + dev) * piece, piece), piece)
            for k in range(n_chunks):
                out_ref[k, at, :] = ctx[dev * rows + k * piece:dev * rows + (k + 1) * piece, :]
        return carry

    lax.fori_loop(0, n_tok // KEY_BLOCK, attend, 0)


def attend_rows(own, wq, wk, wv, q_gain, k_gain, cos_t, sin_t, collective_id):
    n_dev = N_Z * N_Y * 2
    rows, width = own.shape
    n_tok = n_dev * rows
    operands = (own, wq, wk, wv, q_gain, k_gain, cos_t, sin_t)
    return pl.pallas_call(
        attend_kernel,
        in_specs=[pl.BlockSpec(memory_space=pltpu.VMEM)] * len(operands),
        out_specs=pl.BlockSpec(memory_space=pltpu.VMEM),
        out_shape=jax.ShapeDtypeStruct((N_CHUNKS, n_tok // N_CHUNKS, HEAD_DIM), jnp.bfloat16),
        scratch_shapes=[
            pltpu.VMEM((n_dev, rows, width), jnp.bfloat16),
            pltpu.VMEM((width, 3 * HEAD_DIM), jnp.bfloat16),
            pltpu.VMEM((HEAD_DIM, n_tok), jnp.float32),
            pltpu.VMEM((HEAD_DIM, n_tok), jnp.float32),
            pltpu.VMEM((HEAD_DIM, n_tok), jnp.bfloat16),
            pltpu.VMEM((HEAD_DIM, n_tok), jnp.bfloat16),
            pltpu.VMEM((n_tok, HEAD_DIM), jnp.bfloat16),
            pltpu.VMEM((2, n_tok), jnp.float32),
            pltpu.VMEM((n_dev, 2, n_tok), jnp.float32),
            pltpu.VMEM((n_tok, KEY_BLOCK), jnp.float32),
            pltpu.SemaphoreType.DMA((n_dev,)),
            pltpu.SemaphoreType.DMA((n_dev,)),
        ] + chunk_sems(Gather, 1),
        compiler_params=pltpu.CompilerParams(collective_id=collective_id, has_side_effects=True, vmem_limit_bytes=VMEM_LIMIT),
        name="attend_rows",
    )(*operands)


SUM_STEPS = {0: 0, 1: 1, 3: 2, 4: 3, 5: 4, 6: 5}


def moe_kernel(n_chunks, exp_step, ctx_ref, wo_ref, x_ref, gain_ref, mask_ref, wr_ref, wg_ref, wu_ref, wd_ref, out_ref, acc_ref, gate_ref, full, part, total, m_own, h_own, *rest):
    bufs, rest = rest[:6], rest[6:]
    n_sc = len(Scatter.SEMS)
    attn_sems, moe_sems, gather_sems = rest[:n_sc], rest[n_sc:2 * n_sc], rest[2 * n_sc:]
    chunk, step = pl.program_id(0), pl.program_id(1)
    n_steps = pl.num_programs(1)
    rows = m_own.shape[0] // n_chunks
    n_exp = wr_ref.shape[0]
    exp_ff = wg_ref.shape[0] // exp_step
    n_tok = full.shape[1]
    nt_dims = (((1,), (1,)), ((), ()))
    place = Place()
    loc_rows = lambda k: pl.ds(pl.multiple_of(k * rows, rows), rows)
    block = lambda ref: (lambda d, k: ref.at[k, pl.ds(pl.multiple_of(d * rows, rows), rows), :])
    gath = Gather(place, lambda k: m_own.at[loc_rows(k), :], block(full), gather_sems)
    attn = Scatter(place, block(part), bufs, total, attn_sems)
    scat = Scatter(place, block(part), bufs, total, moe_sems)

    def project(k):
        part[k] = jnp.dot(ctx_ref[k], wo_ref[...], preferred_element_type=jnp.float32).astype(jnp.bfloat16)

    def attn_stage(number, k):
        attn.stage(number, k)
        if number == N_STAGES - 1:
            attn_out = total[...].astype(jnp.bfloat16).astype(jnp.float32)
            hidden = (x_ref[loc_rows(k), :].astype(jnp.float32) + attn_out).astype(jnp.bfloat16)
            h_own[loc_rows(k), :] = hidden
            normed = norm_rows(hidden.astype(jnp.float32), gain_ref[...].astype(jnp.float32))
            m_own[loc_rows(k), :] = normed
            full[k, pl.ds(pl.multiple_of(place.me * rows, rows), rows), :] = normed

    def moe_stage(number, k):
        scat.stage(number, k)
        if number == N_STAGES - 1:
            moe_out = total[...].astype(jnp.bfloat16).astype(jnp.float32)
            out_ref[loc_rows(k), :] = (h_own[loc_rows(k), :].astype(jnp.float32) + moe_out).astype(jnp.bfloat16)

    @pl.when((chunk == 0) & (step == 0))
    def _():
        entry_barrier(place)
        for k in (0, 1):
            project(k)
            attn_stage(0, k)
        attn_stage(1, 0)
        for k in range(2, n_chunks):
            project(k)
            attn_stage(0, k)
        attn_stage(1, 1)
        for number in range(2, N_STAGES):
            attn_stage(number, 0)
        attn_stage(2, 1)
        gath.stage(0, 0)
        attn_stage(3, 1)
        for number in (1, 4):
            gath.stage(number, 0)
        attn_stage(4, 1)
        for number in (2, 5):
            gath.stage(number, 0)
        attn_stage(5, 1)
        for number in (3, 6, 7, 8):
            gath.stage(number, 0)

    for at in range(2 * N_Z):
        @pl.when((step == at) & (chunk + 1 < n_chunks))
        def _():
            gath.stage(at, chunk + 1)

        if at in SUM_STEPS:
            @pl.when((step == at) & (chunk > 0))
            def _():
                moe_stage(SUM_STEPS[at], chunk - 1)

            if at > 0:
                @pl.when((step == at) & (chunk == 0))
                def _():
                    attn_stage(SUM_STEPS[at], 2)

    for at_chunk, at, number in ((0, 5, 1), (0, 7, 2), (1, 0, 3), (1, 1, 4), (1, 2, 5)):
        @pl.when((step == at) & (chunk == at_chunk))
        def _():
            attn_stage(number, 3)

    @pl.when((step == 0) & (chunk > 0))
    def _():
        gath.stage(GATHER_LAST, chunk)

    @pl.when(step == 0)
    def _():
        logits = lax.dot_general(full[chunk], wr_ref[...], nt_dims, preferred_element_type=jnp.float32)
        logits = logits - jnp.max(logits, axis=-1, keepdims=True)
        expd = jnp.exp(logits)
        gates = expd / jnp.sum(expd, axis=-1, keepdims=True) * mask_ref[0]
        for grp in range(n_exp // exp_step):
            gate_ref[grp] = gates[:, grp * exp_step:(grp + 1) * exp_step]
        acc_ref[...] = jnp.zeros_like(acc_ref)

    m_rows = full[chunk]
    gate_proj = lax.dot_general(m_rows, wg_ref[...], nt_dims, preferred_element_type=jnp.float32)
    up_proj = lax.dot_general(m_rows, wu_ref[...], nt_dims, preferred_element_type=jnp.float32)
    act = (gate_proj / (1.0 + jnp.exp(-gate_proj)) * up_proj).astype(jnp.bfloat16).astype(jnp.float32)
    gates = gate_ref[step]
    lane = lax.broadcasted_iota(jnp.int32, (n_tok, 2 * exp_ff), 1)
    pieces = []
    for pair in range(exp_step // 2):
        pieces.append(jnp.where(lane < exp_ff, gates[:, 2 * pair:2 * pair + 1], gates[:, 2 * pair + 1:2 * pair + 2]))
    scaled = act * jnp.concatenate(pieces, axis=1)
    high = scaled.astype(jnp.bfloat16)
    low = (scaled - high.astype(jnp.float32)).astype(jnp.bfloat16)
    acc_ref[...] += jnp.dot(high, wd_ref[...], preferred_element_type=jnp.float32) + jnp.dot(low, wd_ref[...], preferred_element_type=jnp.float32)

    @pl.when(step == n_steps - 1)
    def _():
        attn.drain(chunk)
        part[chunk] = acc_ref[...].astype(jnp.bfloat16)

    @pl.when((step == n_steps - 1) & (chunk == n_chunks - 1))
    def _():
        for number in range(N_STAGES):
            moe_stage(number, n_chunks - 1)

        def drain(k, carry):
            gath.drain(k)
            scat.drain(k)
            return carry

        lax.fori_loop(0, n_chunks, drain, 0)


def moe_layer(ctx, w_out, x_loc, gain, mask, wr_t, wg_t, wu_t, w_dn, collective_id):
    rows_loc, width = x_loc.shape
    n_chunks, n_tok, n_exp = mask.shape
    n_ff = wg_t.shape[0]
    step_cols = n_ff // n_exp * EXP_PER_STEP
    rows = rows_loc // n_chunks
    const = lambda k, s: (0, 0)
    return pl.pallas_call(
        functools.partial(moe_kernel, n_chunks, EXP_PER_STEP),
        grid=(n_chunks, n_ff // step_cols),
        in_specs=[
            pl.BlockSpec(ctx.shape, lambda k, s: (0, 0, 0)),
            pl.BlockSpec(w_out.shape, const),
            pl.BlockSpec((rows_loc, width), const),
            pl.BlockSpec((1, width), const),
            pl.BlockSpec((1, n_tok, n_exp), lambda k, s: (k, 0, 0)),
            pl.BlockSpec((n_exp, width), const),
            pl.BlockSpec((step_cols, width), lambda k, s: (s, 0)),
            pl.BlockSpec((step_cols, width), lambda k, s: (s, 0)),
            pl.BlockSpec((step_cols, width), lambda k, s: (s, 0)),
        ],
        out_specs=pl.BlockSpec((rows_loc, width), const),
        out_shape=jax.ShapeDtypeStruct((rows_loc, width), jnp.bfloat16),
        scratch_shapes=[
            pltpu.VMEM((n_tok, width), jnp.float32),
            pltpu.VMEM((n_exp // EXP_PER_STEP, n_tok, EXP_PER_STEP), jnp.float32),
            pltpu.VMEM((n_chunks, n_tok, width), jnp.bfloat16),
            pltpu.VMEM((n_chunks, n_tok, width), jnp.bfloat16),
            pltpu.VMEM((rows, width), jnp.float32),
            pltpu.VMEM((rows_loc, width), jnp.bfloat16),
            pltpu.VMEM((rows_loc, width), jnp.bfloat16),
        ] + chunk_bufs(n_chunks, rows, width) + chunk_sems(Scatter, n_chunks) + chunk_sems(Scatter, n_chunks) + chunk_sems(Gather, n_chunks),
        compiler_params=pltpu.CompilerParams(dimension_semantics=("arbitrary", "arbitrary"), collective_id=collective_id, has_side_effects=True, vmem_limit_bytes=VMEM_LIMIT),
        name="moe_layer",
    )(ctx, w_out, x_loc, gain.reshape(1, width), mask, wr_t, wg_t, wu_t, w_dn)


def solution(mesh):
    tp_size = mesh.shape["tp"]
    in_specs = (P("dp", None), P("dp", None, None), P("tp", None), P(None), P(None, "tp"), P(None, "tp"), P(None, "tp"), P("tp", None), P("tp"), P("tp"), P(None), P(None, None), P(None, None, "tp"), P(None, None, "tp"), P(None, "tp", None))

    def device_fn(token_ids, route_idx, embed_table, attn_norm, w_query, w_key, w_value, w_out, q_gain, k_gain, mlp_norm, w_router, w_gate, w_up, w_down):
        batch_loc, seq_len = token_ids.shape
        vocab_loc, model_dim = embed_table.shape
        tp_rank = lax.axis_index("tp")
        local_ids = token_ids - tp_rank * vocab_loc
        in_range = (local_ids >= 0) & (local_ids < vocab_loc)
        looked_up = jnp.take(embed_table, jnp.clip(local_ids, 0, vocab_loc - 1).reshape(-1), axis=0, mode="clip")
        x_loc, a_loc = scatter_rows(looked_up, in_range.astype(jnp.float32), attn_norm, 0)
        cos_tab, sin_tab = rope_tables(seq_len)
        as_column = lambda gain: gain.astype(jnp.float32).reshape(-1, 1)
        context = attend_rows(a_loc, w_query, w_key, w_value, as_column(q_gain), as_column(k_gain), cos_tab.T, sin_tab.T, 1)
        n_exp = w_gate.shape[0]
        wg_t = jnp.swapaxes(w_gate, 1, 2).reshape(-1, model_dim)
        wu_t = jnp.swapaxes(w_up, 1, 2).reshape(-1, model_dim)
        w_dn = w_down.reshape(-1, model_dim)
        wr_t = w_router.T
        expert_iota = jnp.arange(n_exp, dtype=jnp.int32)
        chosen = route_idx.reshape(batch_loc * seq_len, -1)
        mask = jnp.any(chosen[:, :, None] == expert_iota[None, None, :], axis=1).astype(jnp.float32)
        rows_chunk = x_loc.shape[0] // N_CHUNKS
        to_chunks = lambda arr: arr.reshape(tp_size, N_CHUNKS, rows_chunk, -1).swapaxes(0, 1).reshape(N_CHUNKS, tp_size * rows_chunk, -1)
        out_loc = moe_layer(context, w_out, x_loc, mlp_norm, to_chunks(mask), wr_t, wg_t, wu_t, w_dn, 4)
        return out_loc.reshape(batch_loc, -1, model_dim)

    return jax.shard_map(device_fn, mesh=mesh, in_specs=in_specs, out_specs=P("dp", "tp", None), check_vma=False)
```

```python
import functools

import jax
import jax.numpy as jnp
import numpy as np
from jax import lax
from jax.experimental import pallas as pl
from jax.experimental.pallas import tpu as pltpu
from jax.sharding import PartitionSpec as P

HEAD_DIM = 128
NORM_EPS = 1e-5
N_CHUNKS = 4
EXP_PER_STEP = 8
VMEM_LIMIT = 63 * 1024 * 1024


def rope_tables(seq_len):
    half_dim = HEAD_DIM // 2
    inv_freq = np.float32(1.0) / (np.float32(10000.0) ** (np.arange(half_dim, dtype=np.float32) * np.float32(2.0 / HEAD_DIM)))
    angles = (inv_freq[:, None] * np.arange(seq_len, dtype=np.float32)[None, :]).astype(np.float32)
    return np.cos(angles).astype(np.float32), np.sin(angles).astype(np.float32)


N_STAGES = 6
DOWN_COLS = 256
HOT_COLS = 256
N_Z, N_Y = 4, 2
GATHER_LAST = 8
MESH = pl.DeviceIdType.MESH


class Place:
    def __init__(self):
        self.me = lax.axis_index("tp")
        self.z = self.me // 4
        self.y = self.me % 4 // 2
        self.c = self.me % 2
        self.core_peer = self.me + 1 - 2 * self.c
        self.y_peer = self.me + 2 - 4 * self.y
        self.up = self.me + 4
        self.down = self.me - 4

    def index(self, zz, yy, cc):
        return zz * 4 + yy * 2 + cc


def remote(src, dst, send_sem, recv_sem, device):
    return pltpu.make_async_remote_copy(src_ref=src, dst_ref=dst, send_sem=send_sem, recv_sem=recv_sem, device_id={"tp": device}, device_id_type=MESH)


def entry_barrier(place):
    barrier = pltpu.get_barrier_semaphore()
    for peer in (place.core_peer, place.y_peer):
        pl.semaphore_signal(barrier, inc=1, device_id={"tp": peer}, device_id_type=MESH)

    @pl.when(place.z > 0)
    def _():
        pl.semaphore_signal(barrier, inc=1, device_id={"tp": place.down}, device_id_type=MESH)

    @pl.when(place.z < N_Z - 1)
    def _():
        pl.semaphore_signal(barrier, inc=1, device_id={"tp": place.up}, device_id_type=MESH)

    pl.semaphore_wait(barrier, 2 + (place.z + 3) // 4 + (6 - place.z) // 4)


def by_distance(place, dist, act):
    if dist == 0:
        act(place.z)
        return

    @pl.when(place.z + dist < N_Z)
    def _():
        act(place.z + dist)

    @pl.when(place.z >= dist)
    def _():
        act(place.z - dist)


class Gather:
    SEMS = [(4,), (4,), (4,), (4,), (4,), (8,), (8,)]

    def __init__(self, place, own, shard, sems):
        self.place, self.own, self.shard = place, own, shard
        self.up_send, self.down_send, self.z_recv, self.y_send, self.y_recv, self.c_send, self.c_recv = sems

    def src(self, d, k, mine):
        return self.own(k) if mine else self.shard(d, k)

    def to_up(self, zz, k, mine=False):
        d = self.place.index(zz, self.place.y, self.place.c)
        return remote(self.src(d, k, mine), self.shard(d, k), self.up_send.at[k, zz], self.z_recv.at[k, zz], self.place.up)

    def to_down(self, zz, k, mine=False):
        d = self.place.index(zz, self.place.y, self.place.c)
        return remote(self.src(d, k, mine), self.shard(d, k), self.down_send.at[k, zz], self.z_recv.at[k, zz], self.place.down)

    def to_y(self, zz, k, mine=False, flip=False):
        d = self.place.index(zz, 1 - self.place.y if flip else self.place.y, self.place.c)
        return remote(self.src(d, k, mine), self.shard(d, k), self.y_send.at[k, zz], self.y_recv.at[k, zz], self.place.y_peer)

    def to_core(self, zz, yy, k, mine=False, flip=False):
        d = self.place.index(zz, yy, 1 - self.place.c if flip else self.place.c)
        slot = zz * 2 + yy
        return remote(self.src(d, k, mine), self.shard(d, k), self.c_send.at[k, slot], self.c_recv.at[k, slot], self.place.core_peer)

    def stage(self, number, k):
        place = self.place
        z, y = place.z, place.y
        if number == 0:
            @pl.when(z < N_Z - 1)
            def _():
                self.to_up(z, k, True).start()

            @pl.when(z > 0)
            def _():
                self.to_down(z, k, True).start()

            self.to_y(z, k, True).start()
            self.to_core(z, y, k, True).start()
        elif number < N_Z:
            @pl.when(z >= number)
            def _():
                zz = z - number
                self.to_up(zz, k).wait_recv()

                @pl.when(z < N_Z - 1)
                def _():
                    self.to_up(zz, k).start()

                self.to_y(zz, k).start()
                self.to_core(zz, y, k).start()

            @pl.when(z + number < N_Z)
            def _():
                zz = z + number
                self.to_down(zz, k).wait_recv()

                @pl.when(z > 0)
                def _():
                    self.to_down(zz, k).start()

                self.to_y(zz, k).start()
                self.to_core(zz, y, k).start()
        elif number < 2 * N_Z:
            def pass_on(zz):
                self.to_y(zz, k, flip=True).wait_recv()
                self.to_core(zz, 1 - y, k).start()

            by_distance(place, number - N_Z, pass_on)
        else:
            for zz in range(N_Z):
                for yy in range(N_Y):
                    self.to_core(zz, yy, k, flip=True).wait_recv()

    def drain(self, k):
        z = self.place.z
        for zz in range(N_Z):
            @pl.when((z >= zz) & (z < N_Z - 1))
            def _():
                self.to_up(zz, k).wait_send()

            @pl.when((z <= zz) & (z > 0))
            def _():
                self.to_down(zz, k).wait_send()

            self.to_y(zz, k).wait_send()
            for yy in range(N_Y):
                self.to_core(zz, yy, k).wait_send()


class Scatter:
    SEMS = [(8,), (8,), (4,), (4,), (4,), (4,), (4,), (4,)]
    BUFS = (8, 4, 4, 4, 4, 4)

    def __init__(self, place, shard, bufs, total, sems):
        self.place, self.shard, self.total = place, shard, total
        self.c_buf, self.y_out, self.y_in, self.z_out, self.from_down, self.from_up = bufs
        self.c_send, self.c_recv, self.y_send, self.y_recv, self.up_send, self.up_recv, self.down_send, self.down_recv = sems

    def to_core(self, zz, yy, k):
        slot = zz * 2 + yy
        d = self.place.index(zz, yy, 1 - self.place.c)
        return remote(self.shard(d, k), self.c_buf.at[k, slot], self.c_send.at[k, slot], self.c_recv.at[k, slot], self.place.core_peer)

    def to_y(self, zz, k):
        return remote(self.y_out.at[k, zz], self.y_in.at[k, zz], self.y_send.at[k, zz], self.y_recv.at[k, zz], self.place.y_peer)

    def to_up(self, zz, k):
        return remote(self.z_out.at[k, zz], self.from_down.at[k, zz], self.up_send.at[k, zz], self.up_recv.at[k, zz], self.place.up)

    def to_down(self, zz, k):
        return remote(self.z_out.at[k, zz], self.from_up.at[k, zz], self.down_send.at[k, zz], self.down_recv.at[k, zz], self.place.down)

    def pair_sum(self, zz, yy, k):
        self.to_core(zz, yy, k).wait_recv()
        mine = self.shard(self.place.index(zz, yy, self.place.c), k)[...].astype(jnp.float32)
        return mine + self.c_buf[k, zz * 2 + yy].astype(jnp.float32)

    def chip_pair_sum(self, zz, k):
        both = self.pair_sum(zz, self.place.y, k)
        self.to_y(zz, k).wait_recv()
        return both + self.y_in[k, zz].astype(jnp.float32)

    def stage(self, number, k):
        place = self.place
        z, y = place.z, place.y
        if number == 0:
            for yy in (1 - y, y):
                for zz in range(N_Z):
                    self.to_core(zz, yy, k).start()
        elif number == 1:
            def send_y(zz):
                self.y_out[k, zz] = self.pair_sum(zz, 1 - y, k).astype(jnp.bfloat16)
                self.to_y(zz, k).start()

            for dist in (3, 2, 1, 0):
                by_distance(place, dist, send_y)
        elif number < N_STAGES - 1:
            dist = N_STAGES - 1 - number

            @pl.when(z + dist < N_Z)
            def _():
                zz = z + dist
                self.total[...] = self.chip_pair_sum(zz, k)

                @pl.when(z > 0)
                def _():
                    self.to_up(zz, k).wait_recv()
                    self.total[...] += self.from_down[k, zz].astype(jnp.float32)

                self.z_out[k, zz] = self.total[...].astype(jnp.bfloat16)
                self.to_up(zz, k).start()

            @pl.when(z >= dist)
            def _():
                zz = z - dist
                self.total[...] = self.chip_pair_sum(zz, k)

                @pl.when(z < N_Z - 1)
                def _():
                    self.to_down(zz, k).wait_recv()
                    self.total[...] += self.from_up[k, zz].astype(jnp.float32)

                self.z_out[k, zz] = self.total[...].astype(jnp.bfloat16)
                self.to_down(zz, k).start()
        else:
            self.total[...] = self.chip_pair_sum(z, k)

            @pl.when(z > 0)
            def _():
                self.to_up(z, k).wait_recv()
                self.total[...] += self.from_down[k, z].astype(jnp.float32)

            @pl.when(z < N_Z - 1)
            def _():
                self.to_down(z, k).wait_recv()
                self.total[...] += self.from_up[k, z].astype(jnp.float32)

    def drain(self, k):
        z = self.place.z
        for zz in range(N_Z):
            for yy in range(N_Y):
                self.to_core(zz, yy, k).wait_send()
            self.to_y(zz, k).wait_send()

            @pl.when(z < zz)
            def _():
                self.to_up(zz, k).wait_send()

            @pl.when(z > zz)
            def _():
                self.to_down(zz, k).wait_send()


def chunk_sems(kind, n_chunks):
    return [pltpu.SemaphoreType.DMA((n_chunks,) + shape) for shape in kind.SEMS]


def chunk_bufs(n_chunks, rows, width):
    return [pltpu.VMEM((n_chunks, slots, rows, width), jnp.bfloat16) for slots in Scatter.BUFS]


def norm_rows(rows_f32, gain_f32):
    mean_sq = jnp.mean(rows_f32 * rows_f32, axis=-1, keepdims=True)
    return (rows_f32 * lax.rsqrt(mean_sq + NORM_EPS) * gain_f32).astype(jnp.bfloat16)


def scatter_kernel(n_chunks, ids_ref, gain, table_ref, sum_ref, norm_ref, table, hot, part, total, table_sem, *scratch):
    bufs, sems = scratch[:6], scratch[6:]
    rows = total.shape[0]
    n_tok, vocab_pad = hot.shape
    vocab = table_ref.shape[0]
    width = table.shape[1]
    lanes = 128
    place = Place()
    chunk_rows = lambda k: pl.ds(pl.multiple_of(k * rows, rows), rows)
    scat = Scatter(place, lambda d, k: part.at[k, pl.ds(pl.multiple_of(d * rows, rows), rows), :], bufs, total, sems)
    load = pltpu.make_async_copy(table_ref, table.at[pl.ds(0, vocab), :], table_sem)
    load.start()
    table[vocab:, :] = jnp.zeros((vocab_pad - vocab, width), jnp.bfloat16)
    entry_barrier(place)

    def look_up(k):
        ids = jnp.broadcast_to(ids_ref[k], (lanes, n_tok)).T - place.me * vocab
        lane = lax.broadcasted_iota(jnp.int32, (n_tok, lanes), 1)
        for col in range(0, vocab_pad, lanes):
            in_table = lane + col < vocab if col + lanes > vocab else True
            hot[:, col:col + lanes] = jnp.where((ids == lane + col) & in_table, 1.0, 0.0).astype(jnp.bfloat16)

    def product(k):
        def columns(n, inner):
            cols = pl.ds(pl.multiple_of(n * HOT_COLS, HOT_COLS), HOT_COLS)
            part[k, :, cols] = jnp.dot(hot[...], table[:, cols], preferred_element_type=jnp.float32).astype(jnp.bfloat16)
            return inner

        lax.fori_loop(0, width // HOT_COLS, columns, 0)

    def finish(k):
        value = total[...].astype(jnp.bfloat16)
        sum_ref[chunk_rows(k), :] = value
        norm_ref[chunk_rows(k), :] = norm_rows(value.astype(jnp.float32), gain[...].astype(jnp.float32))

    def wave(t, carry):
        for number in range(N_STAGES - 1, 1, -1):
            k = t - number

            @pl.when((k >= 0) & (k < n_chunks))
            def _():
                scat.stage(number, k)
                if number == N_STAGES - 1:
                    finish(k)

        @pl.when((t >= 1) & (t - 1 < n_chunks))
        def _():
            scat.stage(1, t - 1)

        @pl.when(t < n_chunks)
        def _():
            look_up(t)

            @pl.when(t == 0)
            def _():
                load.wait()

            product(t)
            scat.stage(0, t)
        return carry

    def drain(k, carry):
        scat.drain(k)
        return carry

    lax.fori_loop(0, n_chunks + N_STAGES - 1, wave, 0)
    lax.fori_loop(0, n_chunks, drain, 0)


def scatter_rows(ids, table, gain, collective_id):
    n_dev = N_Z * N_Y * 2
    vocab, width = table.shape
    n_chunks, _, n_tok = ids.shape
    rows = n_tok // n_dev
    vocab_pad = -(-vocab // 256) * 256
    out = jax.ShapeDtypeStruct((n_chunks * rows, width), jnp.bfloat16)
    vmem = pl.BlockSpec(memory_space=pltpu.VMEM)
    return pl.pallas_call(
        functools.partial(scatter_kernel, n_chunks),
        in_specs=[vmem, vmem, pl.BlockSpec(memory_space=pl.ANY)],
        out_specs=[vmem] * 2,
        out_shape=[out, out],
        scratch_shapes=[
            pltpu.VMEM((vocab_pad, width), jnp.bfloat16),
            pltpu.VMEM((n_tok, vocab_pad), jnp.bfloat16),
            pltpu.VMEM((n_chunks, n_tok, width), jnp.bfloat16),
            pltpu.VMEM((rows, width), jnp.float32),
            pltpu.SemaphoreType.DMA,
        ] + chunk_bufs(n_chunks, rows, width) + chunk_sems(Scatter, n_chunks),
        compiler_params=pltpu.CompilerParams(collective_id=collective_id, has_side_effects=True, vmem_limit_bytes=VMEM_LIMIT),
        name="scatter_rows",
    )(ids, gain.reshape(1, width), table)


KEY_BLOCK = 512


def attend_kernel(own_ref, wq_ref, wk_ref, wv_ref, qg_ref, kg_ref, cos_ref, sin_ref, out_ref, full, w_all, q_t, k_t, v_t, q_b, k_rows, stat, slots, scores, stat_send, stat_recv, *sems):
    n_dev, rows, width = full.shape
    n_tok = n_dev * rows
    dim = HEAD_DIM
    half = dim // 2
    place = Place()
    me, z, y, c = place.me, place.z, place.y, place.c
    gath = Gather(place, lambda k: own_ref, lambda d, k: full.at[d], sems)
    barrier = pltpu.get_barrier_semaphore()
    for off in range(1, n_dev):
        pl.semaphore_signal(barrier, inc=1, device_id={"tp": (me + off) % n_dev}, device_id_type=MESH)
    pl.semaphore_wait(barrier, n_dev - 1)
    gath.stage(0, 0)
    full[me] = own_ref[...]
    for pos, w_ref in enumerate((wq_ref, wk_ref, wv_ref)):
        w_all[:, pos * dim:(pos + 1) * dim] = w_ref[...]
    packed = jnp.where(z == 0, 228, jnp.where(z == 1, 225, jnp.where(z == 2, 30, 27)))

    def event(e, carry):
        turn, kind = e // 4, e % 4
        rank = turn - (kind + 1) // 2
        valid = (rank >= 0) & (rank < N_Z)
        zz = (packed >> (2 * jnp.clip(rank, 0, N_Z - 1))) & 3

        @pl.when(valid & (kind == 0) & (zz < z))
        def _():
            gath.to_up(zz, 0).wait_recv()

            @pl.when(z < N_Z - 1)
            def _():
                gath.to_up(zz, 0).start()

        @pl.when(valid & (kind == 0) & (zz > z))
        def _():
            gath.to_down(zz, 0).wait_recv()

            @pl.when(z > 0)
            def _():
                gath.to_down(zz, 0).start()

        @pl.when(valid & (kind == 0) & (rank > 0))
        def _():
            gath.to_y(zz, 0).start()
            gath.to_core(zz, y, 0).start()

        @pl.when(valid & (kind == 1))
        def _():
            gath.to_core(zz, y, 0, flip=True).wait_recv()

        @pl.when(valid & (kind == 2))
        def _():
            gath.to_y(zz, 0, flip=True).wait_recv()
            gath.to_core(zz, 1 - y, 0).start()

        @pl.when(valid & (kind == 3))
        def _():
            gath.to_core(zz, 1 - y, 0, flip=True).wait_recv()

        @pl.when(valid)
        def _():
            d = zz * 4 + (y + kind // 2) % 2 * 2 + (c + kind) % 2
            lanes = pl.ds(pl.multiple_of(d * rows, rows), rows)
            qkv = jnp.dot(full[d], w_all[...], preferred_element_type=jnp.float32)
            q_blk, k_blk, v_blk = (qkv[:, i * dim:(i + 1) * dim].T for i in range(3))
            q_t[:, lanes] = q_blk
            k_t[:, lanes] = k_blk
            v_t[:, lanes] = v_blk.astype(jnp.bfloat16)
            stat[0:1, lanes] = jnp.sum(q_blk * q_blk, axis=0, keepdims=True)
            stat[1:2, lanes] = jnp.sum(k_blk * k_blk, axis=0, keepdims=True)
        return carry

    lax.fori_loop(0, 24, event, 0)
    gath.drain(0)

    def to_peer(off):
        return remote(stat, slots.at[me], stat_send.at[off], stat_recv.at[me], (me + off) % n_dev)

    for off in range(1, n_dev):
        to_peer(off).start()
    slots[me] = stat[...]
    for off in range(1, n_dev):
        other = (me + off) % n_dev
        remote(stat, slots.at[other], stat_send.at[off], stat_recv.at[other], other).wait_recv()
    stat_total = jnp.sum(slots[...], axis=0)
    inv_rms = lax.rsqrt(stat_total / (n_dev * dim) + NORM_EPS)
    for off in range(1, n_dev):
        to_peer(off).wait_send()
    slots[0] = inv_rms

    def rotate(blk, carry):
        lanes = pl.ds(pl.multiple_of(blk * KEY_BLOCK, KEY_BLOCK), KEY_BLOCK)
        cos_b, sin_b = cos_ref[:, lanes], sin_ref[:, lanes]
        heads = []
        for row, raw, gain in ((0, q_t, qg_ref), (1, k_t, kg_ref)):
            normed = raw[:, lanes] * slots[0, row:row + 1, lanes] * gain[...]
            first, second = normed[:half], normed[half:]
            heads.append(jnp.concatenate([first * cos_b - second * sin_b, second * cos_b + first * sin_b], axis=0))
        q_b[:, lanes] = heads[0].astype(jnp.bfloat16)
        k_rows[lanes, :] = heads[1].T.astype(jnp.bfloat16)
        return carry

    lax.fori_loop(0, n_tok // KEY_BLOCK, rotate, 0)

    def attend(blk, carry):
        queries = pl.ds(pl.multiple_of(blk * KEY_BLOCK, KEY_BLOCK), KEY_BLOCK)
        q_blk = q_b[:, queries]
        key_rows = lambda j: pl.ds(pl.multiple_of(j * KEY_BLOCK, KEY_BLOCK), KEY_BLOCK)

        def score(j, top):
            raw = jnp.dot(k_rows[key_rows(j), :], q_blk, preferred_element_type=jnp.float32) * (dim ** -0.5)
            key_pos = lax.broadcasted_iota(jnp.int32, raw.shape, 0) + (j - blk) * KEY_BLOCK
            raw = jnp.where(key_pos <= lax.broadcasted_iota(jnp.int32, raw.shape, 1), raw, -1e30)
            scores[key_rows(j), :] = raw
            return jnp.maximum(top, jnp.max(raw, axis=0, keepdims=True))

        top = lax.fori_loop(0, blk + 1, score, jnp.full((1, KEY_BLOCK), -1e30, jnp.float32))

        def expo(j, norm):
            raised = jnp.exp(scores[key_rows(j), :] - top)
            scores[key_rows(j), :] = raised
            return norm + jnp.sum(raised, axis=0, keepdims=True)

        norm = lax.fori_loop(0, blk + 1, expo, jnp.zeros((1, KEY_BLOCK), jnp.float32))
        inv_norm = 1.0 / norm

        def weigh(j, acc):
            prob = (scores[key_rows(j), :] * inv_norm).astype(jnp.bfloat16)
            return acc + jnp.dot(v_t[:, key_rows(j)], prob, preferred_element_type=jnp.float32)

        ctx = lax.fori_loop(0, blk + 1, weigh, jnp.zeros((dim, KEY_BLOCK), jnp.float32)).T.astype(jnp.bfloat16)
        n_chunks = out_ref.shape[0]
        piece = rows // n_chunks
        for dev in range(KEY_BLOCK // rows):
            at = pl.ds(pl.multiple_of((blk * (KEY_BLOCK // rows) + dev) * piece, piece), piece)
            for k in range(n_chunks):
                out_ref[k, at, :] = ctx[dev * rows + k * piece:dev * rows + (k + 1) * piece, :]
        return carry

    lax.fori_loop(0, n_tok // KEY_BLOCK, attend, 0)


def attend_rows(own, wq, wk, wv, q_gain, k_gain, cos_t, sin_t, collective_id):
    n_dev = N_Z * N_Y * 2
    rows, width = own.shape
    n_tok = n_dev * rows
    operands = (own, wq, wk, wv, q_gain, k_gain, cos_t, sin_t)
    return pl.pallas_call(
        attend_kernel,
        in_specs=[pl.BlockSpec(memory_space=pltpu.VMEM)] * len(operands),
        out_specs=pl.BlockSpec(memory_space=pltpu.VMEM),
        out_shape=jax.ShapeDtypeStruct((N_CHUNKS, n_tok // N_CHUNKS, HEAD_DIM), jnp.bfloat16),
        scratch_shapes=[
            pltpu.VMEM((n_dev, rows, width), jnp.bfloat16),
            pltpu.VMEM((width, 3 * HEAD_DIM), jnp.bfloat16),
            pltpu.VMEM((HEAD_DIM, n_tok), jnp.float32),
            pltpu.VMEM((HEAD_DIM, n_tok), jnp.float32),
            pltpu.VMEM((HEAD_DIM, n_tok), jnp.bfloat16),
            pltpu.VMEM((HEAD_DIM, n_tok), jnp.bfloat16),
            pltpu.VMEM((n_tok, HEAD_DIM), jnp.bfloat16),
            pltpu.VMEM((2, n_tok), jnp.float32),
            pltpu.VMEM((n_dev, 2, n_tok), jnp.float32),
            pltpu.VMEM((n_tok, KEY_BLOCK), jnp.float32),
            pltpu.SemaphoreType.DMA((n_dev,)),
            pltpu.SemaphoreType.DMA((n_dev,)),
        ] + chunk_sems(Gather, 1),
        compiler_params=pltpu.CompilerParams(collective_id=collective_id, has_side_effects=True, vmem_limit_bytes=VMEM_LIMIT),
        name="attend_rows",
    )(*operands)


SUM_STEPS = {0: 0, 1: 1, 3: 2, 4: 3, 5: 4, 6: 5}


def moe_kernel(n_chunks, exp_step, ctx_ref, wo_ref, x_ref, gain_ref, mask_ref, wr_ref, wg_ref, wu_ref, wd_ref, out_ref, acc_ref, gate_ref, full, part, total, m_own, h_own, *rest):
    bufs, rest = rest[:6], rest[6:]
    n_sc = len(Scatter.SEMS)
    attn_sems, moe_sems, gather_sems = rest[:n_sc], rest[n_sc:2 * n_sc], rest[2 * n_sc:]
    chunk, step = pl.program_id(0), pl.program_id(1)
    n_steps = pl.num_programs(1)
    rows = m_own.shape[0] // n_chunks
    n_exp = wr_ref.shape[0]
    exp_ff = wg_ref.shape[0] // exp_step
    n_tok = full.shape[1]
    nt_dims = (((1,), (1,)), ((), ()))
    place = Place()
    loc_rows = lambda k: pl.ds(pl.multiple_of(k * rows, rows), rows)
    block = lambda ref: (lambda d, k: ref.at[k, pl.ds(pl.multiple_of(d * rows, rows), rows), :])
    gath = Gather(place, lambda k: m_own.at[loc_rows(k), :], block(full), gather_sems)
    attn = Scatter(place, block(part), bufs, total, attn_sems)
    scat = Scatter(place, block(part), bufs, total, moe_sems)

    def project(k):
        part[k] = jnp.dot(ctx_ref[k], wo_ref[...], preferred_element_type=jnp.float32).astype(jnp.bfloat16)

    def attn_stage(number, k):
        attn.stage(number, k)
        if number == N_STAGES - 1:
            attn_out = total[...].astype(jnp.bfloat16).astype(jnp.float32)
            hidden = (x_ref[loc_rows(k), :].astype(jnp.float32) + attn_out).astype(jnp.bfloat16)
            h_own[loc_rows(k), :] = hidden
            normed = norm_rows(hidden.astype(jnp.float32), gain_ref[...].astype(jnp.float32))
            m_own[loc_rows(k), :] = normed
            full[k, pl.ds(pl.multiple_of(place.me * rows, rows), rows), :] = normed

    def moe_stage(number, k):
        scat.stage(number, k)
        if number == N_STAGES - 1:
            moe_out = total[...].astype(jnp.bfloat16).astype(jnp.float32)
            out_ref[loc_rows(k), :] = (h_own[loc_rows(k), :].astype(jnp.float32) + moe_out).astype(jnp.bfloat16)

    @pl.when((chunk == 0) & (step == 0))
    def _():
        entry_barrier(place)
        for k in (0, 1):
            project(k)
            attn_stage(0, k)
        attn_stage(1, 0)
        for k in range(2, n_chunks):
            project(k)
            attn_stage(0, k)
        attn_stage(1, 1)
        for number in range(2, N_STAGES):
            attn_stage(number, 0)
        attn_stage(2, 1)
        gath.stage(0, 0)
        attn_stage(3, 1)
        for number in (1, 4):
            gath.stage(number, 0)
        attn_stage(4, 1)
        for number in (2, 5):
            gath.stage(number, 0)
        attn_stage(5, 1)
        for number in (3, 6, 7, 8):
            gath.stage(number, 0)

    for at in range(2 * N_Z):
        @pl.when((step == at) & (chunk + 1 < n_chunks))
        def _():
            gath.stage(at, chunk + 1)

        if at in SUM_STEPS:
            @pl.when((step == at) & (chunk > 0))
            def _():
                moe_stage(SUM_STEPS[at], chunk - 1)

            if at > 0:
                @pl.when((step == at) & (chunk == 0))
                def _():
                    attn_stage(SUM_STEPS[at], 2)

    for at_chunk, at, number in ((0, 5, 1), (0, 7, 2), (1, 0, 3), (1, 1, 4), (1, 2, 5)):
        @pl.when((step == at) & (chunk == at_chunk))
        def _():
            attn_stage(number, 3)

    @pl.when((step == 0) & (chunk > 0))
    def _():
        gath.stage(GATHER_LAST, chunk)

    @pl.when(step == 0)
    def _():
        logits = lax.dot_general(full[chunk], wr_ref[...], nt_dims, preferred_element_type=jnp.float32)
        logits = logits - jnp.max(logits, axis=-1, keepdims=True)
        expd = jnp.exp(logits)
        gates = expd / jnp.sum(expd, axis=-1, keepdims=True) * mask_ref[0]
        for grp in range(n_exp // exp_step):
            gate_ref[grp] = gates[:, grp * exp_step:(grp + 1) * exp_step]
        acc_ref[...] = jnp.zeros_like(acc_ref)

    m_rows = full[chunk]
    gate_proj = lax.dot_general(m_rows, wg_ref[...], nt_dims, preferred_element_type=jnp.float32)
    up_proj = lax.dot_general(m_rows, wu_ref[...], nt_dims, preferred_element_type=jnp.float32)
    act = (gate_proj / (1.0 + jnp.exp(-gate_proj)) * up_proj).astype(jnp.bfloat16).astype(jnp.float32)
    gates = gate_ref[step]
    lane = lax.broadcasted_iota(jnp.int32, (n_tok, 2 * exp_ff), 1)
    pieces = []
    for pair in range(exp_step // 2):
        pieces.append(jnp.where(lane < exp_ff, gates[:, 2 * pair:2 * pair + 1], gates[:, 2 * pair + 1:2 * pair + 2]))
    scaled = act * jnp.concatenate(pieces, axis=1)
    high = scaled.astype(jnp.bfloat16)
    low = (scaled - high.astype(jnp.float32)).astype(jnp.bfloat16)
    both = jnp.concatenate([high, low], axis=0)
    for col in range(0, acc_ref.shape[1], DOWN_COLS):
        cols = slice(col, col + DOWN_COLS)
        down = jnp.dot(both, wd_ref[:, cols], preferred_element_type=jnp.float32)
        acc_ref[:, cols] += down[:n_tok] + down[n_tok:]

    @pl.when(step == n_steps - 1)
    def _():
        attn.drain(chunk)
        part[chunk] = acc_ref[...].astype(jnp.bfloat16)

    @pl.when((step == n_steps - 1) & (chunk == n_chunks - 1))
    def _():
        for number in range(N_STAGES):
            moe_stage(number, n_chunks - 1)

        def drain(k, carry):
            gath.drain(k)
            scat.drain(k)
            return carry

        lax.fori_loop(0, n_chunks, drain, 0)


def moe_layer(ctx, w_out, x_loc, gain, mask, wr_t, wg_t, wu_t, w_dn, collective_id):
    rows_loc, width = x_loc.shape
    n_chunks, n_tok, n_exp = mask.shape
    n_ff = wg_t.shape[0]
    step_cols = n_ff // n_exp * EXP_PER_STEP
    rows = rows_loc // n_chunks
    const = lambda k, s: (0, 0)
    return pl.pallas_call(
        functools.partial(moe_kernel, n_chunks, EXP_PER_STEP),
        grid=(n_chunks, n_ff // step_cols),
        in_specs=[
            pl.BlockSpec(ctx.shape, lambda k, s: (0, 0, 0)),
            pl.BlockSpec(w_out.shape, const),
            pl.BlockSpec((rows_loc, width), const),
            pl.BlockSpec((1, width), const),
            pl.BlockSpec((1, n_tok, n_exp), lambda k, s: (k, 0, 0)),
            pl.BlockSpec((n_exp, width), const),
            pl.BlockSpec((step_cols, width), lambda k, s: (s, 0)),
            pl.BlockSpec((step_cols, width), lambda k, s: (s, 0)),
            pl.BlockSpec((step_cols, width), lambda k, s: (s, 0)),
        ],
        out_specs=pl.BlockSpec((rows_loc, width), const),
        out_shape=jax.ShapeDtypeStruct((rows_loc, width), jnp.bfloat16),
        scratch_shapes=[
            pltpu.VMEM((n_tok, width), jnp.float32),
            pltpu.VMEM((n_exp // EXP_PER_STEP, n_tok, EXP_PER_STEP), jnp.float32),
            pltpu.VMEM((n_chunks, n_tok, width), jnp.bfloat16),
            pltpu.VMEM((n_chunks, n_tok, width), jnp.bfloat16),
            pltpu.VMEM((rows, width), jnp.float32),
            pltpu.VMEM((rows_loc, width), jnp.bfloat16),
            pltpu.VMEM((rows_loc, width), jnp.bfloat16),
        ] + chunk_bufs(n_chunks, rows, width) + chunk_sems(Scatter, n_chunks) + chunk_sems(Scatter, n_chunks) + chunk_sems(Gather, n_chunks),
        compiler_params=pltpu.CompilerParams(dimension_semantics=("arbitrary", "arbitrary"), collective_id=collective_id, has_side_effects=True, vmem_limit_bytes=VMEM_LIMIT),
        name="moe_layer",
    )(ctx, w_out, x_loc, gain.reshape(1, width), mask, wr_t, wg_t, wu_t, w_dn)


def solution(mesh):
    tp_size = mesh.shape["tp"]
    in_specs = (P("dp", None), P("dp", None, None), P("tp", None), P(None), P(None, "tp"), P(None, "tp"), P(None, "tp"), P("tp", None), P("tp"), P("tp"), P(None), P(None, None), P(None, None, "tp"), P(None, None, "tp"), P(None, "tp", None))

    def device_fn(token_ids, route_idx, embed_table, attn_norm, w_query, w_key, w_value, w_out, q_gain, k_gain, mlp_norm, w_router, w_gate, w_up, w_down):
        batch_loc, seq_len = token_ids.shape
        model_dim = embed_table.shape[1]
        ids = token_ids.reshape(tp_size, N_CHUNKS, -1).swapaxes(0, 1).reshape(N_CHUNKS, 1, -1)
        x_loc, a_loc = scatter_rows(ids, embed_table, attn_norm, 0)
        cos_t, sin_t = (jnp.asarray(tab) for tab in rope_tables(seq_len))
        as_column = lambda gain: gain.astype(jnp.float32).reshape(-1, 1)
        context = attend_rows(a_loc, w_query, w_key, w_value, as_column(q_gain), as_column(k_gain), cos_t, sin_t, 1)
        n_exp = w_gate.shape[0]
        wg_t = jnp.swapaxes(w_gate, 1, 2).reshape(-1, model_dim)
        wu_t = jnp.swapaxes(w_up, 1, 2).reshape(-1, model_dim)
        w_dn = w_down.reshape(-1, model_dim)
        wr_t = w_router.T
        expert_iota = jnp.arange(n_exp, dtype=jnp.int32)
        chosen = route_idx.reshape(batch_loc * seq_len, -1)
        mask = jnp.any(chosen[:, :, None] == expert_iota[None, None, :], axis=1).astype(jnp.float32)
        rows_chunk = x_loc.shape[0] // N_CHUNKS
        to_chunks = lambda arr: arr.reshape(tp_size, N_CHUNKS, rows_chunk, -1).swapaxes(0, 1).reshape(N_CHUNKS, tp_size * rows_chunk, -1)
        out_loc = moe_layer(context, w_out, x_loc, mlp_norm, to_chunks(mask), wr_t, wg_t, wu_t, w_dn, 4)
        return out_loc.reshape(batch_loc, -1, model_dim)

    return jax.shard_map(device_fn, mesh=mesh, in_specs=in_specs, out_specs=P("dp", "tp", None), check_vma=False)
```

```python
import functools

import jax
import jax.numpy as jnp
import numpy as np
from jax import lax
from jax.experimental import pallas as pl
from jax.experimental.pallas import tpu as pltpu
from jax.sharding import PartitionSpec as P

HEAD_DIM = 128
NORM_EPS = 1e-5
N_CHUNKS = 8
EXP_PER_STEP = 8
VMEM_LIMIT = 63 * 1024 * 1024


def rope_tables(seq_len):
    half_dim = HEAD_DIM // 2
    inv_freq = np.float32(1.0) / (np.float32(10000.0) ** (np.arange(half_dim, dtype=np.float32) * np.float32(2.0 / HEAD_DIM)))
    angles = (inv_freq[:, None] * np.arange(seq_len, dtype=np.float32)[None, :]).astype(np.float32)
    return np.cos(angles).astype(np.float32), np.sin(angles).astype(np.float32)


N_STAGES = 6
DOWN_COLS = 256
HOT_COLS = 256
N_Z, N_Y = 4, 2
GATHER_LAST = 8
MESH = pl.DeviceIdType.MESH


class Place:
    def __init__(self):
        self.me = lax.axis_index("tp")
        self.z = self.me // 4
        self.y = self.me % 4 // 2
        self.c = self.me % 2
        self.core_peer = self.me + 1 - 2 * self.c
        self.y_peer = self.me + 2 - 4 * self.y
        self.up = self.me + 4
        self.down = self.me - 4

    def index(self, zz, yy, cc):
        return zz * 4 + yy * 2 + cc


def remote(src, dst, send_sem, recv_sem, device):
    return pltpu.make_async_remote_copy(src_ref=src, dst_ref=dst, send_sem=send_sem, recv_sem=recv_sem, device_id={"tp": device}, device_id_type=MESH)


def entry_barrier(place):
    barrier = pltpu.get_barrier_semaphore()
    for peer in (place.core_peer, place.y_peer):
        pl.semaphore_signal(barrier, inc=1, device_id={"tp": peer}, device_id_type=MESH)

    @pl.when(place.z > 0)
    def _():
        pl.semaphore_signal(barrier, inc=1, device_id={"tp": place.down}, device_id_type=MESH)

    @pl.when(place.z < N_Z - 1)
    def _():
        pl.semaphore_signal(barrier, inc=1, device_id={"tp": place.up}, device_id_type=MESH)

    pl.semaphore_wait(barrier, 2 + (place.z + 3) // 4 + (6 - place.z) // 4)


def by_distance(place, dist, act):
    if dist == 0:
        act(place.z)
        return

    @pl.when(place.z + dist < N_Z)
    def _():
        act(place.z + dist)

    @pl.when(place.z >= dist)
    def _():
        act(place.z - dist)


class Gather:
    SEMS = [(4,), (4,), (4,), (4,), (4,), (8,), (8,)]

    def __init__(self, place, own, shard, sems):
        self.place, self.own, self.shard = place, own, shard
        self.up_send, self.down_send, self.z_recv, self.y_send, self.y_recv, self.c_send, self.c_recv = sems

    def src(self, d, k, mine):
        return self.own(k) if mine else self.shard(d, k)

    def to_up(self, zz, k, mine=False):
        d = self.place.index(zz, self.place.y, self.place.c)
        return remote(self.src(d, k, mine), self.shard(d, k), self.up_send.at[k, zz], self.z_recv.at[k, zz], self.place.up)

    def to_down(self, zz, k, mine=False):
        d = self.place.index(zz, self.place.y, self.place.c)
        return remote(self.src(d, k, mine), self.shard(d, k), self.down_send.at[k, zz], self.z_recv.at[k, zz], self.place.down)

    def to_y(self, zz, k, mine=False, flip=False):
        d = self.place.index(zz, 1 - self.place.y if flip else self.place.y, self.place.c)
        return remote(self.src(d, k, mine), self.shard(d, k), self.y_send.at[k, zz], self.y_recv.at[k, zz], self.place.y_peer)

    def to_core(self, zz, yy, k, mine=False, flip=False):
        d = self.place.index(zz, yy, 1 - self.place.c if flip else self.place.c)
        slot = zz * 2 + yy
        return remote(self.src(d, k, mine), self.shard(d, k), self.c_send.at[k, slot], self.c_recv.at[k, slot], self.place.core_peer)

    def stage(self, number, k):
        place = self.place
        z, y = place.z, place.y
        if number == 0:
            @pl.when(z < N_Z - 1)
            def _():
                self.to_up(z, k, True).start()

            @pl.when(z > 0)
            def _():
                self.to_down(z, k, True).start()

            self.to_y(z, k, True).start()
            self.to_core(z, y, k, True).start()
        elif number < N_Z:
            @pl.when(z >= number)
            def _():
                zz = z - number
                self.to_up(zz, k).wait_recv()

                @pl.when(z < N_Z - 1)
                def _():
                    self.to_up(zz, k).start()

                self.to_y(zz, k).start()
                self.to_core(zz, y, k).start()

            @pl.when(z + number < N_Z)
            def _():
                zz = z + number
                self.to_down(zz, k).wait_recv()

                @pl.when(z > 0)
                def _():
                    self.to_down(zz, k).start()

                self.to_y(zz, k).start()
                self.to_core(zz, y, k).start()
        elif number < 2 * N_Z:
            def pass_on(zz):
                self.to_y(zz, k, flip=True).wait_recv()
                self.to_core(zz, 1 - y, k).start()

            by_distance(place, number - N_Z, pass_on)
        else:
            for zz in range(N_Z):
                for yy in range(N_Y):
                    self.to_core(zz, yy, k, flip=True).wait_recv()

    def drain(self, k):
        z = self.place.z
        for zz in range(N_Z):
            @pl.when((z >= zz) & (z < N_Z - 1))
            def _():
                self.to_up(zz, k).wait_send()

            @pl.when((z <= zz) & (z > 0))
            def _():
                self.to_down(zz, k).wait_send()

            self.to_y(zz, k).wait_send()
            for yy in range(N_Y):
                self.to_core(zz, yy, k).wait_send()


class Scatter:
    SEMS = [(8,), (8,), (4,), (4,), (4,), (4,), (4,), (4,)]
    BUFS = (8, 4, 4, 4, 4, 4)

    def __init__(self, place, shard, bufs, total, sems):
        self.place, self.shard, self.total = place, shard, total
        self.c_buf, self.y_out, self.y_in, self.z_out, self.from_down, self.from_up = bufs
        self.c_send, self.c_recv, self.y_send, self.y_recv, self.up_send, self.up_recv, self.down_send, self.down_recv = sems

    def to_core(self, zz, yy, k):
        slot = zz * 2 + yy
        d = self.place.index(zz, yy, 1 - self.place.c)
        return remote(self.shard(d, k), self.c_buf.at[k, slot], self.c_send.at[k, slot], self.c_recv.at[k, slot], self.place.core_peer)

    def to_y(self, zz, k):
        return remote(self.y_out.at[k, zz], self.y_in.at[k, zz], self.y_send.at[k, zz], self.y_recv.at[k, zz], self.place.y_peer)

    def to_up(self, zz, k):
        return remote(self.z_out.at[k, zz], self.from_down.at[k, zz], self.up_send.at[k, zz], self.up_recv.at[k, zz], self.place.up)

    def to_down(self, zz, k):
        return remote(self.z_out.at[k, zz], self.from_up.at[k, zz], self.down_send.at[k, zz], self.down_recv.at[k, zz], self.place.down)

    def pair_sum(self, zz, yy, k):
        self.to_core(zz, yy, k).wait_recv()
        mine = self.shard(self.place.index(zz, yy, self.place.c), k)[...].astype(jnp.float32)
        return mine + self.c_buf[k, zz * 2 + yy].astype(jnp.float32)

    def chip_pair_sum(self, zz, k):
        both = self.pair_sum(zz, self.place.y, k)
        self.to_y(zz, k).wait_recv()
        return both + self.y_in[k, zz].astype(jnp.float32)

    def stage(self, number, k):
        place = self.place
        z, y = place.z, place.y
        if number == 0:
            for yy in (1 - y, y):
                for zz in range(N_Z):
                    self.to_core(zz, yy, k).start()
        elif number == 1:
            def send_y(zz):
                self.y_out[k, zz] = self.pair_sum(zz, 1 - y, k).astype(jnp.bfloat16)
                self.to_y(zz, k).start()

            for dist in (3, 2, 1, 0):
                by_distance(place, dist, send_y)
        elif number < N_STAGES - 1:
            dist = N_STAGES - 1 - number

            @pl.when(z + dist < N_Z)
            def _():
                zz = z + dist
                self.total[...] = self.chip_pair_sum(zz, k)

                @pl.when(z > 0)
                def _():
                    self.to_up(zz, k).wait_recv()
                    self.total[...] += self.from_down[k, zz].astype(jnp.float32)

                self.z_out[k, zz] = self.total[...].astype(jnp.bfloat16)
                self.to_up(zz, k).start()

            @pl.when(z >= dist)
            def _():
                zz = z - dist
                self.total[...] = self.chip_pair_sum(zz, k)

                @pl.when(z < N_Z - 1)
                def _():
                    self.to_down(zz, k).wait_recv()
                    self.total[...] += self.from_up[k, zz].astype(jnp.float32)

                self.z_out[k, zz] = self.total[...].astype(jnp.bfloat16)
                self.to_down(zz, k).start()
        else:
            self.total[...] = self.chip_pair_sum(z, k)

            @pl.when(z > 0)
            def _():
                self.to_up(z, k).wait_recv()
                self.total[...] += self.from_down[k, z].astype(jnp.float32)

            @pl.when(z < N_Z - 1)
            def _():
                self.to_down(z, k).wait_recv()
                self.total[...] += self.from_up[k, z].astype(jnp.float32)

    def drain(self, k):
        z = self.place.z
        for zz in range(N_Z):
            for yy in range(N_Y):
                self.to_core(zz, yy, k).wait_send()
            self.to_y(zz, k).wait_send()

            @pl.when(z < zz)
            def _():
                self.to_up(zz, k).wait_send()

            @pl.when(z > zz)
            def _():
                self.to_down(zz, k).wait_send()


def chunk_sems(kind, n_chunks):
    return [pltpu.SemaphoreType.DMA((n_chunks,) + shape) for shape in kind.SEMS]


def chunk_bufs(n_chunks, rows, width):
    return [pltpu.VMEM((n_chunks, slots, rows, width), jnp.bfloat16) for slots in Scatter.BUFS]


def norm_rows(rows_f32, gain_f32):
    mean_sq = jnp.mean(rows_f32 * rows_f32, axis=-1, keepdims=True)
    return (rows_f32 * lax.rsqrt(mean_sq + NORM_EPS) * gain_f32).astype(jnp.bfloat16)


def scatter_kernel(n_chunks, ids_ref, gain, table_ref, sum_ref, norm_ref, table, hot, part, total, id_cols, table_sem, *scratch):
    bufs, sems = scratch[:6], scratch[6:]
    rows = total.shape[0]
    n_tok, vocab_pad = hot.shape
    vocab = table_ref.shape[0]
    width = table.shape[1]
    lanes = 128
    place = Place()
    chunk_rows = lambda k: pl.ds(pl.multiple_of(k * rows, rows), rows)
    scat = Scatter(place, lambda d, k: part.at[k, pl.ds(pl.multiple_of(d * rows, rows), rows), :], bufs, total, sems)
    load = pltpu.make_async_copy(table_ref, table.at[pl.ds(0, vocab), :], table_sem)
    load.start()
    for d in range(n_tok // rows):
        span = slice(d * rows * n_chunks, (d + 1) * rows * n_chunks)
        id_cols[d] = jnp.broadcast_to(ids_ref[:, span], (lanes, rows * n_chunks)).T
    table[vocab:, :] = jnp.zeros((vocab_pad - vocab, width), jnp.bfloat16)
    entry_barrier(place)

    def look_up(k):
        ids = jnp.concatenate([id_cols[d, chunk_rows(k), :] for d in range(n_tok // rows)], axis=0) - place.me * vocab
        lane = lax.broadcasted_iota(jnp.int32, (n_tok, lanes), 1)
        for col in range(0, vocab_pad, lanes):
            in_table = lane + col < vocab if col + lanes > vocab else True
            hot[:, col:col + lanes] = jnp.where((ids == lane + col) & in_table, 1.0, 0.0).astype(jnp.bfloat16)

    def product(k):
        def columns(n, inner):
            cols = pl.ds(pl.multiple_of(n * HOT_COLS, HOT_COLS), HOT_COLS)
            part[k, :, cols] = jnp.dot(hot[...], table[:, cols], preferred_element_type=jnp.float32).astype(jnp.bfloat16)
            return inner

        lax.fori_loop(0, width // HOT_COLS, columns, 0)

    def finish(k):
        value = total[...].astype(jnp.bfloat16)
        sum_ref[chunk_rows(k), :] = value
        norm_ref[chunk_rows(k), :] = norm_rows(value.astype(jnp.float32), gain[...].astype(jnp.float32).reshape(1, -1))

    def wave(t, carry):
        for number in range(N_STAGES - 1, 1, -1):
            k = t - number

            @pl.when((k >= 0) & (k < n_chunks))
            def _():
                scat.stage(number, k)
                if number == N_STAGES - 1:
                    finish(k)

        @pl.when((t >= 1) & (t - 1 < n_chunks))
        def _():
            scat.stage(1, t - 1)

        @pl.when(t < n_chunks)
        def _():
            look_up(t)

            @pl.when(t == 0)
            def _():
                load.wait()

            product(t)
            scat.stage(0, t)
        return carry

    def drain(k, carry):
        scat.drain(k)
        return carry

    lax.fori_loop(0, n_chunks + N_STAGES - 1, wave, 0)
    lax.fori_loop(0, n_chunks, drain, 0)


def scatter_rows(ids, table, gain, collective_id):
    n_dev = N_Z * N_Y * 2
    vocab, width = table.shape
    n_chunks = N_CHUNKS
    n_tok = ids.shape[1] // n_chunks
    rows = n_tok // n_dev
    vocab_pad = -(-vocab // 256) * 256
    out = jax.ShapeDtypeStruct((n_chunks * rows, width), jnp.bfloat16)
    vmem = pl.BlockSpec(memory_space=pltpu.VMEM)
    return pl.pallas_call(
        functools.partial(scatter_kernel, n_chunks),
        in_specs=[vmem, vmem, pl.BlockSpec(memory_space=pl.ANY)],
        out_specs=[vmem] * 2,
        out_shape=[out, out],
        scratch_shapes=[
            pltpu.VMEM((vocab_pad, width), jnp.bfloat16),
            pltpu.VMEM((n_tok, vocab_pad), jnp.bfloat16),
            pltpu.VMEM((n_chunks, n_tok, width), jnp.bfloat16),
            pltpu.VMEM((rows, width), jnp.float32),
            pltpu.VMEM((n_dev, rows * n_chunks, 128), jnp.int32),
            pltpu.SemaphoreType.DMA,
        ] + chunk_bufs(n_chunks, rows, width) + chunk_sems(Scatter, n_chunks),
        compiler_params=pltpu.CompilerParams(collective_id=collective_id, has_side_effects=True, vmem_limit_bytes=VMEM_LIMIT),
        name="scatter_rows",
    )(ids, gain, table)


KEY_BLOCK = 512


def attend_kernel(own_ref, wq_ref, wk_ref, wv_ref, qg_ref, kg_ref, cos_ref, sin_ref, out_ref, full, w_all, q_t, k_t, v_t, q_b, k_rows, stat, slots, scores, stat_send, stat_recv, *sems):
    n_dev, rows, width = full.shape
    n_tok = n_dev * rows
    dim = HEAD_DIM
    half = dim // 2
    place = Place()
    me, z, y, c = place.me, place.z, place.y, place.c
    gath = Gather(place, lambda k: own_ref, lambda d, k: full.at[d], sems)
    barrier = pltpu.get_barrier_semaphore()
    for off in range(1, n_dev):
        pl.semaphore_signal(barrier, inc=1, device_id={"tp": (me + off) % n_dev}, device_id_type=MESH)
    pl.semaphore_wait(barrier, n_dev - 1)
    gath.stage(0, 0)
    full[me] = own_ref[...]
    for pos, w_ref in enumerate((wq_ref, wk_ref, wv_ref)):
        w_all[:, pos * dim:(pos + 1) * dim] = w_ref[...]
    columns = [jnp.broadcast_to(ref[...].astype(jnp.float32).reshape(1, -1), (dim, dim)).T[:, :1] for ref in (qg_ref, kg_ref)]
    packed = jnp.where(z == 0, 228, jnp.where(z == 1, 225, jnp.where(z == 2, 30, 27)))

    def event(e, carry):
        turn, kind = e // 4, e % 4
        rank = turn - (kind + 1) // 2
        valid = (rank >= 0) & (rank < N_Z)
        zz = (packed >> (2 * jnp.clip(rank, 0, N_Z - 1))) & 3

        @pl.when(valid & (kind == 0) & (zz < z))
        def _():
            gath.to_up(zz, 0).wait_recv()

            @pl.when(z < N_Z - 1)
            def _():
                gath.to_up(zz, 0).start()

        @pl.when(valid & (kind == 0) & (zz > z))
        def _():
            gath.to_down(zz, 0).wait_recv()

            @pl.when(z > 0)
            def _():
                gath.to_down(zz, 0).start()

        @pl.when(valid & (kind == 0) & (rank > 0))
        def _():
            gath.to_y(zz, 0).start()
            gath.to_core(zz, y, 0).start()

        @pl.when(valid & (kind == 1))
        def _():
            gath.to_core(zz, y, 0, flip=True).wait_recv()

        @pl.when(valid & (kind == 2))
        def _():
            gath.to_y(zz, 0, flip=True).wait_recv()
            gath.to_core(zz, 1 - y, 0).start()

        @pl.when(valid & (kind == 3))
        def _():
            gath.to_core(zz, 1 - y, 0, flip=True).wait_recv()

        @pl.when(valid)
        def _():
            d = zz * 4 + (y + kind // 2) % 2 * 2 + (c + kind) % 2
            lanes = pl.ds(pl.multiple_of(d * rows, rows), rows)
            qkv = jnp.dot(full[d], w_all[...], preferred_element_type=jnp.float32)
            q_blk, k_blk, v_blk = (qkv[:, i * dim:(i + 1) * dim].T for i in range(3))
            q_t[:, lanes] = q_blk
            k_t[:, lanes] = k_blk
            v_t[:, lanes] = v_blk.astype(jnp.bfloat16)
            stat[0:1, lanes] = jnp.sum(q_blk * q_blk, axis=0, keepdims=True)
            stat[1:2, lanes] = jnp.sum(k_blk * k_blk, axis=0, keepdims=True)
        return carry

    lax.fori_loop(0, 24, event, 0)
    gath.drain(0)

    def to_peer(off):
        return remote(stat, slots.at[me], stat_send.at[off], stat_recv.at[me], (me + off) % n_dev)

    for off in range(1, n_dev):
        to_peer(off).start()
    slots[me] = stat[...]
    for off in range(1, n_dev):
        other = (me + off) % n_dev
        remote(stat, slots.at[other], stat_send.at[off], stat_recv.at[other], other).wait_recv()
    stat_total = jnp.sum(slots[...], axis=0)
    inv_rms = lax.rsqrt(stat_total / (n_dev * dim) + NORM_EPS)
    for off in range(1, n_dev):
        to_peer(off).wait_send()
    slots[0] = inv_rms

    def rotate(blk, carry):
        lanes = pl.ds(pl.multiple_of(blk * KEY_BLOCK, KEY_BLOCK), KEY_BLOCK)
        cos_b, sin_b = cos_ref[:, lanes], sin_ref[:, lanes]
        heads = []
        for row, raw, gain in ((0, q_t, columns[0]), (1, k_t, columns[1])):
            normed = raw[:, lanes] * slots[0, row:row + 1, lanes] * gain
            first, second = normed[:half], normed[half:]
            heads.append(jnp.concatenate([first * cos_b - second * sin_b, second * cos_b + first * sin_b], axis=0))
        q_b[:, lanes] = heads[0].astype(jnp.bfloat16)
        k_rows[lanes, :] = heads[1].T.astype(jnp.bfloat16)
        return carry

    lax.fori_loop(0, n_tok // KEY_BLOCK, rotate, 0)

    def attend(blk, carry):
        queries = pl.ds(pl.multiple_of(blk * KEY_BLOCK, KEY_BLOCK), KEY_BLOCK)
        q_blk = q_b[:, queries]
        key_rows = lambda j: pl.ds(pl.multiple_of(j * KEY_BLOCK, KEY_BLOCK), KEY_BLOCK)

        def score(j, top):
            raw = jnp.dot(k_rows[key_rows(j), :], q_blk, preferred_element_type=jnp.float32) * (dim ** -0.5)
            key_pos = lax.broadcasted_iota(jnp.int32, raw.shape, 0) + (j - blk) * KEY_BLOCK
            raw = jnp.where(key_pos <= lax.broadcasted_iota(jnp.int32, raw.shape, 1), raw, -1e30)
            scores[key_rows(j), :] = raw
            return jnp.maximum(top, jnp.max(raw, axis=0, keepdims=True))

        top = lax.fori_loop(0, blk + 1, score, jnp.full((1, KEY_BLOCK), -1e30, jnp.float32))

        def expo(j, norm):
            raised = jnp.exp(scores[key_rows(j), :] - top)
            scores[key_rows(j), :] = raised
            return norm + jnp.sum(raised, axis=0, keepdims=True)

        norm = lax.fori_loop(0, blk + 1, expo, jnp.zeros((1, KEY_BLOCK), jnp.float32))
        inv_norm = 1.0 / norm

        def weigh(j, acc):
            prob = (scores[key_rows(j), :] * inv_norm).astype(jnp.bfloat16)
            return acc + jnp.dot(v_t[:, key_rows(j)], prob, preferred_element_type=jnp.float32)

        ctx = lax.fori_loop(0, blk + 1, weigh, jnp.zeros((dim, KEY_BLOCK), jnp.float32)).T.astype(jnp.bfloat16)
        n_chunks = out_ref.shape[0]
        piece = rows // n_chunks
        for dev in range(KEY_BLOCK // rows):
            at = pl.ds(pl.multiple_of((blk * (KEY_BLOCK // rows) + dev) * piece, piece), piece)
            for k in range(n_chunks):
                out_ref[k, at, :] = ctx[dev * rows + k * piece:dev * rows + (k + 1) * piece, :]
        return carry

    lax.fori_loop(0, n_tok // KEY_BLOCK, attend, 0)


def attend_rows(own, wq, wk, wv, q_gain, k_gain, cos_t, sin_t, collective_id):
    n_dev = N_Z * N_Y * 2
    rows, width = own.shape
    n_tok = n_dev * rows
    operands = (own, wq, wk, wv, q_gain, k_gain, cos_t, sin_t)
    return pl.pallas_call(
        attend_kernel,
        in_specs=[pl.BlockSpec(memory_space=pltpu.VMEM)] * len(operands),
        out_specs=pl.BlockSpec(memory_space=pltpu.VMEM),
        out_shape=jax.ShapeDtypeStruct((N_CHUNKS, n_tok // N_CHUNKS, HEAD_DIM), jnp.bfloat16),
        scratch_shapes=[
            pltpu.VMEM((n_dev, rows, width), jnp.bfloat16),
            pltpu.VMEM((width, 3 * HEAD_DIM), jnp.bfloat16),
            pltpu.VMEM((HEAD_DIM, n_tok), jnp.float32),
            pltpu.VMEM((HEAD_DIM, n_tok), jnp.float32),
            pltpu.VMEM((HEAD_DIM, n_tok), jnp.bfloat16),
            pltpu.VMEM((HEAD_DIM, n_tok), jnp.bfloat16),
            pltpu.VMEM((n_tok, HEAD_DIM), jnp.bfloat16),
            pltpu.VMEM((2, n_tok), jnp.float32),
            pltpu.VMEM((n_dev, 2, n_tok), jnp.float32),
            pltpu.VMEM((n_tok, KEY_BLOCK), jnp.float32),
            pltpu.SemaphoreType.DMA((n_dev,)),
            pltpu.SemaphoreType.DMA((n_dev,)),
        ] + chunk_sems(Gather, 1),
        compiler_params=pltpu.CompilerParams(collective_id=collective_id, has_side_effects=True, vmem_limit_bytes=VMEM_LIMIT),
        name="attend_rows",
    )(*operands)


SUM_STEPS = {0: 0, 1: 1, 3: 2, 4: 3, 5: 4, 6: 5}


def moe_kernel(n_chunks, exp_step, ctx_ref, wo_ref, x_ref, gain_ref, route_ref, wr_ref, wg_ref, wu_ref, wd_ref, out_ref, acc_ref, gate_ref, full, part, total, m_own, h_own, chosen, *rest):
    bufs, rest = rest[:6], rest[6:]
    n_sc = len(Scatter.SEMS)
    attn_sems, moe_sems, gather_sems = rest[:n_sc], rest[n_sc:2 * n_sc], rest[2 * n_sc:]
    chunk, step = pl.program_id(0), pl.program_id(1)
    n_steps = pl.num_programs(1)
    rows = m_own.shape[0] // n_chunks
    n_exp = wr_ref.shape[0]
    exp_ff = wg_ref.shape[0] // exp_step
    n_tok = full.shape[1]
    nt_dims = (((1,), (1,)), ((), ()))
    place = Place()
    loc_rows = lambda k: pl.ds(pl.multiple_of(k * rows, rows), rows)
    block = lambda ref: (lambda d, k: ref.at[k, pl.ds(pl.multiple_of(d * rows, rows), rows), :])
    gath = Gather(place, lambda k: m_own.at[loc_rows(k), :], block(full), gather_sems)
    attn = Scatter(place, block(part), bufs, total, attn_sems)
    scat = Scatter(place, block(part), bufs, total, moe_sems)

    def project(k):
        part[k] = jnp.dot(ctx_ref[k], wo_ref[...], preferred_element_type=jnp.float32).astype(jnp.bfloat16)

    def attn_stage(number, k):
        attn.stage(number, k)
        if number == N_STAGES - 1:
            attn_out = total[...].astype(jnp.bfloat16).astype(jnp.float32)
            hidden = (x_ref[loc_rows(k), :].astype(jnp.float32) + attn_out).astype(jnp.bfloat16)
            h_own[loc_rows(k), :] = hidden
            normed = norm_rows(hidden.astype(jnp.float32), gain_ref[...].astype(jnp.float32).reshape(1, -1))
            m_own[loc_rows(k), :] = normed
            full[k, pl.ds(pl.multiple_of(place.me * rows, rows), rows), :] = normed

    def moe_stage(number, k):
        scat.stage(number, k)
        if number == N_STAGES - 1:
            moe_out = total[...].astype(jnp.bfloat16).astype(jnp.float32)
            out_ref[loc_rows(k), :] = (h_own[loc_rows(k), :].astype(jnp.float32) + moe_out).astype(jnp.bfloat16)

    @pl.when((chunk == 0) & (step == 0))
    def _():
        entry_barrier(place)
        for k in (0, 1):
            project(k)
            attn_stage(0, k)
        attn_stage(1, 0)

        def project_next(k, carry):
            project(k)
            attn_stage(0, k)
            return carry

        lax.fori_loop(2, n_chunks, project_next, 0)
        attn_stage(1, 1)
        for dev in range(n_tok // rows):
            routes = route_ref[:, dev * rows * n_chunks:(dev + 1) * rows * n_chunks]
            expert = lax.broadcasted_iota(jnp.int32, (n_exp, rows * n_chunks), 0)
            hits = jnp.zeros(expert.shape, jnp.float32)
            for choice in range(routes.shape[0]):
                hits = jnp.where(routes[choice:choice + 1] == expert, 1.0, hits)
            picked = jnp.concatenate([hits, jnp.zeros_like(hits)], axis=0).T
            for k in range(n_chunks):
                chosen[k, dev * rows:(dev + 1) * rows, :] = picked[k * rows:(k + 1) * rows, :n_exp]
        for number in range(2, N_STAGES):
            attn_stage(number, 0)
        attn_stage(2, 1)
        gath.stage(0, 0)
        attn_stage(3, 1)
        for number in (1, 4):
            gath.stage(number, 0)
        attn_stage(4, 1)
        for number in (2, 5):
            gath.stage(number, 0)
        attn_stage(5, 1)
        for number in (3, 6, 7, 8):
            gath.stage(number, 0)

    for at in range(2 * N_Z):
        @pl.when((step == at) & (chunk + 1 < n_chunks))
        def _():
            gath.stage(at, chunk + 1)

        if at in SUM_STEPS:
            @pl.when((step == at) & (chunk > 0))
            def _():
                moe_stage(SUM_STEPS[at], chunk - 1)

            if at > 0:
                @pl.when((step == at) & (chunk == 0))
                def _():
                    attn_stage(SUM_STEPS[at], 2)

    for at, number in ((5, 1), (7, 2)):
        @pl.when((step == at) & (chunk + 3 < n_chunks))
        def _():
            attn_stage(number, chunk + 3)

    for at, number in ((0, 3), (1, 4), (2, 5)):
        @pl.when((step == at) & (chunk > 0) & (chunk + 2 < n_chunks))
        def _():
            attn_stage(number, chunk + 2)

    @pl.when((step == 0) & (chunk > 0))
    def _():
        gath.stage(GATHER_LAST, chunk)

    @pl.when(step == 0)
    def _():
        logits = lax.dot_general(full[chunk], wr_ref[...], nt_dims, preferred_element_type=jnp.float32)
        logits = logits - jnp.max(logits, axis=-1, keepdims=True)
        expd = jnp.exp(logits)
        gates = expd / jnp.sum(expd, axis=-1, keepdims=True) * chosen[chunk]
        for grp in range(n_exp // exp_step):
            gate_ref[grp] = gates[:, grp * exp_step:(grp + 1) * exp_step]
        acc_ref[...] = jnp.zeros_like(acc_ref)

    m_rows = full[chunk]
    gate_proj = lax.dot_general(m_rows, wg_ref[...], nt_dims, preferred_element_type=jnp.float32)
    up_proj = lax.dot_general(m_rows, wu_ref[...], nt_dims, preferred_element_type=jnp.float32)
    act = (gate_proj / (1.0 + jnp.exp(-gate_proj)) * up_proj).astype(jnp.bfloat16).astype(jnp.float32)
    gates = gate_ref[step]
    lane = lax.broadcasted_iota(jnp.int32, (n_tok, 2 * exp_ff), 1)
    pieces = []
    for pair in range(exp_step // 2):
        pieces.append(jnp.where(lane < exp_ff, gates[:, 2 * pair:2 * pair + 1], gates[:, 2 * pair + 1:2 * pair + 2]))
    scaled = act * jnp.concatenate(pieces, axis=1)
    high = scaled.astype(jnp.bfloat16)
    low = (scaled - high.astype(jnp.float32)).astype(jnp.bfloat16)
    both = jnp.concatenate([high, low], axis=0)
    for col in range(0, acc_ref.shape[1], DOWN_COLS):
        cols = slice(col, col + DOWN_COLS)
        down = jnp.dot(both, wd_ref[:, cols], preferred_element_type=jnp.float32)
        acc_ref[:, cols] += down[:n_tok] + down[n_tok:]

    @pl.when(step == n_steps - 1)
    def _():
        attn.drain(chunk)
        part[chunk] = acc_ref[...].astype(jnp.bfloat16)

    @pl.when((step == n_steps - 1) & (chunk == n_chunks - 1))
    def _():
        for number in range(N_STAGES):
            moe_stage(number, n_chunks - 1)

        def drain(k, carry):
            gath.drain(k)
            scat.drain(k)
            return carry

        lax.fori_loop(0, n_chunks, drain, 0)


def moe_layer(ctx, w_out, x_loc, gain, routes, wr_t, wg_t, wu_t, w_dn, collective_id):
    rows_loc, width = x_loc.shape
    n_chunks, n_tok = ctx.shape[:2]
    n_exp = wr_t.shape[0]
    n_ff = wg_t.shape[0]
    step_cols = n_ff // n_exp * EXP_PER_STEP
    rows = rows_loc // n_chunks
    const = lambda k, s: (0, 0)
    return pl.pallas_call(
        functools.partial(moe_kernel, n_chunks, EXP_PER_STEP),
        grid=(n_chunks, n_ff // step_cols),
        in_specs=[
            pl.BlockSpec(ctx.shape, lambda k, s: (0, 0, 0)),
            pl.BlockSpec(w_out.shape, const),
            pl.BlockSpec((rows_loc, width), const),
            pl.BlockSpec((width,), lambda k, s: (0,)),
            pl.BlockSpec(routes.shape, const),
            pl.BlockSpec((n_exp, width), const),
            pl.BlockSpec((step_cols, width), lambda k, s: (s, 0)),
            pl.BlockSpec((step_cols, width), lambda k, s: (s, 0)),
            pl.BlockSpec((step_cols, width), lambda k, s: (s, 0)),
        ],
        out_specs=pl.BlockSpec((rows_loc, width), const),
        out_shape=jax.ShapeDtypeStruct((rows_loc, width), jnp.bfloat16),
        scratch_shapes=[
            pltpu.VMEM((n_tok, width), jnp.float32),
            pltpu.VMEM((n_exp // EXP_PER_STEP, n_tok, EXP_PER_STEP), jnp.float32),
            pltpu.VMEM((n_chunks, n_tok, width), jnp.bfloat16),
            pltpu.VMEM((n_chunks, n_tok, width), jnp.bfloat16),
            pltpu.VMEM((rows, width), jnp.float32),
            pltpu.VMEM((rows_loc, width), jnp.bfloat16),
            pltpu.VMEM((rows_loc, width), jnp.bfloat16),
            pltpu.VMEM((n_chunks, n_tok, n_exp), jnp.float32),
        ] + chunk_bufs(n_chunks, rows, width) + chunk_sems(Scatter, n_chunks) + chunk_sems(Scatter, n_chunks) + chunk_sems(Gather, n_chunks),
        compiler_params=pltpu.CompilerParams(dimension_semantics=("arbitrary", "arbitrary"), collective_id=collective_id, has_side_effects=True, vmem_limit_bytes=VMEM_LIMIT),
        name="moe_layer",
    )(ctx, w_out, x_loc, gain, routes, wr_t, wg_t, wu_t, w_dn)


def solution(mesh):
    tp_size = mesh.shape["tp"]
    in_specs = (P("dp", None), P("dp", None, None), P("tp", None), P(None), P(None, "tp"), P(None, "tp"), P(None, "tp"), P("tp", None), P("tp"), P("tp"), P(None), P(None, None), P(None, None, "tp"), P(None, None, "tp"), P(None, "tp", None))

    def device_fn(token_ids, route_idx, embed_table, attn_norm, w_query, w_key, w_value, w_out, q_gain, k_gain, mlp_norm, w_router, w_gate, w_up, w_down):
        batch_loc, seq_len = token_ids.shape
        model_dim = embed_table.shape[1]
        x_loc, a_loc = scatter_rows(token_ids.reshape(1, -1), embed_table, attn_norm, 0)
        cos_t, sin_t = (jnp.asarray(tab) for tab in rope_tables(seq_len))
        context = attend_rows(a_loc, w_query, w_key, w_value, q_gain, k_gain, cos_t, sin_t, 1)
        wg_t = jnp.swapaxes(w_gate, 1, 2).reshape(-1, model_dim)
        wu_t = jnp.swapaxes(w_up, 1, 2).reshape(-1, model_dim)
        w_dn = w_down.reshape(-1, model_dim)
        wr_t = w_router.T
        routes = jnp.swapaxes(route_idx, 1, 2).reshape(route_idx.shape[-1], -1)
        out_loc = moe_layer(context, w_out, x_loc, mlp_norm, routes, wr_t, wg_t, wu_t, w_dn, 4)
        return out_loc.reshape(batch_loc, -1, model_dim)

    return jax.shard_map(device_fn, mesh=mesh, in_specs=in_specs, out_specs=P("dp", "tp", None), check_vma=False)
```

```python
import functools

import jax
import jax.numpy as jnp
import numpy as np
from jax import lax
from jax.experimental import pallas as pl
from jax.experimental.pallas import tpu as pltpu
from jax.sharding import PartitionSpec as P

HEAD_DIM = 128
NORM_EPS = 1e-5
N_CHUNKS = 4
N_TABLE_CHUNKS = 4
EXP_PER_STEP = 8
VMEM_LIMIT = 63 * 1024 * 1024


def rope_tables(seq_len):
    half_dim = HEAD_DIM // 2
    inv_freq = np.float32(1.0) / (np.float32(10000.0) ** (np.arange(half_dim, dtype=np.float32) * np.float32(2.0 / HEAD_DIM)))
    angles = (inv_freq[:, None] * np.arange(seq_len, dtype=np.float32)[None, :]).astype(np.float32)
    return np.cos(angles).astype(np.float32), np.sin(angles).astype(np.float32)


N_STAGES = 6
DOWN_COLS = 256
HOT_COLS = 256
N_Z, N_Y = 4, 2
GATHER_LAST = 8
MESH = pl.DeviceIdType.MESH


class Place:
    def __init__(self):
        self.me = lax.axis_index("tp")
        self.z = self.me // 4
        self.y = self.me % 4 // 2
        self.c = self.me % 2
        self.core_peer = self.me + 1 - 2 * self.c
        self.y_peer = self.me + 2 - 4 * self.y
        self.up = self.me + 4
        self.down = self.me - 4

    def index(self, zz, yy, cc):
        return zz * 4 + yy * 2 + cc


def remote(src, dst, send_sem, recv_sem, device):
    return pltpu.make_async_remote_copy(src_ref=src, dst_ref=dst, send_sem=send_sem, recv_sem=recv_sem, device_id={"tp": device}, device_id_type=MESH)


def entry_barrier(place):
    barrier = pltpu.get_barrier_semaphore()
    for peer in (place.core_peer, place.y_peer):
        pl.semaphore_signal(barrier, inc=1, device_id={"tp": peer}, device_id_type=MESH)

    @pl.when(place.z > 0)
    def _():
        pl.semaphore_signal(barrier, inc=1, device_id={"tp": place.down}, device_id_type=MESH)

    @pl.when(place.z < N_Z - 1)
    def _():
        pl.semaphore_signal(barrier, inc=1, device_id={"tp": place.up}, device_id_type=MESH)

    pl.semaphore_wait(barrier, 2 + (place.z + 3) // 4 + (6 - place.z) // 4)


def by_distance(place, dist, act):
    if dist == 0:
        act(place.z)
        return

    @pl.when(place.z + dist < N_Z)
    def _():
        act(place.z + dist)

    @pl.when(place.z >= dist)
    def _():
        act(place.z - dist)


class Gather:
    SEMS = [(4,), (4,), (4,), (4,), (4,), (8,), (8,)]

    def __init__(self, place, own, shard, sems):
        self.place, self.own, self.shard = place, own, shard
        self.up_send, self.down_send, self.z_recv, self.y_send, self.y_recv, self.c_send, self.c_recv = sems

    def src(self, d, k, mine):
        return self.own(k) if mine else self.shard(d, k)

    def to_up(self, zz, k, mine=False):
        d = self.place.index(zz, self.place.y, self.place.c)
        return remote(self.src(d, k, mine), self.shard(d, k), self.up_send.at[k, zz], self.z_recv.at[k, zz], self.place.up)

    def to_down(self, zz, k, mine=False):
        d = self.place.index(zz, self.place.y, self.place.c)
        return remote(self.src(d, k, mine), self.shard(d, k), self.down_send.at[k, zz], self.z_recv.at[k, zz], self.place.down)

    def to_y(self, zz, k, mine=False, flip=False):
        d = self.place.index(zz, 1 - self.place.y if flip else self.place.y, self.place.c)
        return remote(self.src(d, k, mine), self.shard(d, k), self.y_send.at[k, zz], self.y_recv.at[k, zz], self.place.y_peer)

    def to_core(self, zz, yy, k, mine=False, flip=False):
        d = self.place.index(zz, yy, 1 - self.place.c if flip else self.place.c)
        slot = zz * 2 + yy
        return remote(self.src(d, k, mine), self.shard(d, k), self.c_send.at[k, slot], self.c_recv.at[k, slot], self.place.core_peer)

    def stage(self, number, k):
        place = self.place
        z, y = place.z, place.y
        if number == 0:
            @pl.when(z < N_Z - 1)
            def _():
                self.to_up(z, k, True).start()

            @pl.when(z > 0)
            def _():
                self.to_down(z, k, True).start()

            self.to_y(z, k, True).start()
            self.to_core(z, y, k, True).start()
        elif number < N_Z:
            @pl.when(z >= number)
            def _():
                zz = z - number
                self.to_up(zz, k).wait_recv()

                @pl.when(z < N_Z - 1)
                def _():
                    self.to_up(zz, k).start()

                self.to_y(zz, k).start()
                self.to_core(zz, y, k).start()

            @pl.when(z + number < N_Z)
            def _():
                zz = z + number
                self.to_down(zz, k).wait_recv()

                @pl.when(z > 0)
                def _():
                    self.to_down(zz, k).start()

                self.to_y(zz, k).start()
                self.to_core(zz, y, k).start()
        elif number < 2 * N_Z:
            def pass_on(zz):
                self.to_y(zz, k, flip=True).wait_recv()
                self.to_core(zz, 1 - y, k).start()

            by_distance(place, number - N_Z, pass_on)
        else:
            for zz in range(N_Z):
                for yy in range(N_Y):
                    self.to_core(zz, yy, k, flip=True).wait_recv()

    def drain(self, k):
        z = self.place.z
        for zz in range(N_Z):
            @pl.when((z >= zz) & (z < N_Z - 1))
            def _():
                self.to_up(zz, k).wait_send()

            @pl.when((z <= zz) & (z > 0))
            def _():
                self.to_down(zz, k).wait_send()

            self.to_y(zz, k).wait_send()
            for yy in range(N_Y):
                self.to_core(zz, yy, k).wait_send()


class Scatter:
    SEMS = [(8,), (8,), (4,), (4,), (4,), (4,), (4,), (4,)]
    BUFS = (8, 4, 4, 4, 4, 4)

    def __init__(self, place, shard, bufs, total, sems):
        self.place, self.shard, self.total = place, shard, total
        self.c_buf, self.y_out, self.y_in, self.z_out, self.from_down, self.from_up = bufs
        self.c_send, self.c_recv, self.y_send, self.y_recv, self.up_send, self.up_recv, self.down_send, self.down_recv = sems

    def to_core(self, zz, yy, k):
        slot = zz * 2 + yy
        d = self.place.index(zz, yy, 1 - self.place.c)
        return remote(self.shard(d, k), self.c_buf.at[k, slot], self.c_send.at[k, slot], self.c_recv.at[k, slot], self.place.core_peer)

    def to_y(self, zz, k):
        return remote(self.y_out.at[k, zz], self.y_in.at[k, zz], self.y_send.at[k, zz], self.y_recv.at[k, zz], self.place.y_peer)

    def to_up(self, zz, k):
        return remote(self.z_out.at[k, zz], self.from_down.at[k, zz], self.up_send.at[k, zz], self.up_recv.at[k, zz], self.place.up)

    def to_down(self, zz, k):
        return remote(self.z_out.at[k, zz], self.from_up.at[k, zz], self.down_send.at[k, zz], self.down_recv.at[k, zz], self.place.down)

    def pair_sum(self, zz, yy, k):
        self.to_core(zz, yy, k).wait_recv()
        mine = self.shard(self.place.index(zz, yy, self.place.c), k)[...].astype(jnp.float32)
        return mine + self.c_buf[k, zz * 2 + yy].astype(jnp.float32)

    def chip_pair_sum(self, zz, k):
        both = self.pair_sum(zz, self.place.y, k)
        self.to_y(zz, k).wait_recv()
        return both + self.y_in[k, zz].astype(jnp.float32)

    def stage(self, number, k):
        place = self.place
        z, y = place.z, place.y
        if number == 0:
            for yy in (1 - y, y):
                for zz in range(N_Z):
                    self.to_core(zz, yy, k).start()
        elif number == 1:
            def send_y(zz):
                self.y_out[k, zz] = self.pair_sum(zz, 1 - y, k).astype(jnp.bfloat16)
                self.to_y(zz, k).start()

            for dist in (3, 2, 1, 0):
                by_distance(place, dist, send_y)
        elif number < N_STAGES - 1:
            dist = N_STAGES - 1 - number

            @pl.when(z + dist < N_Z)
            def _():
                zz = z + dist
                self.total[...] = self.chip_pair_sum(zz, k)

                @pl.when(z > 0)
                def _():
                    self.to_up(zz, k).wait_recv()
                    self.total[...] += self.from_down[k, zz].astype(jnp.float32)

                self.z_out[k, zz] = self.total[...].astype(jnp.bfloat16)
                self.to_up(zz, k).start()

            @pl.when(z >= dist)
            def _():
                zz = z - dist
                self.total[...] = self.chip_pair_sum(zz, k)

                @pl.when(z < N_Z - 1)
                def _():
                    self.to_down(zz, k).wait_recv()
                    self.total[...] += self.from_up[k, zz].astype(jnp.float32)

                self.z_out[k, zz] = self.total[...].astype(jnp.bfloat16)
                self.to_down(zz, k).start()
        else:
            self.total[...] = self.chip_pair_sum(z, k)

            @pl.when(z > 0)
            def _():
                self.to_up(z, k).wait_recv()
                self.total[...] += self.from_down[k, z].astype(jnp.float32)

            @pl.when(z < N_Z - 1)
            def _():
                self.to_down(z, k).wait_recv()
                self.total[...] += self.from_up[k, z].astype(jnp.float32)

    def drain(self, k):
        z = self.place.z
        for zz in range(N_Z):
            for yy in range(N_Y):
                self.to_core(zz, yy, k).wait_send()
            self.to_y(zz, k).wait_send()

            @pl.when(z < zz)
            def _():
                self.to_up(zz, k).wait_send()

            @pl.when(z > zz)
            def _():
                self.to_down(zz, k).wait_send()


def chunk_sems(kind, n_chunks):
    return [pltpu.SemaphoreType.DMA((n_chunks,) + shape) for shape in kind.SEMS]


def chunk_bufs(n_chunks, rows, width):
    return [pltpu.VMEM((n_chunks, slots, rows, width), jnp.bfloat16) for slots in Scatter.BUFS]


def norm_rows(rows_f32, gain_f32):
    mean_sq = jnp.mean(rows_f32 * rows_f32, axis=-1, keepdims=True)
    return (rows_f32 * lax.rsqrt(mean_sq + NORM_EPS) * gain_f32).astype(jnp.bfloat16)


def scatter_kernel(n_chunks, ids_ref, gain, table_ref, sum_ref, norm_ref, table, hot, part, total, id_cols, table_sem, *scratch):
    bufs, sems = scratch[:6], scratch[6:]
    rows = total.shape[0]
    n_tok, vocab_pad = hot.shape
    vocab = table_ref.shape[0]
    width = table.shape[1]
    lanes = 128
    place = Place()
    chunk_rows = lambda k: pl.ds(pl.multiple_of(k * rows, rows), rows)
    scat = Scatter(place, lambda d, k: part.at[k, pl.ds(pl.multiple_of(d * rows, rows), rows), :], bufs, total, sems)
    load = pltpu.make_async_copy(table_ref, table.at[pl.ds(0, vocab), :], table_sem)
    load.start()
    for d in range(n_tok // rows):
        span = slice(d * rows * n_chunks, (d + 1) * rows * n_chunks)
        id_cols[d] = jnp.broadcast_to(ids_ref[:, span], (lanes, rows * n_chunks)).T
    table[vocab:, :] = jnp.zeros((vocab_pad - vocab, width), jnp.bfloat16)
    entry_barrier(place)

    def look_up(k):
        ids = jnp.concatenate([id_cols[d, chunk_rows(k), :] for d in range(n_tok // rows)], axis=0) - place.me * vocab
        lane = lax.broadcasted_iota(jnp.int32, (n_tok, lanes), 1)
        for col in range(0, vocab_pad, lanes):
            in_table = lane + col < vocab if col + lanes > vocab else True
            hot[:, col:col + lanes] = jnp.where((ids == lane + col) & in_table, 1.0, 0.0).astype(jnp.bfloat16)

    def product(k):
        def columns(n, inner):
            cols = pl.ds(pl.multiple_of(n * HOT_COLS, HOT_COLS), HOT_COLS)
            part[k, :, cols] = jnp.dot(hot[...], table[:, cols], preferred_element_type=jnp.float32).astype(jnp.bfloat16)
            return inner

        lax.fori_loop(0, width // HOT_COLS, columns, 0)

    def finish(k):
        value = total[...].astype(jnp.bfloat16)
        sum_ref[chunk_rows(k), :] = value
        norm_ref[chunk_rows(k), :] = norm_rows(value.astype(jnp.float32), gain[...].astype(jnp.float32).reshape(1, -1))

    def wave(t, carry):
        for number in range(N_STAGES - 1, 1, -1):
            k = t - number

            @pl.when((k >= 0) & (k < n_chunks))
            def _():
                scat.stage(number, k)
                if number == N_STAGES - 1:
                    finish(k)

        @pl.when((t >= 1) & (t - 1 < n_chunks))
        def _():
            scat.stage(1, t - 1)

        @pl.when(t < n_chunks)
        def _():
            look_up(t)

            @pl.when(t == 0)
            def _():
                load.wait()

            product(t)
            scat.stage(0, t)
        return carry

    def drain(k, carry):
        scat.drain(k)
        return carry

    lax.fori_loop(0, n_chunks + N_STAGES - 1, wave, 0)
    lax.fori_loop(0, n_chunks, drain, 0)


def scatter_rows(ids, table, gain, collective_id):
    n_dev = N_Z * N_Y * 2
    vocab, width = table.shape
    n_chunks = N_TABLE_CHUNKS
    n_tok = ids.shape[1] // n_chunks
    rows = n_tok // n_dev
    vocab_pad = -(-vocab // 256) * 256
    out = jax.ShapeDtypeStruct((n_chunks * rows, width), jnp.bfloat16)
    vmem = pl.BlockSpec(memory_space=pltpu.VMEM)
    return pl.pallas_call(
        functools.partial(scatter_kernel, n_chunks),
        in_specs=[vmem, vmem, pl.BlockSpec(memory_space=pl.ANY)],
        out_specs=[vmem] * 2,
        out_shape=[out, out],
        scratch_shapes=[
            pltpu.VMEM((vocab_pad, width), jnp.bfloat16),
            pltpu.VMEM((n_tok, vocab_pad), jnp.bfloat16),
            pltpu.VMEM((n_chunks, n_tok, width), jnp.bfloat16),
            pltpu.VMEM((rows, width), jnp.float32),
            pltpu.VMEM((n_dev, rows * n_chunks, 128), jnp.int32),
            pltpu.SemaphoreType.DMA,
        ] + chunk_bufs(n_chunks, rows, width) + chunk_sems(Scatter, n_chunks),
        compiler_params=pltpu.CompilerParams(collective_id=collective_id, has_side_effects=True, vmem_limit_bytes=VMEM_LIMIT),
        name="scatter_rows",
    )(ids, gain, table)


KEY_BLOCK = 512


def attend_kernel(own_ref, wq_ref, wk_ref, wv_ref, qg_ref, kg_ref, cos_ref, sin_ref, out_ref, full, w_all, q_t, k_t, v_t, q_b, k_rows, stat, slots, scores, stat_send, stat_recv, *sems):
    n_dev, rows, width = full.shape
    n_tok = n_dev * rows
    dim = HEAD_DIM
    half = dim // 2
    place = Place()
    me, z, y, c = place.me, place.z, place.y, place.c
    gath = Gather(place, lambda k: own_ref, lambda d, k: full.at[d], sems)
    barrier = pltpu.get_barrier_semaphore()
    for off in range(1, n_dev):
        pl.semaphore_signal(barrier, inc=1, device_id={"tp": (me + off) % n_dev}, device_id_type=MESH)
    pl.semaphore_wait(barrier, n_dev - 1)
    gath.stage(0, 0)
    full[me] = own_ref[...]
    for pos, w_ref in enumerate((wq_ref, wk_ref, wv_ref)):
        w_all[:, pos * dim:(pos + 1) * dim] = w_ref[...]
    columns = [jnp.broadcast_to(ref[...].astype(jnp.float32).reshape(1, -1), (dim, dim)).T[:, :1] for ref in (qg_ref, kg_ref)]
    packed = jnp.where(z == 0, 228, jnp.where(z == 1, 225, jnp.where(z == 2, 30, 27)))

    def event(e, carry):
        turn, kind = e // 4, e % 4
        rank = turn - (kind + 1) // 2
        valid = (rank >= 0) & (rank < N_Z)
        zz = (packed >> (2 * jnp.clip(rank, 0, N_Z - 1))) & 3

        @pl.when(valid & (kind == 0) & (zz < z))
        def _():
            gath.to_up(zz, 0).wait_recv()

            @pl.when(z < N_Z - 1)
            def _():
                gath.to_up(zz, 0).start()

        @pl.when(valid & (kind == 0) & (zz > z))
        def _():
            gath.to_down(zz, 0).wait_recv()

            @pl.when(z > 0)
            def _():
                gath.to_down(zz, 0).start()

        @pl.when(valid & (kind == 0) & (rank > 0))
        def _():
            gath.to_y(zz, 0).start()
            gath.to_core(zz, y, 0).start()

        @pl.when(valid & (kind == 1))
        def _():
            gath.to_core(zz, y, 0, flip=True).wait_recv()

        @pl.when(valid & (kind == 2))
        def _():
            gath.to_y(zz, 0, flip=True).wait_recv()
            gath.to_core(zz, 1 - y, 0).start()

        @pl.when(valid & (kind == 3))
        def _():
            gath.to_core(zz, 1 - y, 0, flip=True).wait_recv()

        @pl.when(valid)
        def _():
            d = zz * 4 + (y + kind // 2) % 2 * 2 + (c + kind) % 2
            lanes = pl.ds(pl.multiple_of(d * rows, rows), rows)
            qkv = jnp.dot(full[d], w_all[...], preferred_element_type=jnp.float32)
            q_blk, k_blk, v_blk = (qkv[:, i * dim:(i + 1) * dim].T for i in range(3))
            q_t[:, lanes] = q_blk
            k_t[:, lanes] = k_blk
            v_t[:, lanes] = v_blk.astype(jnp.bfloat16)
            stat[0:1, lanes] = jnp.sum(q_blk * q_blk, axis=0, keepdims=True)
            stat[1:2, lanes] = jnp.sum(k_blk * k_blk, axis=0, keepdims=True)
        return carry

    lax.fori_loop(0, 24, event, 0)
    gath.drain(0)

    def to_peer(off):
        return remote(stat, slots.at[me], stat_send.at[off], stat_recv.at[me], (me + off) % n_dev)

    for off in range(1, n_dev):
        to_peer(off).start()
    slots[me] = stat[...]
    for off in range(1, n_dev):
        other = (me + off) % n_dev
        remote(stat, slots.at[other], stat_send.at[off], stat_recv.at[other], other).wait_recv()
    stat_total = jnp.sum(slots[...], axis=0)
    inv_rms = lax.rsqrt(stat_total / (n_dev * dim) + NORM_EPS)
    for off in range(1, n_dev):
        to_peer(off).wait_send()
    slots[0] = inv_rms

    def rotate(blk, carry):
        lanes = pl.ds(pl.multiple_of(blk * KEY_BLOCK, KEY_BLOCK), KEY_BLOCK)
        cos_b, sin_b = cos_ref[:, lanes], sin_ref[:, lanes]
        heads = []
        for row, raw, gain in ((0, q_t, columns[0]), (1, k_t, columns[1])):
            normed = raw[:, lanes] * slots[0, row:row + 1, lanes] * gain
            first, second = normed[:half], normed[half:]
            heads.append(jnp.concatenate([first * cos_b - second * sin_b, second * cos_b + first * sin_b], axis=0))
        q_b[:, lanes] = heads[0].astype(jnp.bfloat16)
        k_rows[lanes, :] = heads[1].T.astype(jnp.bfloat16)
        return carry

    lax.fori_loop(0, n_tok // KEY_BLOCK, rotate, 0)

    def attend(blk, carry):
        queries = pl.ds(pl.multiple_of(blk * KEY_BLOCK, KEY_BLOCK), KEY_BLOCK)
        q_blk = q_b[:, queries]
        key_rows = lambda j: pl.ds(pl.multiple_of(j * KEY_BLOCK, KEY_BLOCK), KEY_BLOCK)

        def score(j, top):
            raw = jnp.dot(k_rows[key_rows(j), :], q_blk, preferred_element_type=jnp.float32) * (dim ** -0.5)
            key_pos = lax.broadcasted_iota(jnp.int32, raw.shape, 0) + (j - blk) * KEY_BLOCK
            raw = jnp.where(key_pos <= lax.broadcasted_iota(jnp.int32, raw.shape, 1), raw, -1e30)
            scores[key_rows(j), :] = raw
            return jnp.maximum(top, jnp.max(raw, axis=0, keepdims=True))

        top = lax.fori_loop(0, blk + 1, score, jnp.full((1, KEY_BLOCK), -1e30, jnp.float32))

        def expo(j, norm):
            raised = jnp.exp(scores[key_rows(j), :] - top)
            scores[key_rows(j), :] = raised
            return norm + jnp.sum(raised, axis=0, keepdims=True)

        norm = lax.fori_loop(0, blk + 1, expo, jnp.zeros((1, KEY_BLOCK), jnp.float32))
        inv_norm = 1.0 / norm

        def weigh(j, acc):
            prob = (scores[key_rows(j), :] * inv_norm).astype(jnp.bfloat16)
            return acc + jnp.dot(v_t[:, key_rows(j)], prob, preferred_element_type=jnp.float32)

        ctx = lax.fori_loop(0, blk + 1, weigh, jnp.zeros((dim, KEY_BLOCK), jnp.float32)).T.astype(jnp.bfloat16)
        n_chunks = out_ref.shape[0]
        piece = rows // n_chunks
        for dev in range(KEY_BLOCK // rows):
            at = pl.ds(pl.multiple_of((blk * (KEY_BLOCK // rows) + dev) * piece, piece), piece)
            for k in range(n_chunks):
                out_ref[k, at, :] = ctx[dev * rows + k * piece:dev * rows + (k + 1) * piece, :]
        return carry

    lax.fori_loop(0, n_tok // KEY_BLOCK, attend, 0)


def attend_rows(own, wq, wk, wv, q_gain, k_gain, cos_t, sin_t, collective_id):
    n_dev = N_Z * N_Y * 2
    rows, width = own.shape
    n_tok = n_dev * rows
    operands = (own, wq, wk, wv, q_gain, k_gain, cos_t, sin_t)
    return pl.pallas_call(
        attend_kernel,
        in_specs=[pl.BlockSpec(memory_space=pltpu.VMEM)] * len(operands),
        out_specs=pl.BlockSpec(memory_space=pltpu.VMEM),
        out_shape=jax.ShapeDtypeStruct((N_CHUNKS, n_tok // N_CHUNKS, HEAD_DIM), jnp.bfloat16),
        scratch_shapes=[
            pltpu.VMEM((n_dev, rows, width), jnp.bfloat16),
            pltpu.VMEM((width, 3 * HEAD_DIM), jnp.bfloat16),
            pltpu.VMEM((HEAD_DIM, n_tok), jnp.float32),
            pltpu.VMEM((HEAD_DIM, n_tok), jnp.float32),
            pltpu.VMEM((HEAD_DIM, n_tok), jnp.bfloat16),
            pltpu.VMEM((HEAD_DIM, n_tok), jnp.bfloat16),
            pltpu.VMEM((n_tok, HEAD_DIM), jnp.bfloat16),
            pltpu.VMEM((2, n_tok), jnp.float32),
            pltpu.VMEM((n_dev, 2, n_tok), jnp.float32),
            pltpu.VMEM((n_tok, KEY_BLOCK), jnp.float32),
            pltpu.SemaphoreType.DMA((n_dev,)),
            pltpu.SemaphoreType.DMA((n_dev,)),
        ] + chunk_sems(Gather, 1),
        compiler_params=pltpu.CompilerParams(collective_id=collective_id, has_side_effects=True, vmem_limit_bytes=VMEM_LIMIT),
        name="attend_rows",
    )(*operands)


SUM_STEPS = {0: 0, 1: 1, 3: 2, 4: 3, 5: 4, 6: 5}


def moe_kernel(n_chunks, exp_step, ctx_ref, wo_ref, x_ref, gain_ref, route_ref, wr_ref, wg_ref, wu_ref, wd_ref, out_ref, acc_ref, gate_ref, full, part, total, m_own, h_own, chosen, *rest):
    bufs, rest = rest[:6], rest[6:]
    n_sc = len(Scatter.SEMS)
    attn_sems, moe_sems, gather_sems = rest[:n_sc], rest[n_sc:2 * n_sc], rest[2 * n_sc:]
    chunk, step = pl.program_id(0), pl.program_id(1)
    n_steps = pl.num_programs(1)
    rows = m_own.shape[0] // n_chunks
    n_exp = wr_ref.shape[0]
    exp_ff = wg_ref.shape[0] // exp_step
    n_tok = full.shape[1]
    nt_dims = (((1,), (1,)), ((), ()))
    place = Place()
    loc_rows = lambda k: pl.ds(pl.multiple_of(k * rows, rows), rows)
    block = lambda ref: (lambda d, k: ref.at[k, pl.ds(pl.multiple_of(d * rows, rows), rows), :])
    gath = Gather(place, lambda k: m_own.at[loc_rows(k), :], block(full), gather_sems)
    attn = Scatter(place, block(part), bufs, total, attn_sems)
    scat = Scatter(place, block(part), bufs, total, moe_sems)

    def project(k):
        part[k] = jnp.dot(ctx_ref[k], wo_ref[...], preferred_element_type=jnp.float32).astype(jnp.bfloat16)

    def attn_stage(number, k):
        attn.stage(number, k)
        if number == N_STAGES - 1:
            attn_out = total[...].astype(jnp.bfloat16).astype(jnp.float32)
            hidden = (x_ref[loc_rows(k), :].astype(jnp.float32) + attn_out).astype(jnp.bfloat16)
            h_own[loc_rows(k), :] = hidden
            normed = norm_rows(hidden.astype(jnp.float32), gain_ref[...].astype(jnp.float32).reshape(1, -1))
            m_own[loc_rows(k), :] = normed
            full[k, pl.ds(pl.multiple_of(place.me * rows, rows), rows), :] = normed

    def moe_stage(number, k):
        scat.stage(number, k)
        if number == N_STAGES - 1:
            moe_out = total[...].astype(jnp.bfloat16).astype(jnp.float32)
            out_ref[loc_rows(k), :] = (h_own[loc_rows(k), :].astype(jnp.float32) + moe_out).astype(jnp.bfloat16)

    @pl.when((chunk == 0) & (step == 0))
    def _():
        entry_barrier(place)
        for k in (0, 1):
            project(k)
            attn_stage(0, k)
        attn_stage(1, 0)

        def project_next(k, carry):
            project(k)
            attn_stage(0, k)
            return carry

        lax.fori_loop(2, n_chunks, project_next, 0)
        attn_stage(1, 1)
        for dev in range(n_tok // rows):
            routes = route_ref[:, dev * rows * n_chunks:(dev + 1) * rows * n_chunks]
            expert = lax.broadcasted_iota(jnp.int32, (n_exp, rows * n_chunks), 0)
            hits = jnp.zeros(expert.shape, jnp.float32)
            for choice in range(routes.shape[0]):
                hits = jnp.where(routes[choice:choice + 1] == expert, 1.0, hits)
            picked = jnp.concatenate([hits, jnp.zeros_like(hits)], axis=0).T
            for k in range(n_chunks):
                chosen[k, dev * rows:(dev + 1) * rows, :] = picked[k * rows:(k + 1) * rows, :n_exp]
        for number in range(2, N_STAGES):
            attn_stage(number, 0)
        attn_stage(2, 1)
        gath.stage(0, 0)
        attn_stage(3, 1)
        for number in (1, 4):
            gath.stage(number, 0)
        attn_stage(4, 1)
        for number in (2, 5):
            gath.stage(number, 0)
        attn_stage(5, 1)
        for number in (3, 6, 7, 8):
            gath.stage(number, 0)

    for at in range(2 * N_Z):
        @pl.when((step == at) & (chunk + 1 < n_chunks))
        def _():
            gath.stage(at, chunk + 1)

        if at in SUM_STEPS:
            @pl.when((step == at) & (chunk > 0))
            def _():
                moe_stage(SUM_STEPS[at], chunk - 1)

            if at > 0:
                @pl.when((step == at) & (chunk == 0))
                def _():
                    attn_stage(SUM_STEPS[at], 2)

    for at, number in ((5, 1), (7, 2)):
        @pl.when((step == at) & (chunk + 3 < n_chunks))
        def _():
            attn_stage(number, chunk + 3)

    for at, number in ((0, 3), (1, 4), (2, 5)):
        @pl.when((step == at) & (chunk > 0) & (chunk + 2 < n_chunks))
        def _():
            attn_stage(number, chunk + 2)

    @pl.when((step == 0) & (chunk > 0))
    def _():
        gath.stage(GATHER_LAST, chunk)

    @pl.when(step == 0)
    def _():
        logits = lax.dot_general(full[chunk], wr_ref[...], nt_dims, preferred_element_type=jnp.float32)
        logits = logits - jnp.max(logits, axis=-1, keepdims=True)
        expd = jnp.exp(logits)
        gates = expd / jnp.sum(expd, axis=-1, keepdims=True) * chosen[chunk]
        for grp in range(n_exp // exp_step):
            gate_ref[grp] = gates[:, grp * exp_step:(grp + 1) * exp_step]
        acc_ref[...] = jnp.zeros_like(acc_ref)

    m_rows = full[chunk]
    gate_proj = lax.dot_general(m_rows, wg_ref[...], nt_dims, preferred_element_type=jnp.float32)
    up_proj = lax.dot_general(m_rows, wu_ref[...], nt_dims, preferred_element_type=jnp.float32)
    act = (gate_proj / (1.0 + jnp.exp(-gate_proj)) * up_proj).astype(jnp.bfloat16).astype(jnp.float32)
    gates = gate_ref[step]
    lane = lax.broadcasted_iota(jnp.int32, (n_tok, 2 * exp_ff), 1)
    pieces = []
    for pair in range(exp_step // 2):
        pieces.append(jnp.where(lane < exp_ff, gates[:, 2 * pair:2 * pair + 1], gates[:, 2 * pair + 1:2 * pair + 2]))
    scaled = act * jnp.concatenate(pieces, axis=1)
    high = scaled.astype(jnp.bfloat16)
    low = (scaled - high.astype(jnp.float32)).astype(jnp.bfloat16)
    both = jnp.concatenate([high, low], axis=0)
    for col in range(0, acc_ref.shape[1], DOWN_COLS):
        cols = slice(col, col + DOWN_COLS)
        down = jnp.dot(both, wd_ref[:, cols], preferred_element_type=jnp.float32)
        acc_ref[:, cols] += down[:n_tok] + down[n_tok:]

    @pl.when(step == n_steps - 1)
    def _():
        attn.drain(chunk)
        part[chunk] = acc_ref[...].astype(jnp.bfloat16)

    @pl.when((step == n_steps - 1) & (chunk == n_chunks - 1))
    def _():
        for number in range(N_STAGES):
            moe_stage(number, n_chunks - 1)

        def drain(k, carry):
            gath.drain(k)
            scat.drain(k)
            return carry

        lax.fori_loop(0, n_chunks, drain, 0)


def moe_layer(ctx, w_out, x_loc, gain, routes, wr_t, wg_t, wu_t, w_dn, collective_id):
    rows_loc, width = x_loc.shape
    n_chunks, n_tok = ctx.shape[:2]
    n_exp = wr_t.shape[0]
    n_ff = wg_t.shape[0]
    step_cols = n_ff // n_exp * EXP_PER_STEP
    rows = rows_loc // n_chunks
    const = lambda k, s: (0, 0)
    return pl.pallas_call(
        functools.partial(moe_kernel, n_chunks, EXP_PER_STEP),
        grid=(n_chunks, n_ff // step_cols),
        in_specs=[
            pl.BlockSpec(ctx.shape, lambda k, s: (0, 0, 0)),
            pl.BlockSpec(w_out.shape, const),
            pl.BlockSpec((rows_loc, width), const),
            pl.BlockSpec((width,), lambda k, s: (0,)),
            pl.BlockSpec(routes.shape, const),
            pl.BlockSpec((n_exp, width), const),
            pl.BlockSpec((step_cols, width), lambda k, s: (s, 0)),
            pl.BlockSpec((step_cols, width), lambda k, s: (s, 0)),
            pl.BlockSpec((step_cols, width), lambda k, s: (s, 0)),
        ],
        out_specs=pl.BlockSpec((rows_loc, width), const),
        out_shape=jax.ShapeDtypeStruct((rows_loc, width), jnp.bfloat16),
        scratch_shapes=[
            pltpu.VMEM((n_tok, width), jnp.float32),
            pltpu.VMEM((n_exp // EXP_PER_STEP, n_tok, EXP_PER_STEP), jnp.float32),
            pltpu.VMEM((n_chunks, n_tok, width), jnp.bfloat16),
            pltpu.VMEM((n_chunks, n_tok, width), jnp.bfloat16),
            pltpu.VMEM((rows, width), jnp.float32),
            pltpu.VMEM((rows_loc, width), jnp.bfloat16),
            pltpu.VMEM((rows_loc, width), jnp.bfloat16),
            pltpu.VMEM((n_chunks, n_tok, n_exp), jnp.float32),
        ] + chunk_bufs(n_chunks, rows, width) + chunk_sems(Scatter, n_chunks) + chunk_sems(Scatter, n_chunks) + chunk_sems(Gather, n_chunks),
        compiler_params=pltpu.CompilerParams(dimension_semantics=("arbitrary", "arbitrary"), collective_id=collective_id, has_side_effects=True, vmem_limit_bytes=VMEM_LIMIT),
        name="moe_layer",
    )(ctx, w_out, x_loc, gain, routes, wr_t, wg_t, wu_t, w_dn)


def solution(mesh):
    tp_size = mesh.shape["tp"]
    in_specs = (P("dp", None), P("dp", None, None), P("tp", None), P(None), P(None, "tp"), P(None, "tp"), P(None, "tp"), P("tp", None), P("tp"), P("tp"), P(None), P(None, None), P(None, None, "tp"), P(None, None, "tp"), P(None, "tp", None))

    def device_fn(token_ids, route_idx, embed_table, attn_norm, w_query, w_key, w_value, w_out, q_gain, k_gain, mlp_norm, w_router, w_gate, w_up, w_down):
        batch_loc, seq_len = token_ids.shape
        model_dim = embed_table.shape[1]
        x_loc, a_loc = scatter_rows(token_ids.reshape(1, -1), embed_table, attn_norm, 0)
        cos_t, sin_t = (jnp.asarray(tab) for tab in rope_tables(seq_len))
        context = attend_rows(a_loc, w_query, w_key, w_value, q_gain, k_gain, cos_t, sin_t, 1)
        wg_t = jnp.swapaxes(w_gate, 1, 2).reshape(-1, model_dim)
        wu_t = jnp.swapaxes(w_up, 1, 2).reshape(-1, model_dim)
        w_dn = w_down.reshape(-1, model_dim)
        wr_t = w_router.T
        routes = jnp.swapaxes(route_idx, 1, 2).reshape(route_idx.shape[-1], -1)
        out_loc = moe_layer(context, w_out, x_loc, mlp_norm, routes, wr_t, wg_t, wu_t, w_dn, 4)
        return out_loc.reshape(batch_loc, -1, model_dim)

    return jax.shard_map(device_fn, mesh=mesh, in_specs=in_specs, out_specs=P("dp", "tp", None), check_vma=False)
```
